32 devices in a mesh: freq: 8 (over z, core), tm: 4 (over y, x).
Axes of the slice: x: 2, y: 2, z: 4, core: 2. Of those that a mesh axis runs over, the one named last changes fastest.
Arguments:
- band_state: float32 [2048, 4096], P('freq', 'tm'), may hold values from -2.5 to 2.5
- lower_rows: int32 [3, 2048], replicated, may hold values from 0 to 2047, as said below
- upper_rows: int32 [3, 2048], replicated, may hold values from 0 to 2047, as said below
- delays: int32 [3, 2048], replicated, may hold values from 0 to 1024, as said below
- counts: int32 [7], replicated, may hold values from 256 to 2048, as said below
Outputs:
- dedispersed: float32 [2048, 4096], P('freq', 'tm')
The draws below stay inside these ranges and needn't reach their ends.
Inputs may be any that keep to these rules, and one draw needn't show every extreme that they name: `counts`: entry 8 - 8 / 2^k + b is the live row count of output sub-band b of iteration k; it lies between half and all of that sub-band's 2 * 2048 / 2^(3 - k) padded rows, and in every iteration some sub-band has all its rows live. With w = 2048 / 2^(3 - k), lower_rows[k, i] is a row of input sub-band 2 * floor(i / (2 * w)) whose position in that sub-band is below its live count (all w rows are live in iteration 0). With w = 2048 / 2^(3 - k), upper_rows[k, i] is a row of input sub-band 2 * floor(i / (2 * w)) + 1 whose position in that sub-band is below its live count (all w rows are live in iteration 0). delays[k, i] is at most 2048 / 2^(3 - k), and equals it at some row in every iteration.
All inputs are finite; a program needn't handle non-finite values.
Results may differ from the reference program's by a relative error of at most 0.0003.
Values sent between devices are 32-bit elements; how exact they have to be, the bound alone decides.
A program may use at most 64 MiB of HBM per device.

```python
import jax
import jax.numpy as jnp
from jax import lax

DMAX = 2048
ITERS = 3
NT = 4096


def table_draws(key):
    count_parts = []
    lower_parts = []
    upper_parts = []
    delay_parts = []
    all_rows = jnp.arange(DMAX, dtype=jnp.int32)
    previous = jnp.full((2 ** ITERS,), DMAX >> ITERS, jnp.int32)
    for iteration in range(ITERS):
        width_in = DMAX >> ITERS - iteration
        width_out = 2 * width_in
        bands_out = DMAX // width_out
        level_keys = jax.random.split(jax.random.fold_in(key, 101 + iteration), 6)
        fresh_counts = jax.random.randint(level_keys[0], (bands_out,), width_out // 2, width_out + 1, dtype=jnp.int32)
        full_band = jax.random.randint(level_keys[5], (), 0, bands_out, dtype=jnp.int32)
        fresh_counts = jnp.where(jnp.arange(bands_out, dtype=jnp.int32) == full_band, width_out, fresh_counts)
        band_index = all_rows // width_out
        lower_live = previous[2 * band_index]
        upper_live = previous[2 * band_index + 1]
        lower_pick = jax.random.randint(level_keys[1], (DMAX,), 0, 1 << 30, dtype=jnp.int32) % lower_live
        upper_pick = jax.random.randint(level_keys[2], (DMAX,), 0, 1 << 30, dtype=jnp.int32) % upper_live
        delay_pick = jax.random.randint(level_keys[3], (DMAX,), 0, width_in + 1, dtype=jnp.int32)
        spot_row = jax.random.randint(level_keys[4], (), 0, DMAX, dtype=jnp.int32)
        delay_pick = jnp.where(all_rows == spot_row, width_in, delay_pick)
        count_parts.append(fresh_counts)
        lower_parts.append(2 * band_index * width_in + lower_pick)
        upper_parts.append((2 * band_index + 1) * width_in + upper_pick)
        delay_parts.append(delay_pick)
        previous = fresh_counts
    return (jnp.concatenate(count_parts), jnp.stack(lower_parts), jnp.stack(upper_parts), jnp.stack(delay_parts))


def draw_counts(key, part):
    return table_draws(key)[0]


def draw_lower_rows(key, part):
    return table_draws(key)[1]


def draw_upper_rows(key, part):
    return table_draws(key)[2]


def draw_delays(key, part):
    return table_draws(key)[3]


def block_levels(stream_key, dims, shards, smallest, top_value):
    def one(position, parts):
        draws = jax.random.uniform(jax.random.fold_in(jax.random.fold_in(stream_key, 6), position), (parts,), jnp.float32, smallest / len(shards), top_value / len(shards))
        return jnp.repeat(jnp.exp(draws), dims[position] // parts).reshape((-1,) + (1,) * (len(dims) - position - 1))

    loudness = one(*shards[0])
    for cut in shards[1:]:
        loudness = loudness * one(*cut)
    return loudness


def noise(key, dims, spread, limit, cuts=(), held_as=jnp.bfloat16):
    drawn = spread * jax.random.normal(key, dims, jnp.float32)
    if cuts:
        drawn = drawn * block_levels(key, dims, cuts, -0.22, 0.18)
    return jnp.clip(drawn, -limit, limit).astype(held_as)


def setup_inputs(seed: int = 0) -> dict:
    streams_of = jax.random.split(jax.random.key(seed), 6)
    band_state = noise(streams_of[0], (DMAX, NT), 0.35, 2.5, ((0, 8), (1, 4)), jnp.float32)
    lower_rows = draw_lower_rows(jax.random.fold_in(streams_of[5], 71), 0)
    upper_rows = draw_upper_rows(jax.random.fold_in(streams_of[5], 71), 0)
    delays = draw_delays(jax.random.fold_in(streams_of[5], 71), 0)
    counts = draw_counts(jax.random.fold_in(streams_of[5], 71), 0)
    return {"band_state": band_state, "lower_rows": lower_rows, "upper_rows": upper_rows, "delays": delays, "counts": counts}


def delayed_rows(source_rows, shifts):
    positions = jnp.arange(source_rows.shape[1], dtype=jnp.int32)[None, :] - shifts[:, None]
    picked = jnp.take_along_axis(source_rows, jnp.maximum(positions, 0), axis=1)
    return jnp.where(positions >= 0, picked, jnp.zeros_like(picked))


def reference(band_state, lower_rows, upper_rows, delays, counts):
    block_rows = min(DMAX, 512)
    all_rows = jnp.arange(DMAX, dtype=jnp.int32)
    current = band_state
    for iteration in range(ITERS):
        width_out = DMAX >> (ITERS - iteration - 1)
        offset = 2 ** ITERS - 2 ** (ITERS - iteration)
        live_rows = (all_rows % width_out) < counts[offset + all_rows // width_out]

        def merge_block(pieces, current=current):
            lower_index, upper_index, shifts, keep_rows = pieces
            summed = current[lower_index] + delayed_rows(current[upper_index], shifts)
            return jnp.where(keep_rows[:, None], summed, jnp.zeros_like(summed))

        pieces = (lower_rows[iteration].reshape(-1, block_rows),
                  upper_rows[iteration].reshape(-1, block_rows),
                  delays[iteration].reshape(-1, block_rows),
                  live_rows.reshape(-1, block_rows))
        merged = lax.map(merge_block, pieces)
        current = merged.reshape(DMAX, -1)
    return current
```

```python
import functools

import jax
import jax.numpy as jnp
from jax import lax
from jax.experimental import pallas as pl
from jax.experimental.pallas import tpu as pltpu
from jax.sharding import PartitionSpec as P

DMAX = 2048
ITERS = 3
LANES = 128
SUBLANES = 8
UNROLL = 16
CHUNKS_0 = 4
CHUNK_ROWS = 16
HALO_LAG = 2
MERGE_LAG = 3
EDGE_LAG = 2


def shifted_2(block, axis, distance):
    devices = range(lax.axis_size(axis))
    route = [(i - distance, i) for i in devices if i - distance in devices]
    return lax.ppermute(block, axis, route)


def delay_columns(extended, shifts, widest):
    row_count = extended.shape[0]
    for bit_index in range(widest.bit_length()):
        stride = 1 << bit_index
        shifted = jnp.concatenate(
            [jnp.zeros((row_count, stride), extended.dtype), extended[:, :-stride]], axis=1
        )
        extended = jnp.where((shifts >> bit_index & 1)[:, None] == 1, shifted, extended)
    return extended


def live_mask(global_rows, counts, width_out, offset, bands_out):
    band_index = global_rows // width_out
    band_counts = counts[offset : offset + bands_out]
    matches = band_index[:, None] == jnp.arange(bands_out, dtype=jnp.int32)[None, :]
    live_count = jnp.sum(jnp.where(matches, band_counts[None, :], 0), axis=1)
    return global_rows % width_out < live_count


def per_device_general(band_state, lower_rows, upper_rows, delays, counts):
    row_count, samples = band_state.shape
    freq_index = lax.axis_index("freq")
    first_row = freq_index * row_count
    global_rows = first_row + jnp.arange(row_count, dtype=jnp.int32)
    current = band_state
    for iteration in range(ITERS):
        width_in = DMAX >> ITERS - iteration
        width_out = 2 * width_in
        bands_out = DMAX // width_out
        offset = 2**ITERS - 2 ** (ITERS - iteration)
        lower_source = lax.dynamic_slice_in_dim(lower_rows[iteration], first_row, row_count)
        upper_source = lax.dynamic_slice_in_dim(upper_rows[iteration], first_row, row_count)
        own_delays = lax.dynamic_slice_in_dim(delays[iteration], first_row, row_count)
        gathered = lax.all_gather(current, "freq", axis=0, tiled=True)
        lower_values = jnp.take(gathered, lower_source, axis=0)
        upper_values = jnp.take(gathered, upper_source, axis=0)
        rim_columns = shifted_2(upper_values[:, samples - width_in :], "tm", 1)
        extended = jnp.concatenate([rim_columns, upper_values], axis=1)
        delayed = delay_columns(extended, own_delays, width_in)[:, width_in:]
        live_rows = live_mask(global_rows, counts, width_out, offset, bands_out)
        current = jnp.where(live_rows[:, None], lower_values + delayed, jnp.zeros_like(delayed))
    return current


MESH = pl.DeviceIdType.MESH


def kernel(
    tiles, tm_size, x_ref, lower, upper, delays, counts, select, order,
    out_ref, raw, mine, cur, own_in, far_in, far_pass, halo_in, halo_pass,
    picked, land, early, joined, final,
    s_raw, s_far, s_far_pass, s_own, s_halo, s_halo_pass, s_fo, s_no, s_fi, s_edge,
):
    f, t = lax.axis_index("freq"), lax.axis_index("tm")
    c, z = lax.rem(f, 2), lax.div(f, 2)
    zb, half = lax.rem(z, 2), lax.div(z, 2)
    rows = x_ref.shape[0]
    chunk = CHUNK_ROWS
    n = rows // chunk
    at = lambda ff, tt: {"freq": ff, "tm": tt}
    partner = at(f + 1 - 2 * c, t)
    near = at(f + 2 - 4 * zb, t)
    across = at(f + 4 - 8 * half, t)
    facing = at(f + 2 - 4 * half, t)
    later = at(f, t + 1)
    earlier = at(f, t - 1)
    inner = zb != half
    outer = zb == half
    has_later, has_earlier = t < tm_size - 1, t > 0

    barrier = pltpu.get_barrier_semaphore()

    def greet(target):
        pl.semaphore_signal(barrier, inc=1, device_id=target, device_id_type=MESH)

    greet(partner)
    greet(near)
    greet(across)
    for cond, target in ((inner, facing), (has_earlier, earlier), (has_later, later)):
        pl.when(cond)(functools.partial(greet, target))
    one = lambda cond: jnp.where(cond, 1, 0)
    pl.semaphore_wait(barrier, 3 + one(inner) + one(has_earlier) + one(has_later))

    lane = lax.broadcasted_iota(jnp.int32, (tiles, LANES), 1)
    zero = jnp.zeros((tiles, LANES), jnp.float32)

    def when(cond, action):
        pl.when(cond)(action)

    def remote(src, dst, sems, j, target):
        return pltpu.make_async_remote_copy(
            src_ref=src, dst_ref=dst, send_sem=sems.at[0, j], recv_sem=sems.at[1, j],
            device_id=target, device_id_type=MESH,
        )

    def span(j):
        return pl.ds(pl.multiple_of(j * chunk, chunk), chunk)

    def delayed(source, row, d, first):
        q, r = d >> 7, d & (LANES - 1)
        a = source[row, pl.ds(tiles - q, tiles), :]
        b = source[row, pl.ds(jnp.maximum(tiles - 1 - q, first), tiles), :]
        a, b = pltpu.roll(a, r, 1), pltpu.roll(b, r, 1)
        return jnp.where(lane >= r, a, b)

    def blocks(start, count, value, store):
        def body(step, carry):
            base = start + step * UNROLL
            values = [(base + u, value(base + u)) for u in range(UNROLL)]
            for m, v in values:
                store(m, v)
            return carry

        if count == UNROLL:
            body(0, 0)
        else:
            lax.fori_loop(0, count // UNROLL, body, 0)

    rim0 = rows // LANES
    n0, chunk0 = CHUNKS_0, rows // CHUNKS_0

    def raw_copy(kind, j, row, target, source_at, target_at, size):
        span0 = pl.ds(row + j * chunk0, chunk0)
        return remote(
            raw.at[span0, pl.ds(source_at, size)], raw.at[span0, pl.ds(target_at, size)],
            s_raw, kind * n0 + j, target,
        )

    tail0 = (2 * tiles - rim0, tiles - rim0, rim0)
    kept0 = (tiles - rim0, tiles - rim0, rim0)
    full0 = (tiles, tiles, tiles)
    own0 = lambda j, row: raw_copy(0, j, row, partner, *full0)
    rim_out0 = lambda j: raw_copy(1, j, rows, later, *tail0)
    rim_in0 = lambda j: raw_copy(2, j, rows, partner, *kept0)

    def spread(first, count):
        def body(step, carry):
            r = first + step * SUBLANES
            for tile in range(tiles):
                raw[pl.ds(c * rows + r, SUBLANES), tiles + tile, :] = x_ref[
                    pl.ds(r, SUBLANES), pl.ds(tile * LANES, LANES)
                ]
            return carry

        lax.fori_loop(0, count // SUBLANES, body, 0)

    for j in range(n0):
        spread(j * chunk0, chunk0)
        when((c == 1) & has_later, rim_out0(j).start)
        own0(j, c * rows).start()

    def clear(count, store):
        def body(i, carry):
            for u in range(UNROLL):
                store(i * UNROLL + u)
            return carry

        lax.fori_loop(0, count // UNROLL, body, 0)

    @pl.when(t == 0)
    def _():
        def clear_raw(i):
            raw[rows + i, :tiles, :] = zero

        def clear_cur(i):
            cur[2 * rows + i, :tiles, :] = zero

        def clear_early(i):
            early[i] = zero

        clear(rows, clear_raw)
        clear(2 * rows, clear_cur)
        clear(rows, clear_early)

    for j in range(n0):

        @pl.when((c == 1) & has_earlier)
        def _():
            rim_out0(j).wait_recv()
            rim_in0(j).start()

    for j in range(n0):
        own0(j, (1 - c) * rows).wait_recv()
        when((c == 0) & has_earlier, rim_in0(j).wait_recv)

    own_base, far_base = zb * 2 * rows, (1 - zb) * 2 * rows
    up_base = 2 * rows
    limit0 = counts[z]

    def value0(m):
        i = order[zb, c * rows + m]
        g = z * 2 * rows + i
        wrap = 2 * rows - 1
        lo, up, d = lower[0, g] & wrap, upper[0, g] & wrap, delays[0, g]
        total = raw[lo, tiles:, :] + delayed(raw, up, d, tiles - rim0)
        return jnp.where(i < limit0, total, zero)

    def store0(m, v):
        mine[m] = v
        cur[own_base + c * rows + m, tiles:, :] = v

    limit1 = counts[2 ** (ITERS - 1) + half]
    rim1 = 2 * rows // LANES

    def value1(target_f):
        def value(m):
            j = select[target_f * rows + m]
            wrap = 2 * rows - 1
            a, b = order[2, lower[1, j] & wrap], order[3, upper[1, j] & wrap]
            total = cur[a, tiles:, :] + delayed(cur, up_base + b, delays[1, j], tiles - rim1)
            return jnp.where((j & (4 * rows - 1)) < limit1, total, zero)

        return value

    def store_picked(kind):
        def store(m, v):
            picked[kind, m] = v

        return store

    def store_land(m, v):
        land[half, m] = v

    limit2 = counts[2**ITERS - 2]

    def join(m):
        joined[m, :tiles, :] = early[m]
        joined[m, tiles:, :] = land[1, m]

    def value2(m):
        g = f * rows + m
        total = land[0, m] + delayed(joined, m, delays[2, g], 0)
        return jnp.where(g < limit2, total, zero)

    def store2(m, v):
        final[m] = v

    def finish(k):
        start = pl.multiple_of(k * chunk, chunk)
        for u in range(chunk):
            join(start + u)
        blocks(start, chunk, value2, store2)
        for step in range(chunk // SUBLANES):
            r = pl.multiple_of(start + step * SUBLANES, SUBLANES)
            for tile in range(tiles):
                out_ref[pl.ds(r, SUBLANES), pl.ds(tile * LANES, LANES)] = final[pl.ds(r, SUBLANES), tile, :]

    rim = pl.ds(tiles - rim1, rim1)
    far = lambda j: remote(mine.at[span(j)], far_in.at[span(j)], s_far, j, near)
    far_on = lambda j: remote(far_in.at[span(j)], far_pass.at[span(j)], s_far_pass, j, partner)
    own1 = lambda j: remote(mine.at[span(j)], own_in.at[span(j)], s_own, j, partner)
    halo_mine = lambda j: remote(mine.at[span(j), rim], halo_in.at[span(j), rim], s_halo, j, later)
    halo_far = lambda j: remote(far_in.at[span(j), rim], halo_in.at[span(j), rim], s_halo, j, later)
    halo_on = lambda j: remote(halo_in.at[span(j), rim], halo_pass.at[span(j), rim], s_halo_pass, j, partner)
    far_outer = lambda j, h: remote(picked.at[0, span(j)], land.at[h, span(j)], s_fo, j, across)
    near_outer = lambda j, h: remote(picked.at[1, span(j)], land.at[h, span(j)], s_no, j, near)
    far_inner = lambda j, h: remote(picked.at[2, span(j)], land.at[h, span(j)], s_fi, j, facing)
    edge = lambda j: remote(land.at[1, span(j)], early.at[span(j)], s_edge, j, later)

    def loop(count, body):
        def step(j, carry):
            body(j)
            return carry

        lax.fori_loop(0, count, step, 0)

    f_across, f_near, f_facing = f + 4 - 8 * half, f + 2 - 4 * zb, f + 2 - 4 * half

    def finish_lagged(j):
        @pl.when(j >= EDGE_LAG)
        def _():
            k = j - EDGE_LAG
            when(has_earlier, edge(k).wait_recv)
            finish(k)

    @pl.when(outer)
    def _():
        def produce(j):
            blocks(j * chunk, chunk, value0, store0)
            far(j).start()

        loop(n, produce)

        def from_across(j):
            far_outer(j, 1 - half).wait_recv()
            when((half == 0) & has_later, edge(j).start)

        loop(n, from_across)

        def from_near(j):
            @pl.when(j < n)
            def _():
                near_outer(j, half).wait_recv()
                when((half == 1) & has_later, edge(j).start)

            finish_lagged(j)

        loop(n + EDGE_LAG, from_near)

        def drain(j):
            far(j).wait_send()
            when(has_later, edge(j).wait_send)

        loop(n, drain)

    @pl.when(inner)
    def _():
        def produce(j):
            blocks(j * chunk, chunk, value0, store0)
            own1(j).start()
            when((half == 0) & has_later, halo_mine(j).start)

        loop(n, produce)

        def gather(k):
            far_on(k).wait_recv()
            own1(k).wait_recv()
            start = pl.multiple_of(k * chunk, chunk)
            mine_at, other_at = c * rows + start, (1 - c) * rows + start
            for u in range(chunk):
                cur[own_base + other_at + u, tiles:, :] = own_in[start + u]
                cur[far_base + mine_at + u, tiles:, :] = far_in[start + u]
                cur[far_base + other_at + u, tiles:, :] = far_pass[start + u]

            @pl.when(has_earlier)
            def _():
                halo_on(k).wait_recv()
                for u in range(chunk):
                    cur[up_base + mine_at + u, :tiles, :] = halo_in[start + u]
                    cur[up_base + other_at + u, :tiles, :] = halo_pass[start + u]

            blocks(k * chunk, chunk, value1(f_across), store_picked(0))
            far_outer(k, half).start()

        def stream(j):
            @pl.when(j < n)
            def _():
                far(j).wait_recv()
                far_on(j).start()
                when((half == 1) & has_later, halo_far(j).start)

            @pl.when((j >= HALO_LAG) & (j < n + HALO_LAG) & has_earlier)
            def _():
                halo_mine(j - HALO_LAG).wait_recv()
                halo_on(j - HALO_LAG).start()

            @pl.when(j >= MERGE_LAG)
            def _():
                gather(j - MERGE_LAG)

        loop(n + MERGE_LAG, stream)

        def rest(j):
            blocks(j * chunk, chunk, value1(f_facing), store_picked(2))
            far_inner(j, half).start()
            blocks(j * chunk, chunk, value1(f_near), store_picked(1))
            near_outer(j, half).start()
            blocks(j * chunk, chunk, value1(f), store_land)
            when((half == 1) & has_later, edge(j).start)

        loop(n, rest)

        def receive(j):
            @pl.when(j < n)
            def _():
                far_inner(j, 1 - half).wait_recv()
                when((half == 0) & has_later, edge(j).start)

            finish_lagged(j)

        loop(n + EDGE_LAG, receive)

        def drain(j):
            own1(j).wait_send()
            far_on(j).wait_send()
            when(has_later, halo_mine(j).wait_send)
            when(has_earlier, halo_on(j).wait_send)
            far_outer(j, half).wait_send()
            near_outer(j, half).wait_send()
            far_inner(j, half).wait_send()
            when(has_later, edge(j).wait_send)

        loop(n, drain)

    for j in range(n0):
        own0(j, c * rows).wait_send()
        when((c == 1) & has_later, rim_out0(j).wait_send)
        when((c == 1) & has_earlier, rim_in0(j).wait_send)


def first_use_order(lower_rows, upper_rows, row_count):
    half = lax.axis_index("freq") // 4
    chip_rows, half_rows = 2 * row_count, 4 * row_count
    select = jnp.where(half == 0, lower_rows[2], upper_rows[2])
    wanted = jnp.where(half == 0, select[3 * chip_rows :], select[:chip_rows])
    wanted = wanted.reshape(2, row_count).T.reshape(-1) & (half_rows - 1)
    tables = jnp.stack([lower_rows[1], upper_rows[1]]).reshape(2, 2, half_rows)
    tables = jnp.where(half == 0, tables[:, 0], tables[:, 1]) & (chip_rows - 1)
    at_half = jnp.arange(half_rows, dtype=jnp.int32)
    at_chip = jnp.arange(chip_rows, dtype=jnp.int32)
    hit = wanted[:, None] == at_half[None, :]
    used = jnp.sum(jnp.where(hit[None], tables[:, None, :], 0), axis=2)
    same = used[:, :, None] == at_chip[None, None, :]
    first = jnp.min(jnp.where(same, at_chip[None, :, None], chip_rows), axis=1)
    key = first * chip_rows + at_chip[None, :]
    rank = jnp.sum((key[:, None, :] < key[:, :, None]).astype(jnp.int32), axis=2)
    place = (rank % 2) * row_count + rank // 2
    holds = place[:, :, None] == at_chip[None, None, :]
    row_at = jnp.sum(jnp.where(holds, at_chip[None, :, None], 0), axis=1)
    return select, jnp.concatenate([row_at, place], axis=0)


def per_device_fused(tm_size, band_state, lower_rows, upper_rows, delays, counts):
    row_count, samples = band_state.shape
    tiles = samples // LANES
    n = row_count // CHUNK_ROWS
    dma = pltpu.SemaphoreType.DMA
    wide = pltpu.VMEM((row_count, tiles, LANES), jnp.float32)
    select, order = first_use_order(lower_rows, upper_rows, row_count)
    return pl.pallas_call(
        functools.partial(kernel, tiles, tm_size),
        out_shape=jax.ShapeDtypeStruct((row_count, samples), jnp.float32),
        in_specs=[pl.BlockSpec(memory_space=pltpu.VMEM)] + [pl.BlockSpec(memory_space=pltpu.SMEM)] * 6,
        out_specs=pl.BlockSpec(memory_space=pltpu.VMEM),
        scratch_shapes=[
            pltpu.VMEM((2 * row_count, 2 * tiles, LANES), jnp.float32),
            wide,
            pltpu.VMEM((4 * row_count, 2 * tiles, LANES), jnp.float32),
            wide, wide, wide, wide, wide,
            pltpu.VMEM((3, row_count, tiles, LANES), jnp.float32),
            pltpu.VMEM((2, row_count, tiles, LANES), jnp.float32),
            wide,
            pltpu.VMEM((row_count, 2 * tiles, LANES), jnp.float32),
            wide,
            dma((2, 3 * CHUNKS_0)),
        ]
        + [dma((2, n))] * 9,
        compiler_params=pltpu.CompilerParams(
            collective_id=0, has_side_effects=True, vmem_limit_bytes=60 * 2**20
        ),
    )(band_state, lower_rows, upper_rows, delays, counts, select, order)


def solution(mesh):
    if mesh.shape["freq"] == 2**ITERS:
        body = functools.partial(per_device_fused, mesh.shape["tm"])
    else:
        body = per_device_general
    return jax.shard_map(
        body,
        mesh=mesh,
        in_specs=(P("freq", "tm"), P(), P(), P(), P()),
        out_specs=P("freq", "tm"),
        check_vma=False,
    )
```

```python
import contextlib
import functools

import jax
import jax.numpy as jnp
from jax import lax
from jax.experimental import pallas as pl
from jax.experimental.pallas import tpu as pltpu
from jax.sharding import PartitionSpec as P

DMAX = 2048
ITERS = 3
LANES = 128
SUBLANES = 8
UNROLL = 16
CHUNKS_0 = 4
CHUNK_ROWS = 16
HALO_LAG = 2
MERGE_LAG = 3
OWN_GROUP = 4
OUTER_GROUP = 4
NEAR_GROUP = 2
EDGE_LAG = 4


def shifted_2(block, axis, distance):
    devices = range(lax.axis_size(axis))
    route = [(i - distance, i) for i in devices if i - distance in devices]
    return lax.ppermute(block, axis, route)


def delay_columns(extended, shifts, widest):
    row_count = extended.shape[0]
    for bit_index in range(widest.bit_length()):
        stride = 1 << bit_index
        shifted = jnp.concatenate(
            [jnp.zeros((row_count, stride), extended.dtype), extended[:, :-stride]], axis=1
        )
        extended = jnp.where((shifts >> bit_index & 1)[:, None] == 1, shifted, extended)
    return extended


def live_mask(global_rows, counts, width_out, offset, bands_out):
    band_index = global_rows // width_out
    band_counts = counts[offset : offset + bands_out]
    matches = band_index[:, None] == jnp.arange(bands_out, dtype=jnp.int32)[None, :]
    live_count = jnp.sum(jnp.where(matches, band_counts[None, :], 0), axis=1)
    return global_rows % width_out < live_count


def per_device_general(band_state, lower_rows, upper_rows, delays, counts):
    row_count, samples = band_state.shape
    freq_index = lax.axis_index("freq")
    first_row = freq_index * row_count
    global_rows = first_row + jnp.arange(row_count, dtype=jnp.int32)
    current = band_state
    for iteration in range(ITERS):
        width_in = DMAX >> ITERS - iteration
        width_out = 2 * width_in
        bands_out = DMAX // width_out
        offset = 2**ITERS - 2 ** (ITERS - iteration)
        lower_source = lax.dynamic_slice_in_dim(lower_rows[iteration], first_row, row_count)
        upper_source = lax.dynamic_slice_in_dim(upper_rows[iteration], first_row, row_count)
        own_delays = lax.dynamic_slice_in_dim(delays[iteration], first_row, row_count)
        gathered = lax.all_gather(current, "freq", axis=0, tiled=True)
        lower_values = jnp.take(gathered, lower_source, axis=0)
        upper_values = jnp.take(gathered, upper_source, axis=0)
        rim_columns = shifted_2(upper_values[:, samples - width_in :], "tm", 1)
        extended = jnp.concatenate([rim_columns, upper_values], axis=1)
        delayed = delay_columns(extended, own_delays, width_in)[:, width_in:]
        live_rows = live_mask(global_rows, counts, width_out, offset, bands_out)
        current = jnp.where(live_rows[:, None], lower_values + delayed, jnp.zeros_like(delayed))
    return current


MESH = pl.DeviceIdType.MESH


def phase(name):
    return contextlib.nullcontext()


def kernel(
    tiles, tm_size, x_ref, lower, upper, delays, counts, select, order,
    out_ref, raw, mine, cur, own_in, far_in, far_pass, halo_in, halo_pass,
    picked, land, early, joined, final,
    sent, s_raw, s_far, s_far_pass, s_own, s_halo, s_halo_pass, s_fo, s_no, s_fi, s_edge,
):
    f, t = lax.axis_index("freq"), lax.axis_index("tm")
    c, z = lax.rem(f, 2), lax.div(f, 2)
    zb, half = lax.rem(z, 2), lax.div(z, 2)
    rows = x_ref.shape[0]
    chunk = CHUNK_ROWS
    n = rows // chunk
    at = lambda ff, tt: {"freq": ff, "tm": tt}
    partner = at(f + 1 - 2 * c, t)
    near = at(f + 2 - 4 * zb, t)
    across = at(f + 4 - 8 * half, t)
    facing = at(f + 2 - 4 * half, t)
    later = at(f, t + 1)
    earlier = at(f, t - 1)
    inner = zb != half
    outer = zb == half
    has_later, has_earlier = t < tm_size - 1, t > 0

    barrier = pltpu.get_barrier_semaphore()

    def greet(target):
        pl.semaphore_signal(barrier, inc=1, device_id=target, device_id_type=MESH)

    greet(partner)
    greet(near)
    greet(across)
    for cond, target in ((inner, facing), (has_earlier, earlier), (has_later, later)):
        pl.when(cond)(functools.partial(greet, target))

    lane = lax.broadcasted_iota(jnp.int32, (tiles, LANES), 1)
    zero = jnp.zeros((tiles, LANES), jnp.float32)

    def when(cond, action):
        pl.when(cond)(action)

    def remote(src, dst, flow, sem, target):
        return pltpu.make_async_remote_copy(
            src_ref=src, dst_ref=dst, send_sem=sent.at[flow], recv_sem=sem,
            device_id=target, device_id_type=MESH,
        )

    def span(j, group=1):
        return pl.ds(pl.multiple_of(j * chunk * group, chunk * group), chunk * group)

    def delayed(source, row, d, first):
        q, r = d >> 7, d & (LANES - 1)
        a = source[row, pl.ds(tiles - q, tiles), :]
        b = source[row, pl.ds(jnp.maximum(tiles - 1 - q, first), tiles), :]
        a, b = pltpu.roll(a, r, 1), pltpu.roll(b, r, 1)
        return jnp.where(lane >= r, a, b)

    def blocks(start, count, value, store):
        def body(step, carry):
            base = start + step * UNROLL
            values = [(base + u, value(base + u)) for u in range(UNROLL)]
            for m, v in values:
                store(m, v)
            return carry

        if count == UNROLL:
            body(0, 0)
        else:
            lax.fori_loop(0, count // UNROLL, body, 0)

    rim0 = rows // LANES
    n0, chunk0 = CHUNKS_0, rows // CHUNKS_0

    def raw_copy(kind, j, row, target, source_at, target_at, size):
        span0 = pl.ds(row + j * chunk0, chunk0)
        return remote(
            raw.at[span0, pl.ds(source_at, size)], raw.at[span0, pl.ds(target_at, size)],
            kind, s_raw.at[kind * n0 + j], target,
        )

    tail0 = (2 * tiles - rim0, tiles - rim0, rim0)
    kept0 = (tiles - rim0, tiles - rim0, rim0)
    full0 = (tiles, tiles, tiles)
    own0 = lambda j, row: raw_copy(0, j, row, partner, *full0)
    rim_out0 = lambda j: raw_copy(1, j, rows, later, *tail0)
    rim_in0 = lambda j: raw_copy(2, j, rows, partner, *kept0)

    def spread(first, count):
        def body(step, carry):
            r = first + step * SUBLANES
            for tile in range(tiles):
                raw[pl.ds(c * rows + r, SUBLANES), tiles + tile, :] = x_ref[
                    pl.ds(r, SUBLANES), pl.ds(tile * LANES, LANES)
                ]
            return carry

        lax.fori_loop(0, count // SUBLANES, body, 0)

    with phase("spread"):
        spread(0, rows)
    one = lambda cond: jnp.where(cond, 1, 0)
    with phase("greet"):
        pl.semaphore_wait(barrier, 3 + one(inner) + one(has_earlier) + one(has_later))
    with phase("send0"):
        for j in range(n0):
            when((c == 1) & has_later, rim_out0(j).start)
            own0(j, c * rows).start()

    def clear(count, store):
        def body(i, carry):
            for u in range(UNROLL):
                store(i * UNROLL + u)
            return carry

        lax.fori_loop(0, count // UNROLL, body, 0)

    @pl.when(t == 0)
    def _():
        def clear_raw(i):
            raw[rows + i, :tiles, :] = zero

        def clear_cur(i):
            cur[2 * rows + i, :tiles, :] = zero

        def clear_early(i):
            early[i] = zero

        clear(rows, clear_raw)
        clear(2 * rows, clear_cur)
        clear(rows, clear_early)

    for j in range(n0):

        @pl.when((c == 1) & has_earlier)
        def _():
            with phase("rim_out"):
                rim_out0(j).wait_recv()
                rim_in0(j).start()

    for j in range(n0):
        with phase("own0"):
            own0(j, (1 - c) * rows).wait_recv()
        with phase("rim_in"):
            when((c == 0) & has_earlier, rim_in0(j).wait_recv)

    own_base, far_base = zb * 2 * rows, (1 - zb) * 2 * rows
    up_base = 2 * rows
    limit0 = counts[z]

    def value0(m):
        i = order[zb, c * rows + m]
        g = z * 2 * rows + i
        wrap = 2 * rows - 1
        lo, up, d = lower[0, g] & wrap, upper[0, g] & wrap, delays[0, g]
        total = raw[lo, tiles:, :] + delayed(raw, up, d, tiles - rim0)
        return jnp.where(i < limit0, total, zero)

    def store0(m, v):
        mine[m] = v
        cur[own_base + c * rows + m, tiles:, :] = v

    limit1 = counts[2 ** (ITERS - 1) + half]
    rim1 = 2 * rows // LANES

    def value1(target_f):
        def value(m):
            j = select[target_f * rows + m]
            wrap = 2 * rows - 1
            a, b = order[2, lower[1, j] & wrap], order[3, upper[1, j] & wrap]
            total = cur[a, tiles:, :] + delayed(cur, up_base + b, delays[1, j], tiles - rim1)
            return jnp.where((j & (4 * rows - 1)) < limit1, total, zero)

        return value

    def store_picked(kind):
        def store(m, v):
            picked[kind, m] = v

        return store

    def store_land(m, v):
        land[half, m] = v

    limit2 = counts[2**ITERS - 2]

    def join(m):
        joined[m, :tiles, :] = early[m]
        joined[m, tiles:, :] = land[1, m]

    def value2(m):
        g = f * rows + m
        total = land[0, m] + delayed(joined, m, delays[2, g], 0)
        return jnp.where(g < limit2, total, zero)

    def store2(m, v):
        final[m] = v

    def finish(k):
        start = pl.multiple_of(k * chunk, chunk)
        for u in range(chunk):
            join(start + u)
        blocks(start, chunk, value2, store2)
        for step in range(chunk // SUBLANES):
            r = pl.multiple_of(start + step * SUBLANES, SUBLANES)
            for tile in range(tiles):
                out_ref[pl.ds(r, SUBLANES), pl.ds(tile * LANES, LANES)] = final[pl.ds(r, SUBLANES), tile, :]

    rim = pl.ds(tiles - rim1, rim1)
    every = pl.ds(0, rows)

    def flow(index, src, dst, sems, target):
        def copy(j, group=1, sem=None):
            at_rows = span(j, group)
            return remote(src(at_rows), dst(at_rows), index, sems.at[j if sem is None else sem], target)

        return copy, remote(src(every), dst(every), index, sems.at[0], target)

    far, far_all = flow(3, lambda r: mine.at[r], lambda r: far_in.at[r], s_far, near)
    far_on, far_on_all = flow(4, lambda r: far_in.at[r], lambda r: far_pass.at[r], s_far_pass, partner)
    own1, own1_all = flow(5, lambda r: mine.at[r], lambda r: own_in.at[r], s_own, partner)
    halo_mine, halo_all = flow(6, lambda r: mine.at[r, rim], lambda r: halo_in.at[r, rim], s_halo, later)
    halo_far, _ = flow(6, lambda r: far_in.at[r, rim], lambda r: halo_in.at[r, rim], s_halo, later)
    halo_on, halo_on_all = flow(7, lambda r: halo_in.at[r, rim], lambda r: halo_pass.at[r, rim], s_halo_pass, partner)
    to_half = lambda h: lambda r: land.at[h, r]
    far_outer, far_outer_all = flow(8, lambda r: picked.at[0, r], to_half(half), s_fo, across)
    near_outer, near_outer_all = flow(9, lambda r: picked.at[1, r], to_half(half), s_no, near)
    far_inner, far_inner_all = flow(10, lambda r: picked.at[2, r], to_half(half), s_fi, facing)
    got_across, _ = flow(8, lambda r: picked.at[0, r], to_half(1 - half), s_fo, across)
    got_facing, _ = flow(10, lambda r: picked.at[2, r], to_half(1 - half), s_fi, facing)
    edge, edge_all = flow(11, lambda r: land.at[1, r], lambda r: early.at[r], s_edge, later)

    def loop(name, count, body):
        def step(j, carry):
            with phase(name):
                body(j)
            return carry

        lax.fori_loop(0, count, step, 0)

    f_across, f_near, f_facing = f + 4 - 8 * half, f + 2 - 4 * zb, f + 2 - 4 * half

    def finish_lagged(j):
        @pl.when(j >= EDGE_LAG)
        def _():
            k = j - EDGE_LAG
            when(has_earlier, edge(k).wait_recv)
            finish(k)

    @pl.when(outer)
    def _():
        def produce(j):
            blocks(j * chunk, chunk, value0, store0)
            far(j).start()

        loop("produce", n, produce)

        def from_across(j):
            got_across(j, OUTER_GROUP).wait_recv()
            for i in range(OUTER_GROUP):
                when((half == 0) & has_later, edge(j * OUTER_GROUP + i).start)

        loop("from_across", n // OUTER_GROUP, from_across)

        def from_near(j):
            @pl.when(j < n)
            def _():
                @pl.when(lax.rem(j, NEAR_GROUP) == 0)
                def _():
                    near_outer(lax.div(j, NEAR_GROUP), NEAR_GROUP).wait_recv()

                when((half == 1) & has_later, edge(j).start)

            finish_lagged(j)

        loop("from_near", n + EDGE_LAG, from_near)

        with phase("drain"):
            far_all.wait_send()
            when(has_later, edge_all.wait_send)

    @pl.when(inner)
    def _():
        def produce(j):
            for i in range(OWN_GROUP):
                blocks((j * OWN_GROUP + i) * chunk, chunk, value0, store0)
                when((half == 0) & has_later, halo_mine(j * OWN_GROUP + i).start)
            own1(j, OWN_GROUP).start()

        loop("produce", n // OWN_GROUP, produce)

        def gather(k):
            @pl.when(lax.rem(k, OWN_GROUP) == 0)
            def _():
                own1(lax.div(k, OWN_GROUP), OWN_GROUP).wait_recv()

            far_on(k).wait_recv()
            start = pl.multiple_of(k * chunk, chunk)
            mine_at, other_at = c * rows + start, (1 - c) * rows + start
            for u in range(chunk):
                cur[own_base + other_at + u, tiles:, :] = own_in[start + u]
                cur[far_base + mine_at + u, tiles:, :] = far_in[start + u]
                cur[far_base + other_at + u, tiles:, :] = far_pass[start + u]

            @pl.when(has_earlier)
            def _():
                halo_on(k).wait_recv()
                for u in range(chunk):
                    cur[up_base + mine_at + u, :tiles, :] = halo_in[start + u]
                    cur[up_base + other_at + u, :tiles, :] = halo_pass[start + u]

            blocks(k * chunk, chunk, value1(f_across), store_picked(0))
            far_outer(k, 1, lax.div(k, OUTER_GROUP)).start()

        def stream(j):
            @pl.when(j < n)
            def _():
                far(j).wait_recv()
                far_on(j).start()
                when((half == 1) & has_later, halo_far(j).start)

            @pl.when((j >= HALO_LAG) & (j < n + HALO_LAG) & has_earlier)
            def _():
                halo_mine(j - HALO_LAG).wait_recv()
                halo_on(j - HALO_LAG).start()

            @pl.when(j >= MERGE_LAG)
            def _():
                gather(j - MERGE_LAG)

        loop("stream", n + MERGE_LAG, stream)

        def rest(j):
            for i in range(NEAR_GROUP):
                k = j * NEAR_GROUP + i
                blocks(k * chunk, chunk, value1(f_facing), store_picked(2))
                far_inner(k).start()
                blocks(k * chunk, chunk, value1(f_near), store_picked(1))
                blocks(k * chunk, chunk, value1(f), store_land)
                when((half == 1) & has_later, edge(k).start)
            near_outer(j, NEAR_GROUP).start()

        loop("rest", n // NEAR_GROUP, rest)

        def receive(j):
            @pl.when(j < n)
            def _():
                got_facing(j).wait_recv()
                when((half == 0) & has_later, edge(j).start)

            finish_lagged(j)

        loop("receive", n + EDGE_LAG, receive)

        with phase("drain"):
            own1_all.wait_send()
            far_on_all.wait_send()
            when(has_later, halo_all.wait_send)
            when(has_earlier, halo_on_all.wait_send)
            far_outer_all.wait_send()
            near_outer_all.wait_send()
            far_inner_all.wait_send()
            when(has_later, edge_all.wait_send)

    raw_all = lambda kind, row, target, source_at, target_at, size: remote(
        raw.at[pl.ds(row, rows), pl.ds(source_at, size)], raw.at[pl.ds(row, rows), pl.ds(target_at, size)],
        kind, s_raw.at[0], target,
    )
    raw_all(0, c * rows, partner, *full0).wait_send()
    when((c == 1) & has_later, raw_all(1, rows, later, *tail0).wait_send)
    when((c == 1) & has_earlier, raw_all(2, rows, partner, *kept0).wait_send)


def first_use_order(lower_rows, upper_rows, row_count):
    half = lax.axis_index("freq") // 4
    chip_rows, half_rows = 2 * row_count, 4 * row_count
    select = jnp.where(half == 0, lower_rows[2], upper_rows[2])
    wanted = jnp.where(half == 0, select[3 * chip_rows :], select[:chip_rows])
    wanted = wanted.reshape(2, row_count).T.reshape(-1) & (half_rows - 1)
    tables = jnp.stack([lower_rows[1], upper_rows[1]]).reshape(2, 2, half_rows)
    tables = jnp.where(half == 0, tables[:, 0], tables[:, 1]) & (chip_rows - 1)
    at_half = jnp.arange(half_rows, dtype=jnp.int32)
    at_chip = jnp.arange(chip_rows, dtype=jnp.int32)
    hit = wanted[:, None] == at_half[None, :]
    used = jnp.sum(jnp.where(hit[None], tables[:, None, :], 0), axis=2)
    same = used[:, :, None] == at_chip[None, None, :]
    first = jnp.min(jnp.where(same, at_chip[None, :, None], chip_rows), axis=1)
    key = first * chip_rows + at_chip[None, :]
    rank = jnp.sum((key[:, None, :] < key[:, :, None]).astype(jnp.int32), axis=2)
    place = (rank % 2) * row_count + rank // 2
    holds = place[:, :, None] == at_chip[None, None, :]
    row_at = jnp.sum(jnp.where(holds, at_chip[None, :, None], 0), axis=1)
    return select, jnp.concatenate([row_at, place], axis=0)


def per_device_fused(tm_size, band_state, lower_rows, upper_rows, delays, counts):
    row_count, samples = band_state.shape
    tiles = samples // LANES
    n = row_count // CHUNK_ROWS
    dma = pltpu.SemaphoreType.DMA
    wide = pltpu.VMEM((row_count, tiles, LANES), jnp.float32)
    select, order = first_use_order(lower_rows, upper_rows, row_count)
    return pl.pallas_call(
        functools.partial(kernel, tiles, tm_size),
        out_shape=jax.ShapeDtypeStruct((row_count, samples), jnp.float32),
        in_specs=[pl.BlockSpec(memory_space=pltpu.VMEM)] + [pl.BlockSpec(memory_space=pltpu.SMEM)] * 6,
        out_specs=pl.BlockSpec(memory_space=pltpu.VMEM),
        scratch_shapes=[
            pltpu.VMEM((2 * row_count, 2 * tiles, LANES), jnp.float32),
            wide,
            pltpu.VMEM((4 * row_count, 2 * tiles, LANES), jnp.float32),
            wide, wide, wide, wide, wide,
            pltpu.VMEM((3, row_count, tiles, LANES), jnp.float32),
            pltpu.VMEM((2, row_count, tiles, LANES), jnp.float32),
            wide,
            pltpu.VMEM((row_count, 2 * tiles, LANES), jnp.float32),
            wide,
            dma((12,)),
            dma((3 * CHUNKS_0,)),
            dma((n,)),
            dma((n,)),
            dma((n // OWN_GROUP,)),
            dma((n,)),
            dma((n,)),
            dma((n // OUTER_GROUP,)),
            dma((n // NEAR_GROUP,)),
            dma((n,)),
            dma((n,)),
        ],
        compiler_params=pltpu.CompilerParams(
            collective_id=0, has_side_effects=True, vmem_limit_bytes=36 * 2**20
        ),
    )(band_state, lower_rows, upper_rows, delays, counts, select, order)


def solution(mesh):
    if mesh.shape["freq"] == 2**ITERS:
        body = functools.partial(per_device_fused, mesh.shape["tm"])
    else:
        body = per_device_general
    return jax.shard_map(
        body,
        mesh=mesh,
        in_specs=(P("freq", "tm"), P(), P(), P(), P()),
        out_specs=P("freq", "tm"),
        check_vma=False,
    )
```

```python
import contextlib
import functools

import jax
import jax.numpy as jnp
from jax import lax
from jax.experimental import pallas as pl
from jax.experimental.pallas import tpu as pltpu
from jax.sharding import PartitionSpec as P

DMAX = 2048
ITERS = 3
LANES = 128
SUBLANES = 8
UNROLL = 16
CHUNKS_0 = 4
CHUNK_ROWS = 16
HALO_LAG = 2
MERGE_LAG = 3
OWN_GROUP = 4
OUTER_GROUP = 4
NEAR_GROUP = 2
PLAN_UNROLL = 8
EDGE_LAG = 4


def shifted_2(block, axis, distance):
    devices = range(lax.axis_size(axis))
    route = [(i - distance, i) for i in devices if i - distance in devices]
    return lax.ppermute(block, axis, route)


def delay_columns(extended, shifts, widest):
    row_count = extended.shape[0]
    for bit_index in range(widest.bit_length()):
        stride = 1 << bit_index
        shifted = jnp.concatenate(
            [jnp.zeros((row_count, stride), extended.dtype), extended[:, :-stride]], axis=1
        )
        extended = jnp.where((shifts >> bit_index & 1)[:, None] == 1, shifted, extended)
    return extended


def live_mask(global_rows, counts, width_out, offset, bands_out):
    band_index = global_rows // width_out
    band_counts = counts[offset : offset + bands_out]
    matches = band_index[:, None] == jnp.arange(bands_out, dtype=jnp.int32)[None, :]
    live_count = jnp.sum(jnp.where(matches, band_counts[None, :], 0), axis=1)
    return global_rows % width_out < live_count


def per_device_general(band_state, lower_rows, upper_rows, delays, counts):
    row_count, samples = band_state.shape
    freq_index = lax.axis_index("freq")
    first_row = freq_index * row_count
    global_rows = first_row + jnp.arange(row_count, dtype=jnp.int32)
    current = band_state
    for iteration in range(ITERS):
        width_in = DMAX >> ITERS - iteration
        width_out = 2 * width_in
        bands_out = DMAX // width_out
        offset = 2**ITERS - 2 ** (ITERS - iteration)
        lower_source = lax.dynamic_slice_in_dim(lower_rows[iteration], first_row, row_count)
        upper_source = lax.dynamic_slice_in_dim(upper_rows[iteration], first_row, row_count)
        own_delays = lax.dynamic_slice_in_dim(delays[iteration], first_row, row_count)
        gathered = lax.all_gather(current, "freq", axis=0, tiled=True)
        lower_values = jnp.take(gathered, lower_source, axis=0)
        upper_values = jnp.take(gathered, upper_source, axis=0)
        rim_columns = shifted_2(upper_values[:, samples - width_in :], "tm", 1)
        extended = jnp.concatenate([rim_columns, upper_values], axis=1)
        delayed = delay_columns(extended, own_delays, width_in)[:, width_in:]
        live_rows = live_mask(global_rows, counts, width_out, offset, bands_out)
        current = jnp.where(live_rows[:, None], lower_values + delayed, jnp.zeros_like(delayed))
    return current


MESH = pl.DeviceIdType.MESH


def phase(name):
    return contextlib.nullcontext()


def kernel(
    tiles, tm_size, x_ref, lower, upper, delays, counts,
    out_ref, columns, columns_0, places, plan_v, plan, picks_v, picks, raw, mine, cur, own_in, far_in, far_pass, halo_in, halo_pass,
    picked, land, early, joined, final,
    sent, s_plan, s_raw, s_far, s_far_pass, s_own, s_halo, s_halo_pass, s_fo, s_no, s_fi, s_edge,
):
    f, t = lax.axis_index("freq"), lax.axis_index("tm")
    c, z = lax.rem(f, 2), lax.div(f, 2)
    zb, half = lax.rem(z, 2), lax.div(z, 2)
    rows = x_ref.shape[0]
    chunk = CHUNK_ROWS
    n = rows // chunk
    at = lambda ff, tt: {"freq": ff, "tm": tt}
    partner = at(f + 1 - 2 * c, t)
    near = at(f + 2 - 4 * zb, t)
    across = at(f + 4 - 8 * half, t)
    facing = at(f + 2 - 4 * half, t)
    later = at(f, t + 1)
    earlier = at(f, t - 1)
    inner = zb != half
    outer = zb == half
    has_later, has_earlier = t < tm_size - 1, t > 0

    barrier = pltpu.get_barrier_semaphore()

    def greet(target):
        pl.semaphore_signal(barrier, inc=1, device_id=target, device_id_type=MESH)

    greet(partner)
    greet(near)
    greet(across)
    for cond, target in ((inner, facing), (has_earlier, earlier), (has_later, later)):
        pl.when(cond)(functools.partial(greet, target))

    lane = lax.broadcasted_iota(jnp.int32, (tiles, LANES), 1)
    zero = jnp.zeros((tiles, LANES), jnp.float32)

    def when(cond, action):
        pl.when(cond)(action)

    def remote(src, dst, flow, sem, target):
        return pltpu.make_async_remote_copy(
            src_ref=src, dst_ref=dst, send_sem=sent.at[flow], recv_sem=sem,
            device_id=target, device_id_type=MESH,
        )

    def span(j, group=1):
        return pl.ds(pl.multiple_of(j * chunk * group, chunk * group), chunk * group)

    def delayed(source, row, d, first):
        q, r = d >> 7, d & (LANES - 1)
        a = source[row, pl.ds(tiles - q, tiles), :]
        b = source[row, pl.ds(jnp.maximum(tiles - 1 - q, first), tiles), :]
        a, b = pltpu.roll(a, r, 1), pltpu.roll(b, r, 1)
        return jnp.where(lane >= r, a, b)

    def blocks(start, count, value, store):
        def body(step, carry):
            base = start + step * UNROLL
            values = [(base + u, value(base, u)) for u in range(UNROLL)]
            for m, v in values:
                store(m, v)
            return carry

        if count == UNROLL:
            body(0, 0)
        else:
            lax.fori_loop(0, count // UNROLL, body, 0)

    rim0 = rows // LANES
    n0, chunk0 = CHUNKS_0, rows // CHUNKS_0

    def raw_copy(kind, j, row, target, source_at, target_at, size):
        span0 = pl.ds(row + j * chunk0, chunk0)
        return remote(
            raw.at[span0, pl.ds(source_at, size)], raw.at[span0, pl.ds(target_at, size)],
            kind, s_raw.at[kind * n0 + j], target,
        )

    tail0 = (2 * tiles - rim0, tiles - rim0, rim0)
    kept0 = (tiles - rim0, tiles - rim0, rim0)
    full0 = (tiles, tiles, tiles)
    own0 = lambda j, row: raw_copy(0, j, row, partner, *full0)
    rim_out0 = lambda j: raw_copy(1, j, rows, later, *tail0)
    rim_in0 = lambda j: raw_copy(2, j, rows, partner, *kept0)

    def spread(first, count):
        def body(step, carry):
            r = first + step * SUBLANES
            for tile in range(tiles):
                raw[pl.ds(c * rows + r, SUBLANES), tiles + tile, :] = x_ref[
                    pl.ds(r, SUBLANES), pl.ds(tile * LANES, LANES)
                ]
            return carry

        lax.fori_loop(0, count // SUBLANES, body, 0)

    with phase("spread"):
        spread(0, rows)
    one = lambda cond: jnp.where(cond, 1, 0)
    with phase("greet"):
        pl.semaphore_wait(barrier, 3 + one(inner) + one(has_earlier) + one(has_later))
    with phase("send0"):
        for j in range(n0):
            when((c == 1) & has_later, rim_out0(j).start)
            own0(j, c * rows).start()

    def clear(count, store):
        def body(i, carry):
            for u in range(UNROLL):
                store(i * UNROLL + u)
            return carry

        lax.fori_loop(0, count // UNROLL, body, 0)

    @pl.when(t == 0)
    def _():
        def clear_raw(i):
            raw[rows + i, :tiles, :] = zero

        def clear_cur(i):
            cur[2 * rows + i, :tiles, :] = zero

        def clear_early(i):
            early[i] = zero

        clear(rows, clear_raw)
        clear(2 * rows, clear_cur)
        clear(rows, clear_early)

    chip_rows, half_rows = 2 * rows, 4 * rows
    flat = (SUBLANES, LANES)
    lane_at = lax.broadcasted_iota(jnp.int32, flat, 1)
    line_at = lax.broadcasted_iota(jnp.int32, flat, 0)
    none = jnp.zeros(flat, jnp.int32)
    groups = lambda count: range(count // LANES)

    def row_of(table, level, start):
        return jnp.broadcast_to(table[level : level + 1, pl.ds(pl.multiple_of(start, LANES), LANES)], flat)

    def wanted(start):
        return jnp.where(half == 0, row_of(lower, ITERS - 1, start), row_of(upper, ITERS - 1, start)) & (half_rows - 1)

    def set_columns(target, start, row):
        target[pl.ds(start, LANES), :] = jnp.broadcast_to(row[0:1], (LANES, LANES)).T

    def fold(values, combine):
        for s in (4, 2, 1):
            values = [combine(v, pltpu.roll(v, s, 0)) for v in values]
        return values

    def scan(count, init, step):
        def body(i, carry):
            for u in range(PLAN_UNROLL):
                at_row = (i * PLAN_UNROLL + u) * SUBLANES
                carry = step(pl.multiple_of(at_row, SUBLANES), line_at + at_row, carry)
            return carry

        return lax.fori_loop(0, count // SUBLANES // PLAN_UNROLL, body, init)

    add, least = lambda a, b: a + b, jnp.minimum
    bit = lambda cond, place: jnp.where(cond, 1 << place, 0)

    def find_order():
        for g in groups(half_rows):
            start = half * half_rows + g * LANES
            low, high = row_of(lower, 1, start), row_of(upper, 1, start)
            set_columns(columns, g * LANES, (low & (chip_rows - 1)) | (high & (chip_rows - 1)) << 9)
        want = [wanted((1 - half) * 3 * chip_rows + g * LANES) for g in groups(chip_rows)]

        def use(at_row, index, carry):
            line = columns[pl.ds(at_row, SUBLANES), :]
            return tuple(v + jnp.where(w == index, line, 0) for v, w in zip(carry, want))

        used = fold(scan(half_rows, (none,) * len(want), use), add)
        for g, row in enumerate(used):
            set_columns(columns, g * LANES, row)

        def meet(at_row, index, carry):
            line = columns[pl.ds(at_row, SUBLANES), :]
            low, high = line & (chip_rows - 1), line >> 9
            turn = 2 * (index & (rows - 1)) + lax.div(index, rows)
            hits = [(part, g) for part in (low, high) for g in groups(chip_rows)]
            return tuple(
                least(v, jnp.where(part == lane_at + g * LANES, turn, chip_rows)) for v, (part, g) in zip(carry, hits)
            )

        never = jnp.full(flat, chip_rows, jnp.int32)
        first = fold(scan(chip_rows, (never,) * (2 * len(want)), meet), least)
        keys = [v * chip_rows + lane_at + (g % len(want)) * LANES for g, v in enumerate(first)]
        for g, row in enumerate(keys):
            set_columns(columns, g * LANES, row)

        def count(at_row, index, carry):
            low = columns[pl.ds(at_row, SUBLANES), :]
            high = columns[pl.ds(chip_rows + at_row, SUBLANES), :]
            parts = [low] * len(want) + [high] * len(want)
            return tuple(v + jnp.where(part < key, 1, 0) for v, part, key in zip(carry, parts, keys))

        ranks = fold(scan(chip_rows, (none,) * len(keys), count), add)
        place = [(v & 1) * rows + (v >> 1) for v in ranks]
        for g in groups(chip_rows):
            low, high = place[g], place[len(want) + g]
            set_columns(places, g * LANES, low | high << 9)
            start = z * chip_rows + g * LANES
            low, high = row_of(lower, 0, start), row_of(upper, 0, start)
            live = bit(lane_at + g * LANES < counts[z], 28)
            word = (low & (chip_rows - 1)) | (high & (chip_rows - 1)) << 9 | row_of(delays, 0, start) << 18 | live
            set_columns(columns_0, g * LANES, word)

        def pick(at_row, index, carry):
            line = places[pl.ds(at_row, SUBLANES), :]
            own = jnp.where(zb == 0, line & (chip_rows - 1), line >> 9)
            word = columns_0[pl.ds(at_row, SUBLANES), :]
            return tuple(
                v + jnp.where(own == lane_at + (c * rows + g * LANES), word, 0) for g, v in enumerate(carry)
            )

        words = fold(scan(chip_rows, (none,) * len(groups(rows)), pick), add)
        for g, row in enumerate(words):
            plan_v[pl.ds(g, 1), :] = row[0:1]
            start = f * rows + g * LANES
            live = bit(lane_at + start < counts[2**ITERS - 2], 12)
            plan_v[pl.ds(rows // LANES + g, 1), :] = (row_of(delays, 2, start) | live)[0:1]
        pltpu.make_async_copy(plan_v, plan, s_plan.at[0]).start()

    def place_rows():
        marks = [half * half_rows + g * LANES for g in groups(half_rows)]
        low = [row_of(lower, 1, start) & (chip_rows - 1) for start in marks]
        high = [row_of(upper, 1, start) & (chip_rows - 1) for start in marks]

        def put(at_row, index, carry):
            line = places[pl.ds(at_row, SUBLANES), :]
            shifted = line >> 9 << 9
            line = line & (chip_rows - 1)
            return tuple(
                v + jnp.where(a == index, line, 0) + jnp.where(b == index, shifted, 0)
                for v, a, b in zip(carry, low, high)
            )

        words = fold(scan(chip_rows, (none,) * len(marks), put), add)
        for g, (start, word) in enumerate(zip(marks, words)):
            live = bit(lane_at + g * LANES < counts[2 ** (ITERS - 1) + half], 28)
            set_columns(columns, g * LANES, word | row_of(delays, 1, start) << 18 | live)

    def pick_rows():
        targets = (f + 4 - 8 * half, f + 2 - 4 * zb, f + 2 - 4 * half, f)
        want = [wanted(target * rows + g * LANES) for target in targets for g in groups(rows)]

        def pick(at_row, index, carry):
            line = columns[pl.ds(at_row, SUBLANES), :]
            return tuple(v + jnp.where(w == index, line, 0) for v, w in zip(carry, want))

        words = fold(scan(half_rows, (none,) * len(want), pick), add)
        for g, row in enumerate(words):
            picks_v[pl.ds(g, 1), :] = row[0:1]
        pltpu.make_async_copy(picks_v, picks, s_plan.at[1]).start()

    with phase("order"):
        find_order()

    for j in range(n0):

        @pl.when((c == 1) & has_earlier)
        def _():
            with phase("rim_out"):
                rim_out0(j).wait_recv()
                rim_in0(j).start()

    for j in range(n0):
        with phase("own0"):
            own0(j, (1 - c) * rows).wait_recv()
        with phase("rim_in"):
            when((c == 0) & has_earlier, rim_in0(j).wait_recv)

    pltpu.make_async_copy(plan_v, plan, s_plan.at[0]).wait()
    own_base, far_base = zb * 2 * rows, (1 - zb) * 2 * rows
    up_base = 2 * rows
    def entry(table, first, base, u):
        return table[first + (base >> 7), (base & (LANES - 1)) + u]

    def value0(base, u):
        word = entry(plan, 0, base, u)
        lo, up, d = word & 511, (word >> 9) & 511, (word >> 18) & 1023
        total = raw[lo, tiles:, :] + delayed(raw, up, d, tiles - rim0)
        return jnp.where((word >> 28) == 1, total, zero)

    def store0(m, v):
        mine[m] = v
        cur[own_base + c * rows + m, tiles:, :] = v

    rim1 = 2 * rows // LANES

    def value1(kind):
        def value(base, u):
            word = entry(picks, kind * (rows // LANES), base, u)
            a, b, d = word & 511, (word >> 9) & 511, (word >> 18) & 1023
            total = cur[a, tiles:, :] + delayed(cur, up_base + b, d, tiles - rim1)
            return jnp.where((word >> 28) == 1, total, zero)

        return value

    def store_picked(kind):
        def store(m, v):
            picked[kind, m] = v

        return store

    def store_land(m, v):
        land[half, m] = v

    def join(m):
        joined[m, :tiles, :] = early[m]
        joined[m, tiles:, :] = land[1, m]

    def value2(base, u):
        word = entry(plan, rows // LANES, base, u)
        total = land[0, base + u] + delayed(joined, base + u, word & 4095, 0)
        return jnp.where((word >> 12) == 1, total, zero)

    def store2(m, v):
        final[m] = v

    def finish(k):
        start = pl.multiple_of(k * chunk, chunk)
        for u in range(chunk):
            join(start + u)
        blocks(start, chunk, value2, store2)
        for step in range(chunk // SUBLANES):
            r = pl.multiple_of(start + step * SUBLANES, SUBLANES)
            for tile in range(tiles):
                out_ref[pl.ds(r, SUBLANES), pl.ds(tile * LANES, LANES)] = final[pl.ds(r, SUBLANES), tile, :]

    rim = pl.ds(tiles - rim1, rim1)
    every = pl.ds(0, rows)

    def flow(index, src, dst, sems, target):
        def copy(j, group=1, sem=None):
            at_rows = span(j, group)
            return remote(src(at_rows), dst(at_rows), index, sems.at[j if sem is None else sem], target)

        return copy, remote(src(every), dst(every), index, sems.at[0], target)

    far, far_all = flow(3, lambda r: mine.at[r], lambda r: far_in.at[r], s_far, near)
    far_on, far_on_all = flow(4, lambda r: far_in.at[r], lambda r: far_pass.at[r], s_far_pass, partner)
    own1, own1_all = flow(5, lambda r: mine.at[r], lambda r: own_in.at[r], s_own, partner)
    halo_mine, halo_all = flow(6, lambda r: mine.at[r, rim], lambda r: halo_in.at[r, rim], s_halo, later)
    halo_far, _ = flow(6, lambda r: far_in.at[r, rim], lambda r: halo_in.at[r, rim], s_halo, later)
    halo_on, halo_on_all = flow(7, lambda r: halo_in.at[r, rim], lambda r: halo_pass.at[r, rim], s_halo_pass, partner)
    to_half = lambda h: lambda r: land.at[h, r]
    far_outer, far_outer_all = flow(8, lambda r: picked.at[0, r], to_half(half), s_fo, across)
    near_outer, near_outer_all = flow(9, lambda r: picked.at[1, r], to_half(half), s_no, near)
    far_inner, far_inner_all = flow(10, lambda r: picked.at[2, r], to_half(half), s_fi, facing)
    got_across, _ = flow(8, lambda r: picked.at[0, r], to_half(1 - half), s_fo, across)
    got_facing, _ = flow(10, lambda r: picked.at[2, r], to_half(1 - half), s_fi, facing)
    edge, edge_all = flow(11, lambda r: land.at[1, r], lambda r: early.at[r], s_edge, later)

    def loop(name, count, body):
        def step(j, carry):
            with phase(name):
                body(j)
            return carry

        lax.fori_loop(0, count, step, 0)

    def finish_lagged(j):
        @pl.when(j >= EDGE_LAG)
        def _():
            k = j - EDGE_LAG
            when(has_earlier, edge(k).wait_recv)
            finish(k)

    @pl.when(outer)
    def _():
        def produce(j):
            blocks(j * chunk, chunk, value0, store0)
            far(j).start()

        loop("produce", n, produce)

        def from_across(j):
            got_across(j, OUTER_GROUP).wait_recv()
            for i in range(OUTER_GROUP):
                when((half == 0) & has_later, edge(j * OUTER_GROUP + i).start)

        loop("from_across", n // OUTER_GROUP, from_across)

        def from_near(j):
            @pl.when(j < n)
            def _():
                @pl.when(lax.rem(j, NEAR_GROUP) == 0)
                def _():
                    near_outer(lax.div(j, NEAR_GROUP), NEAR_GROUP).wait_recv()

                when((half == 1) & has_later, edge(j).start)

            finish_lagged(j)

        loop("from_near", n + EDGE_LAG, from_near)

        with phase("drain"):
            far_all.wait_send()
            when(has_later, edge_all.wait_send)

    @pl.when(inner)
    def _():
        def produce(j):
            for i in range(OWN_GROUP):
                blocks((j * OWN_GROUP + i) * chunk, chunk, value0, store0)
                when((half == 0) & has_later, halo_mine(j * OWN_GROUP + i).start)
            own1(j, OWN_GROUP).start()

        loop("produce", n // OWN_GROUP, produce)

        def gather(k):
            @pl.when(lax.rem(k, OWN_GROUP) == 0)
            def _():
                own1(lax.div(k, OWN_GROUP), OWN_GROUP).wait_recv()

            far_on(k).wait_recv()
            start = pl.multiple_of(k * chunk, chunk)
            mine_at, other_at = c * rows + start, (1 - c) * rows + start
            for u in range(chunk):
                cur[own_base + other_at + u, tiles:, :] = own_in[start + u]
                cur[far_base + mine_at + u, tiles:, :] = far_in[start + u]
                cur[far_base + other_at + u, tiles:, :] = far_pass[start + u]

            @pl.when(has_earlier)
            def _():
                halo_on(k).wait_recv()
                for u in range(chunk):
                    cur[up_base + mine_at + u, :tiles, :] = halo_in[start + u]
                    cur[up_base + other_at + u, :tiles, :] = halo_pass[start + u]

            blocks(k * chunk, chunk, value1(0), store_picked(0))
            far_outer(k, 1, lax.div(k, OUTER_GROUP)).start()

        def stream(j):
            @pl.when(j < n)
            def _():
                far(j).wait_recv()
                far_on(j).start()
                when((half == 1) & has_later, halo_far(j).start)

            pl.when(j == 0)(place_rows)
            pl.when(j == 1)(pick_rows)

            @pl.when((j >= HALO_LAG) & (j < n + HALO_LAG) & has_earlier)
            def _():
                halo_mine(j - HALO_LAG).wait_recv()
                halo_on(j - HALO_LAG).start()

            when(j == MERGE_LAG, pltpu.make_async_copy(picks_v, picks, s_plan.at[1]).wait)

            @pl.when(j >= MERGE_LAG)
            def _():
                gather(j - MERGE_LAG)

        loop("stream", n + MERGE_LAG, stream)

        def rest(j):
            for i in range(NEAR_GROUP):
                k = j * NEAR_GROUP + i
                blocks(k * chunk, chunk, value1(2), store_picked(2))
                far_inner(k).start()
                blocks(k * chunk, chunk, value1(1), store_picked(1))
                blocks(k * chunk, chunk, value1(3), store_land)
                when((half == 1) & has_later, edge(k).start)
            near_outer(j, NEAR_GROUP).start()

        loop("rest", n // NEAR_GROUP, rest)

        def receive(j):
            @pl.when(j < n)
            def _():
                got_facing(j).wait_recv()
                when((half == 0) & has_later, edge(j).start)

            finish_lagged(j)

        loop("receive", n + EDGE_LAG, receive)

        with phase("drain"):
            own1_all.wait_send()
            far_on_all.wait_send()
            when(has_later, halo_all.wait_send)
            when(has_earlier, halo_on_all.wait_send)
            far_outer_all.wait_send()
            near_outer_all.wait_send()
            far_inner_all.wait_send()
            when(has_later, edge_all.wait_send)

    raw_all = lambda kind, row, target, source_at, target_at, size: remote(
        raw.at[pl.ds(row, rows), pl.ds(source_at, size)], raw.at[pl.ds(row, rows), pl.ds(target_at, size)],
        kind, s_raw.at[0], target,
    )
    raw_all(0, c * rows, partner, *full0).wait_send()
    when((c == 1) & has_later, raw_all(1, rows, later, *tail0).wait_send)
    when((c == 1) & has_earlier, raw_all(2, rows, partner, *kept0).wait_send)


def per_device_fused(tm_size, band_state, lower_rows, upper_rows, delays, counts):
    row_count, samples = band_state.shape
    tiles = samples // LANES
    n = row_count // CHUNK_ROWS
    dma = pltpu.SemaphoreType.DMA
    wide = pltpu.VMEM((row_count, tiles, LANES), jnp.float32)
    return pl.pallas_call(
        functools.partial(kernel, tiles, tm_size),
        out_shape=jax.ShapeDtypeStruct((row_count, samples), jnp.float32),
        in_specs=[pl.BlockSpec(memory_space=pltpu.VMEM)] * 4 + [pl.BlockSpec(memory_space=pltpu.SMEM)],
        out_specs=pl.BlockSpec(memory_space=pltpu.VMEM),
        scratch_shapes=[
            pltpu.VMEM((4 * row_count, LANES), jnp.int32),
            pltpu.VMEM((2 * row_count, LANES), jnp.int32),
            pltpu.VMEM((2 * row_count, LANES), jnp.int32),
            pltpu.VMEM((2 * row_count // LANES, LANES), jnp.int32),
            pltpu.SMEM((2 * row_count // LANES, LANES), jnp.int32),
            pltpu.VMEM((4 * row_count // LANES, LANES), jnp.int32),
            pltpu.SMEM((4 * row_count // LANES, LANES), jnp.int32),
            pltpu.VMEM((2 * row_count, 2 * tiles, LANES), jnp.float32),
            wide,
            pltpu.VMEM((4 * row_count, 2 * tiles, LANES), jnp.float32),
            wide, wide, wide, wide, wide,
            pltpu.VMEM((3, row_count, tiles, LANES), jnp.float32),
            pltpu.VMEM((2, row_count, tiles, LANES), jnp.float32),
            wide,
            pltpu.VMEM((row_count, 2 * tiles, LANES), jnp.float32),
            wide,
            dma((12,)),
            dma((2,)),
            dma((3 * CHUNKS_0,)),
            dma((n,)),
            dma((n,)),
            dma((n // OWN_GROUP,)),
            dma((n,)),
            dma((n,)),
            dma((n // OUTER_GROUP,)),
            dma((n // NEAR_GROUP,)),
            dma((n,)),
            dma((n,)),
        ],
        compiler_params=pltpu.CompilerParams(
            collective_id=0, has_side_effects=True, vmem_limit_bytes=36 * 2**20
        ),
    )(band_state, lower_rows, upper_rows, delays, counts)


def solution(mesh):
    if mesh.shape["freq"] == 2**ITERS:
        body = functools.partial(per_device_fused, mesh.shape["tm"])
    else:
        body = per_device_general
    return jax.shard_map(
        body,
        mesh=mesh,
        in_specs=(P("freq", "tm"), P(), P(), P(), P()),
        out_specs=P("freq", "tm"),
        check_vma=False,
    )
```

```python
import contextlib
import functools

import jax
import jax.numpy as jnp
from jax import lax
from jax.experimental import pallas as pl
from jax.experimental.pallas import tpu as pltpu
from jax.sharding import PartitionSpec as P

DMAX = 2048
ITERS = 3
LANES = 128
SUBLANES = 8
UNROLL = 16
CHUNKS_0 = 4
CHUNK_ROWS = 16
HEAD = 4
HALO_LAG = 2
OWN_GROUP = 2
PLAN_UNROLL = 8
EDGE_LAG = 3
REST_FIRST = 20
REST_STEP = 3
OWN_LEAD = 2
COARSE = 64
FINE = 8


def shifted_2(block, axis, distance):
    devices = range(lax.axis_size(axis))
    route = [(i - distance, i) for i in devices if i - distance in devices]
    return lax.ppermute(block, axis, route)


def delay_columns(extended, shifts, widest):
    row_count = extended.shape[0]
    for bit_index in range(widest.bit_length()):
        stride = 1 << bit_index
        shifted = jnp.concatenate(
            [jnp.zeros((row_count, stride), extended.dtype), extended[:, :-stride]], axis=1
        )
        extended = jnp.where((shifts >> bit_index & 1)[:, None] == 1, shifted, extended)
    return extended


def live_mask(global_rows, counts, width_out, offset, bands_out):
    band_index = global_rows // width_out
    band_counts = counts[offset : offset + bands_out]
    matches = band_index[:, None] == jnp.arange(bands_out, dtype=jnp.int32)[None, :]
    live_count = jnp.sum(jnp.where(matches, band_counts[None, :], 0), axis=1)
    return global_rows % width_out < live_count


def per_device_general(band_state, lower_rows, upper_rows, delays, counts):
    row_count, samples = band_state.shape
    freq_index = lax.axis_index("freq")
    first_row = freq_index * row_count
    global_rows = first_row + jnp.arange(row_count, dtype=jnp.int32)
    current = band_state
    for iteration in range(ITERS):
        width_in = DMAX >> ITERS - iteration
        width_out = 2 * width_in
        bands_out = DMAX // width_out
        offset = 2**ITERS - 2 ** (ITERS - iteration)
        lower_source = lax.dynamic_slice_in_dim(lower_rows[iteration], first_row, row_count)
        upper_source = lax.dynamic_slice_in_dim(upper_rows[iteration], first_row, row_count)
        own_delays = lax.dynamic_slice_in_dim(delays[iteration], first_row, row_count)
        gathered = lax.all_gather(current, "freq", axis=0, tiled=True)
        lower_values = jnp.take(gathered, lower_source, axis=0)
        upper_values = jnp.take(gathered, upper_source, axis=0)
        rim_columns = shifted_2(upper_values[:, samples - width_in :], "tm", 1)
        extended = jnp.concatenate([rim_columns, upper_values], axis=1)
        delayed = delay_columns(extended, own_delays, width_in)[:, width_in:]
        live_rows = live_mask(global_rows, counts, width_out, offset, bands_out)
        current = jnp.where(live_rows[:, None], lower_values + delayed, jnp.zeros_like(delayed))
    return current


MESH = pl.DeviceIdType.MESH


def phase(name):
    return contextlib.nullcontext()


def kernel(
    tiles, tm_size, x_in, lower_in, upper_in, delays_in, counts_in,
    out_ref, x_ref, lower, upper, delays, counts, columns, columns_0, places, plan_v, plan, picks_v, picks, raw, rim_in, mine, cur, own_in, far_in, far_pass, halo_in, halo_pass,
    picked, land, early, joined, final,
    sent, s_load, s_plan, s_raw, s_head, s_far, s_far_pass, s_own, s_halo, s_halo_pass, s_fo, s_last, s_edge,
):
    f, t = lax.axis_index("freq"), lax.axis_index("tm")
    c, z = lax.rem(f, 2), lax.div(f, 2)
    zb, half = lax.rem(z, 2), lax.div(z, 2)
    rows = x_ref.shape[0]
    chunk = CHUNK_ROWS
    n = rows // chunk
    at = lambda ff, tt: {"freq": ff, "tm": tt}
    partner = at(f + 1 - 2 * c, t)
    near = at(f + 2 - 4 * zb, t)
    across = at(f + 4 - 8 * half, t)
    facing = at(f + 2 - 4 * half, t)
    later = at(f, t + 1)
    earlier = at(f, t - 1)
    inner = zb != half
    outer = zb == half
    has_later, has_earlier = t < tm_size - 1, t > 0

    n0, chunk0 = CHUNKS_0, rows // CHUNKS_0

    def load(j, source, target):
        return pltpu.make_async_copy(source, target, s_load.at[j])

    parts = [pl.ds(j * chunk0, chunk0) for j in range(n0)]
    loads = [load(j, x_in.at[part], x_ref.at[part]) for j, part in enumerate(parts)]
    pairs = ((lower_in, lower), (upper_in, upper), (delays_in, delays), (counts_in, counts))
    table_loads = [load(n0 + j, *pair) for j, pair in enumerate(pairs)]
    for copy in loads + table_loads:
        copy.start()

    barrier = pltpu.get_barrier_semaphore()

    def greet(target):
        pl.semaphore_signal(barrier, inc=1, device_id=target, device_id_type=MESH)

    greet(partner)
    greet(near)
    greet(across)
    for cond, target in ((inner, facing), (has_earlier, earlier), (has_later, later)):
        pl.when(cond)(functools.partial(greet, target))

    lane = lax.broadcasted_iota(jnp.int32, (tiles, LANES), 1)
    zero = jnp.zeros((tiles, LANES), jnp.float32)

    def when(cond, action):
        pl.when(cond)(action)

    def remote(src, dst, flow, sem, target):
        return pltpu.make_async_remote_copy(
            src_ref=src, dst_ref=dst, send_sem=sent.at[flow], recv_sem=sem,
            device_id=target, device_id_type=MESH,
        )

    def span(j, group=1):
        return pl.ds(pl.multiple_of(j * chunk * group, chunk * group), chunk * group)

    n_fine = rows // FINE

    def coarse(j):
        return pl.ds(pl.multiple_of(j * COARSE, COARSE), COARSE)

    def fine(j):
        return pl.ds(pl.multiple_of(j * FINE, FINE), FINE)

    def delayed(source, row, d, first):
        q, r = d >> 7, d & (LANES - 1)
        a = source[row, pl.ds(tiles - q, tiles), :]
        b = source[row, pl.ds(jnp.maximum(tiles - 1 - q, first), tiles), :]
        a, b = pltpu.roll(a, r, 1), pltpu.roll(b, r, 1)
        return jnp.where(lane >= r, a, b)

    def blocks(start, count, value, store):
        def body(base, size):
            values = [(base + u, value(base, u)) for u in range(size)]
            for m, v in values:
                store(m, v)

        def step(i, carry):
            body(start + i * UNROLL, UNROLL)
            return carry

        if count <= UNROLL:
            body(start, count)
        else:
            lax.fori_loop(0, count // UNROLL, step, 0)

    rim0 = rows // LANES
    full0, tail0, kept0 = pl.ds(tiles, tiles), pl.ds(2 * tiles - rim0, rim0), pl.ds(tiles - rim0, rim0)

    def part_of(j, row=0):
        return pl.ds(row, rows) if j is None else pl.ds(row + j * chunk0, chunk0)

    def own0(j, row):
        at_rows = raw.at[part_of(j, row), full0]
        return remote(at_rows, at_rows, 0, s_raw.at[j or 0], partner)

    def rim_out0(j):
        return remote(raw.at[part_of(j, rows), tail0], rim_in.at[part_of(j), kept0], 1, s_raw.at[n0 + (j or 0)], later)

    def rim_in0(j):
        at_rows = rim_in.at[part_of(j), kept0]
        return remote(at_rows, at_rows, 2, s_raw.at[2 * n0 + (j or 0)], partner)

    def spread(first, count):
        def body(step, carry):
            r = first + step * SUBLANES
            for tile in range(tiles):
                raw[pl.ds(c * rows + r, SUBLANES), tiles + tile, :] = x_ref[
                    pl.ds(r, SUBLANES), pl.ds(tile * LANES, LANES)
                ]
            return carry

        lax.fori_loop(0, count // SUBLANES, body, 0)

    for j in range(n0):
        with phase("spread"):
            loads[j].wait()
            spread(j * chunk0, chunk0)
    one = lambda cond: jnp.where(cond, 1, 0)
    with phase("greet"):
        pl.semaphore_wait(barrier, 3 + one(inner) + one(has_earlier) + one(has_later))
    with phase("send0"):
        for j in range(n0):
            when((c == 1) & has_later, rim_out0(j).start)
            own0(j, c * rows).start()

    def clear(count, store):
        def body(i, carry):
            for u in range(UNROLL):
                store(i * UNROLL + u)
            return carry

        lax.fori_loop(0, count // UNROLL, body, 0)

    @pl.when(t == 0)
    def _():
        def clear_raw(i):
            raw[rows + i, :tiles, :] = zero

        def clear_cur(i):
            cur[2 * rows + i, :tiles, :] = zero

        def clear_early(i):
            early[i] = zero

        clear(rows, clear_raw)
        clear(2 * rows, clear_cur)
        clear(rows, clear_early)

    chip_rows, half_rows = 2 * rows, 4 * rows
    flat = (SUBLANES, LANES)
    lane_at = lax.broadcasted_iota(jnp.int32, flat, 1)
    line_at = lax.broadcasted_iota(jnp.int32, flat, 0)
    none = jnp.zeros(flat, jnp.int32)
    groups = lambda count: range(count // LANES)

    def row_of(table, level, start):
        return jnp.broadcast_to(table[level : level + 1, pl.ds(pl.multiple_of(start, LANES), LANES)], flat)

    def wanted(start):
        return jnp.where(half == 0, row_of(lower, ITERS - 1, start), row_of(upper, ITERS - 1, start)) & (half_rows - 1)

    def set_columns(target, start, row):
        target[pl.ds(start, LANES), :] = jnp.broadcast_to(row[0:1], (LANES, LANES)).T

    def fold(values, combine):
        for s in (4, 2, 1):
            values = [combine(v, pltpu.roll(v, s, 0)) for v in values]
        return values

    def scan(count, init, step):
        def body(i, carry):
            for u in range(PLAN_UNROLL):
                at_row = (i * PLAN_UNROLL + u) * SUBLANES
                carry = step(pl.multiple_of(at_row, SUBLANES), line_at + at_row, carry)
            return carry

        return lax.fori_loop(0, count // SUBLANES // PLAN_UNROLL, body, init)

    add, least = lambda a, b: a + b, jnp.minimum
    bit = lambda cond, place: jnp.where(cond, 1 << place, 0)

    def find_order():
        for g in groups(half_rows):
            start = half * half_rows + g * LANES
            low, high = row_of(lower, 1, start), row_of(upper, 1, start)
            set_columns(columns, g * LANES, (low & (chip_rows - 1)) | (high & (chip_rows - 1)) << 9)
        want = [wanted((1 - half) * 3 * chip_rows + g * LANES) for g in groups(chip_rows)]

        def use(at_row, index, carry):
            line = columns[pl.ds(at_row, SUBLANES), :]
            return tuple(v + jnp.where(w == index, line, 0) for v, w in zip(carry, want))

        used = fold(scan(half_rows, (none,) * len(want), use), add)
        for g, row in enumerate(used):
            set_columns(columns, g * LANES, row)

        def meet(at_row, index, carry):
            line = columns[pl.ds(at_row, SUBLANES), :]
            low, high = line & (chip_rows - 1), line >> 9
            turn = 2 * (index & (rows - 1)) + lax.div(index, rows)
            hits = [(part, g) for part in (low, high) for g in groups(chip_rows)]
            return tuple(
                least(v, jnp.where(part == lane_at + g * LANES, turn, chip_rows)) for v, (part, g) in zip(carry, hits)
            )

        never = jnp.full(flat, chip_rows, jnp.int32)
        first = fold(scan(chip_rows, (never,) * (2 * len(want)), meet), least)
        keys = [v * chip_rows + lane_at + (g % len(want)) * LANES for g, v in enumerate(first)]
        for g, row in enumerate(keys):
            set_columns(columns, g * LANES, row)

        def count(at_row, index, carry):
            low = columns[pl.ds(at_row, SUBLANES), :]
            high = columns[pl.ds(chip_rows + at_row, SUBLANES), :]
            parts = [low] * len(want) + [high] * len(want)
            return tuple(v + jnp.where(part < key, 1, 0) for v, part, key in zip(carry, parts, keys))

        ranks = fold(scan(chip_rows, (none,) * len(keys), count), add)
        place = [(v & 1) * rows + (v >> 1) for v in ranks]
        for g in groups(chip_rows):
            low, high = place[g], place[len(want) + g]
            set_columns(places, g * LANES, low | high << 9)
            start = z * chip_rows + g * LANES
            low, high = row_of(lower, 0, start), row_of(upper, 0, start)
            live = bit(lane_at + g * LANES < counts[z], 28)
            word = (low & (chip_rows - 1)) | (high & (chip_rows - 1)) << 9 | row_of(delays, 0, start) << 18 | live
            set_columns(columns_0, g * LANES, word)

        def pick(at_row, index, carry):
            line = places[pl.ds(at_row, SUBLANES), :]
            own = jnp.where(zb == 0, line & (chip_rows - 1), line >> 9)
            word = columns_0[pl.ds(at_row, SUBLANES), :]
            return tuple(
                v + jnp.where(own == lane_at + (c * rows + g * LANES), word, 0) for g, v in enumerate(carry)
            )

        words = fold(scan(chip_rows, (none,) * len(groups(rows)), pick), add)
        for g, row in enumerate(words):
            plan_v[pl.ds(g, 1), :] = row[0:1]
            start = f * rows + g * LANES
            live = bit(lane_at + start < counts[2**ITERS - 2], 12)
            plan_v[pl.ds(rows // LANES + g, 1), :] = (row_of(delays, 2, start) | live)[0:1]
        pltpu.make_async_copy(plan_v, plan, s_plan.at[0]).start()

    def place_rows():
        marks = [half * half_rows + g * LANES for g in groups(half_rows)]
        low = [row_of(lower, 1, start) & (chip_rows - 1) for start in marks]
        high = [row_of(upper, 1, start) & (chip_rows - 1) for start in marks]

        def put(at_row, index, carry):
            line = places[pl.ds(at_row, SUBLANES), :]
            shifted = line >> 9 << 9
            line = line & (chip_rows - 1)
            return tuple(
                v + jnp.where(a == index, line, 0) + jnp.where(b == index, shifted, 0)
                for v, a, b in zip(carry, low, high)
            )

        words = fold(scan(chip_rows, (none,) * len(marks), put), add)
        for g, (start, word) in enumerate(zip(marks, words)):
            live = bit(lane_at + g * LANES < counts[2 ** (ITERS - 1) + half], 28)
            set_columns(columns, g * LANES, word | row_of(delays, 1, start) << 18 | live)

    def pick_rows():
        targets = (f + 4 - 8 * half, f + 2 - 4 * zb, f + 2 - 4 * half, f)
        want = [wanted(target * rows + g * LANES) for target in targets for g in groups(rows)]

        def pick(at_row, index, carry):
            line = columns[pl.ds(at_row, SUBLANES), :]
            return tuple(v + jnp.where(w == index, line, 0) for v, w in zip(carry, want))

        words = fold(scan(half_rows, (none,) * len(want), pick), add)
        for g, row in enumerate(words):
            picks_v[pl.ds(g, 1), :] = row[0:1]
        pltpu.make_async_copy(picks_v, picks, s_plan.at[1]).start()

    with phase("order"):
        for copy in table_loads:
            copy.wait()
        find_order()

    def take_rim():
        for j in range(n0):

            @pl.when((c == 1) & has_earlier)
            def _():
                with phase("rim_out"):
                    rim_out0(j).wait_recv()
                    rim_in0(j).start()

        for j in range(n0):
            with phase("rim_in"):
                when((c == 0) & has_earlier, rim_in0(j).wait_recv)

        @pl.when(has_earlier)
        def _():
            def fill(i):
                raw[rows + i, :tiles, :] = rim_in[i]

            clear(rows, fill)

    own_base, far_base = zb * 2 * rows, (1 - zb) * 2 * rows
    up_base = 2 * rows
    def entry(table, first, base, u):
        return table[first + (base >> 7), (base & (LANES - 1)) + u]

    def value0(base, u):
        word = entry(plan, 0, base, u)
        lo, up, d = word & 511, (word >> 9) & 511, (word >> 18) & 1023
        total = raw[lo, tiles:, :] + delayed(raw, up, d, tiles - rim0)
        return jnp.where((word >> 28) == 1, total, zero)

    split = tiles // 2

    def store0(m, v):
        mine[m] = v
        cur[own_base + c * rows + m, tiles:, :] = v

    def store_mine(m, v):
        mine[m] = v

    def store_head(m, v):
        mine[m, split:, :] = v[split:, :]

    def store_tail(m, v):
        mine[m, :split, :] = v[:split, :]

    rim1 = 2 * rows // LANES

    def value1(kind):
        def value(base, u):
            word = entry(picks, kind * (rows // LANES), base, u)
            a, b, d = word & 511, (word >> 9) & 511, (word >> 18) & 1023
            total = cur[a, tiles:, :] + delayed(cur, up_base + b, d, tiles - rim1)
            return jnp.where((word >> 28) == 1, total, zero)

        return value

    def store_picked(kind):
        def store(m, v):
            picked[kind, m] = v

        return store

    def store_land(m, v):
        land[half, m] = v

    def join(m):
        joined[m, :tiles, :] = early[m]
        joined[m, tiles:, :] = land[1, m]

    def value2(base, u):
        word = entry(plan, rows // LANES, base, u)
        total = land[0, base + u] + delayed(joined, base + u, word & 4095, 0)
        return jnp.where((word >> 12) == 1, total, zero)

    def store2(m, v):
        final[m] = v

    def finish(first, count):
        def step(i, carry):
            start = pl.multiple_of(first + i * FINE, FINE)
            for u in range(FINE):
                join(start + u)
            blocks(start, FINE, value2, store2)
            for tile in range(tiles):
                at_tile = pl.ds(tile * LANES, LANES)
                out_ref[pl.ds(start, FINE), at_tile] = final[pl.ds(start, FINE), tile, :]
            return carry

        lax.fori_loop(0, count // FINE, step, 0)

    rim = pl.ds(tiles - rim1, rim1)
    every = pl.ds(0, rows)

    def flow(index, src, dst, sems, target):
        def copy(j, group=1):
            at_rows = span(j, group)
            return remote(src(at_rows), dst(at_rows), index, sems.at[j], target)

        copy.coarse = lambda j: remote(src(coarse(j)), dst(coarse(j)), index, sems.at[j], target)
        copy.fine = lambda j: remote(src(fine(j)), dst(fine(j)), index, sems.at[lax.div(j, n_fine // sems.shape[0])], target)

        return copy, remote(src(every), dst(every), index, sems.at[0], target)

    lead, trail = pl.ds(split, tiles - split), pl.ds(0, split)
    head, head_all = flow(3, lambda r: mine.at[r, lead], lambda r: far_in.at[r, lead], s_head, near)
    far, far_all = flow(12, lambda r: mine.at[r, trail], lambda r: far_in.at[r, trail], s_far, near)
    far_on, far_on_all = flow(4, lambda r: far_in.at[r], lambda r: far_pass.at[r], s_far_pass, partner)
    own1, own1_all = flow(5, lambda r: mine.at[r], lambda r: own_in.at[r], s_own, partner)
    halo_mine, halo_all = flow(6, lambda r: mine.at[r, rim], lambda r: halo_in.at[r, rim], s_halo, later)
    halo_far, _ = flow(6, lambda r: far_in.at[r, rim], lambda r: halo_in.at[r, rim], s_halo, later)
    halo_on, halo_on_all = flow(7, lambda r: halo_in.at[r, rim], lambda r: halo_pass.at[r, rim], s_halo_pass, partner)
    to_half = lambda h: lambda r: land.at[h, r]
    _, far_outer_all = flow(8, lambda r: picked.at[0, r], to_half(half), s_fo, across)
    far_outer = lambda j: remote(
        picked.at[0, span(j)], land.at[half, span(j)], 8, s_fo.at[lax.div(j * chunk, COARSE)], across
    )
    near_outer, near_outer_all = flow(9, lambda r: picked.at[1, r], to_half(half), s_last, near)
    far_inner, far_inner_all = flow(10, lambda r: picked.at[2, r], to_half(half), s_last, facing)
    got_across, _ = flow(8, lambda r: picked.at[0, r], to_half(1 - half), s_fo, across)
    got_facing, _ = flow(10, lambda r: picked.at[2, r], to_half(1 - half), s_last, facing)
    edge, edge_all = flow(11, lambda r: land.at[1, r], lambda r: early.at[r], s_edge, later)

    def loop(name, count, body):
        def step(j, carry):
            with phase(name):
                body(j)
            return carry

        lax.fori_loop(0, count, step, 0)

    last_rows = zb == 1
    pieces = chunk // FINE
    taken = (n_fine - 1 - REST_FIRST) // REST_STEP + 1

    def take(j):
        when(inner, got_facing.fine(j).wait_recv)
        when(outer, near_outer.fine(j).wait_recv)
        when(last_rows & has_later, edge.fine(j).start)

    def keep_own(p):
        blocks(p * chunk, chunk, value1(3), store_land)

    def receive(p):
        @pl.when(p < n)
        def _():
            for i in range(pieces):
                j = p * pieces + i
                when(outer | (half == 1) | (j >= taken), functools.partial(take, j))

        when(inner & (half == 0) & (p < n - OWN_LEAD), functools.partial(keep_own, p + OWN_LEAD))

        @pl.when(p >= EDGE_LAG)
        def _():
            k = p - EDGE_LAG
            when(has_earlier, edge(k).wait_recv)
            finish(k * chunk, chunk)

    when(inner, place_rows)
    when(inner, pick_rows)
    for j in range(n0):
        with phase("own0"):
            own0(j, (1 - c) * rows).wait_recv()
    pltpu.make_async_copy(plan_v, plan, s_plan.at[0]).wait()

    @pl.when(outer)
    def _():
        def send_head(j):
            blocks(j * chunk, chunk, value0, store_head)
            head(j).start()

        loop("heads", HEAD, send_head)
        take_rim()

        def produce(j):
            @pl.when(j < HEAD)
            def _():
                blocks(j * chunk, chunk, value0, store_tail)

            far(j).start()

            @pl.when(j + HEAD < n)
            def _():
                blocks((j + HEAD) * chunk, chunk, value0, store_mine)
                head(j + HEAD).start()

        loop("produce", n, produce)

        def from_across(j):
            got_across.coarse(j).wait_recv()

            @pl.when((half == 0) & has_later)
            def _():
                for i in range(COARSE // FINE):
                    edge.fine(j * (COARSE // FINE) + i).start()

        loop("from_across", rows // COARSE, from_across)

    @pl.when(inner)
    def _():
        def produce(j):
            for i in range(OWN_GROUP):
                blocks((j * OWN_GROUP + i) * chunk, chunk, value0, store0)
                when((half == 0) & has_later, halo_mine(j * OWN_GROUP + i).start)
            own1(j, OWN_GROUP).start()

        take_rim()

        def pass_head(j):
            head(j).wait_recv()
            when((half == 1) & has_later, halo_far(j).start)

        def pass_halo(j):
            @pl.when(has_earlier)
            def _():
                halo_mine(j).wait_recv()
                halo_on(j).start()

        first_rows = functools.partial(loop, "produce", HEAD // OWN_GROUP, produce)
        when(half == 0, first_rows)
        loop("heads", HEAD, pass_head)
        when(half == 1, first_rows)
        pltpu.make_async_copy(picks_v, picks, s_plan.at[1]).wait()
        loop("halos", HEAD - HALO_LAG, pass_halo)

        def gather(k):
            @pl.when(lax.rem(k, OWN_GROUP) == 0)
            def _():
                own1(lax.div(k, OWN_GROUP), OWN_GROUP).wait_recv()

            far_on(k).wait_recv()
            start = pl.multiple_of(k * chunk, chunk)
            mine_at, other_at = c * rows + start, (1 - c) * rows + start
            for u in range(chunk):
                cur[own_base + other_at + u, tiles:, :] = own_in[start + u]
                cur[far_base + mine_at + u, tiles:, :] = far_in[start + u]
                cur[far_base + other_at + u, tiles:, :] = far_pass[start + u]

            @pl.when(has_earlier)
            def _():
                halo_on(k).wait_recv()
                for u in range(chunk):
                    cur[up_base + mine_at + u, :tiles, :] = halo_in[start + u]
                    cur[up_base + other_at + u, :tiles, :] = halo_pass[start + u]

            blocks(k * chunk, chunk, value1(0), store_picked(0))
            far_outer(k).start()

        def stream(j):
            when(j > 0, functools.partial(gather, j - 1))

            @pl.when(j < n)
            def _():
                far(j).wait_recv()
                far_on(j).start()

            when(j < n - HEAD, functools.partial(pass_head, j + HEAD))
            when(j < n - HEAD + HALO_LAG, functools.partial(pass_halo, j + HEAD - HALO_LAG))
            group = lax.div(j + HEAD, OWN_GROUP)
            when((lax.rem(j, OWN_GROUP) == 0) & (group < n // OWN_GROUP), functools.partial(produce, group))

        loop("stream", n + 1, stream)

        def rest(j):
            blocks(j * FINE, FINE, value1(2), store_picked(2))
            far_inner.fine(j).start()
            blocks(j * FINE, FINE, value1(1), store_picked(1))
            near_outer.fine(j).start()

            @pl.when(half == 1)
            def _():
                blocks(j * FINE, FINE, value1(3), store_land)
                when(has_later, edge.fine(j).start)

            turn = j - REST_FIRST

            @pl.when((half == 0) & (turn >= 0) & (lax.rem(jnp.maximum(turn, 0), REST_STEP) == 0))
            def _():
                take(lax.div(turn, REST_STEP))

        loop("rest", n_fine, rest)
        when(half == 0, functools.partial(loop, "own", OWN_LEAD, keep_own))

    loop("receive", n + EDGE_LAG, receive)

    @pl.when(outer)
    def _():
        head_all.wait_send()
        far_all.wait_send()

    @pl.when(inner)
    def _():
        own1_all.wait_send()
        far_on_all.wait_send()
        when(has_later, halo_all.wait_send)
        when(has_earlier, halo_on_all.wait_send)
        far_outer_all.wait_send()
        near_outer_all.wait_send()
        far_inner_all.wait_send()

    when(has_later, edge_all.wait_send)
    own0(None, c * rows).wait_send()
    when((c == 1) & has_later, rim_out0(None).wait_send)
    when((c == 1) & has_earlier, rim_in0(None).wait_send)


def per_device_fused(tm_size, band_state, lower_rows, upper_rows, delays, counts):
    row_count, samples = band_state.shape
    tiles = samples // LANES
    n = row_count // CHUNK_ROWS
    dma = pltpu.SemaphoreType.DMA
    wide = pltpu.VMEM((row_count, tiles, LANES), jnp.float32)
    return pl.pallas_call(
        functools.partial(kernel, tiles, tm_size),
        out_shape=pltpu.VMEM((row_count, samples), jnp.float32),
        in_specs=[pl.BlockSpec(memory_space=pltpu.HBM)] * 5,
        out_specs=pl.BlockSpec(memory_space=pltpu.VMEM),
        scratch_shapes=[
            pltpu.VMEM(band_state.shape, jnp.float32),
            pltpu.VMEM(lower_rows.shape, jnp.int32),
            pltpu.VMEM(upper_rows.shape, jnp.int32),
            pltpu.VMEM(delays.shape, jnp.int32),
            pltpu.SMEM(counts.shape, jnp.int32),
            pltpu.VMEM((4 * row_count, LANES), jnp.int32),
            pltpu.VMEM((2 * row_count, LANES), jnp.int32),
            pltpu.VMEM((2 * row_count, LANES), jnp.int32),
            pltpu.VMEM((2 * row_count // LANES, LANES), jnp.int32),
            pltpu.SMEM((2 * row_count // LANES, LANES), jnp.int32),
            pltpu.VMEM((4 * row_count // LANES, LANES), jnp.int32),
            pltpu.SMEM((4 * row_count // LANES, LANES), jnp.int32),
            pltpu.VMEM((2 * row_count, 2 * tiles, LANES), jnp.float32),
            wide,
            wide,
            pltpu.VMEM((4 * row_count, 2 * tiles, LANES), jnp.float32),
            wide, wide, wide, wide, wide,
            pltpu.VMEM((3, row_count, tiles, LANES), jnp.float32),
            pltpu.VMEM((2, row_count, tiles, LANES), jnp.float32),
            wide,
            pltpu.VMEM((row_count, 2 * tiles, LANES), jnp.float32),
            wide,
            dma((13,)),
            dma((CHUNKS_0 + 4,)),
            dma((2,)),
            dma((3 * CHUNKS_0,)),
            dma((n,)),
            dma((n,)),
            dma((n,)),
            dma((n // OWN_GROUP,)),
            dma((n,)),
            dma((n,)),
            dma((row_count // COARSE,)),
            dma((row_count // FINE,)),
            dma((n,)),
        ],
        compiler_params=pltpu.CompilerParams(
            collective_id=0, has_side_effects=True, vmem_limit_bytes=58 * 2**20
        ),
    )(band_state, lower_rows, upper_rows, delays, counts)


def solution(mesh):
    if mesh.shape["freq"] == 2**ITERS:
        body = functools.partial(per_device_fused, mesh.shape["tm"])
    else:
        body = per_device_general
    return jax.shard_map(
        body,
        mesh=mesh,
        in_specs=(P("freq", "tm"), P(), P(), P(), P()),
        out_specs=P("freq", "tm"),
        check_vma=False,
    )
```

```python
import contextlib
import functools

import jax
import jax.numpy as jnp
from jax import lax
from jax.experimental import pallas as pl
from jax.experimental.pallas import tpu as pltpu
from jax.sharding import PartitionSpec as P

DMAX = 2048
ITERS = 3
LANES = 128
SUBLANES = 8
UNROLL = 16
CHUNKS_0 = 2
CHUNK_ROWS = 16
HEAD = 2
HALO_LAG = 2
FIRST_OWN = 2
OWN_GROUP = 2
PLAN_UNROLL = 8
EDGE_LAG = 3
REST_FIRST = 9
REST_STEP = 2
OWN_LEAD = 2
COARSE = 64
FINE = 16


def shifted_2(block, axis, distance):
    devices = range(lax.axis_size(axis))
    route = [(i - distance, i) for i in devices if i - distance in devices]
    return lax.ppermute(block, axis, route)


def delay_columns(extended, shifts, widest):
    row_count = extended.shape[0]
    for bit_index in range(widest.bit_length()):
        stride = 1 << bit_index
        shifted = jnp.concatenate(
            [jnp.zeros((row_count, stride), extended.dtype), extended[:, :-stride]], axis=1
        )
        extended = jnp.where((shifts >> bit_index & 1)[:, None] == 1, shifted, extended)
    return extended


def live_mask(global_rows, counts, width_out, offset, bands_out):
    band_index = global_rows // width_out
    band_counts = counts[offset : offset + bands_out]
    matches = band_index[:, None] == jnp.arange(bands_out, dtype=jnp.int32)[None, :]
    live_count = jnp.sum(jnp.where(matches, band_counts[None, :], 0), axis=1)
    return global_rows % width_out < live_count


def per_device_general(band_state, lower_rows, upper_rows, delays, counts):
    row_count, samples = band_state.shape
    freq_index = lax.axis_index("freq")
    first_row = freq_index * row_count
    global_rows = first_row + jnp.arange(row_count, dtype=jnp.int32)
    current = band_state
    for iteration in range(ITERS):
        width_in = DMAX >> ITERS - iteration
        width_out = 2 * width_in
        bands_out = DMAX // width_out
        offset = 2**ITERS - 2 ** (ITERS - iteration)
        lower_source = lax.dynamic_slice_in_dim(lower_rows[iteration], first_row, row_count)
        upper_source = lax.dynamic_slice_in_dim(upper_rows[iteration], first_row, row_count)
        own_delays = lax.dynamic_slice_in_dim(delays[iteration], first_row, row_count)
        gathered = lax.all_gather(current, "freq", axis=0, tiled=True)
        lower_values = jnp.take(gathered, lower_source, axis=0)
        upper_values = jnp.take(gathered, upper_source, axis=0)
        rim_columns = shifted_2(upper_values[:, samples - width_in :], "tm", 1)
        extended = jnp.concatenate([rim_columns, upper_values], axis=1)
        delayed = delay_columns(extended, own_delays, width_in)[:, width_in:]
        live_rows = live_mask(global_rows, counts, width_out, offset, bands_out)
        current = jnp.where(live_rows[:, None], lower_values + delayed, jnp.zeros_like(delayed))
    return current


MESH = pl.DeviceIdType.MESH


def phase(name):
    return contextlib.nullcontext()


def kernel(
    tiles, tm_size, x_in, lower_in, upper_in, delays_in, counts_in,
    out_ref, x_ref, lower, upper, delays, counts, columns, columns_0, places, plan_v, plan, picks_v, picks, raw, rim_in, mine, cur, own_in, far_in, far_pass, halo_in, halo_pass,
    picked, land, early, joined, final,
    sent, s_load, s_plan, s_raw, s_head, s_far, s_far_pass, s_own, s_halo, s_halo_pass, s_fo, s_last, s_edge,
):
    f, t = lax.axis_index("freq"), lax.axis_index("tm")
    c, z = lax.rem(f, 2), lax.div(f, 2)
    zb, half = lax.rem(z, 2), lax.div(z, 2)
    rows = x_ref.shape[0]
    chunk = CHUNK_ROWS
    n = rows // chunk
    at = lambda ff, tt: {"freq": ff, "tm": tt}
    partner = at(f + 1 - 2 * c, t)
    near = at(f + 2 - 4 * zb, t)
    across = at(f + 4 - 8 * half, t)
    facing = at(f + 2 - 4 * half, t)
    later = at(f, t + 1)
    earlier = at(f, t - 1)
    inner = zb != half
    outer = zb == half
    has_later, has_earlier = t < tm_size - 1, t > 0

    n0, chunk0 = CHUNKS_0, rows // CHUNKS_0

    def load(j, source, target):
        return pltpu.make_async_copy(source, target, s_load.at[j])

    parts = [pl.ds(j * chunk0, chunk0) for j in range(n0)]
    loads = [load(j, x_in.at[part], x_ref.at[part]) for j, part in enumerate(parts)]
    pairs = ((lower_in, lower), (upper_in, upper), (delays_in, delays), (counts_in, counts))
    table_loads = [load(n0 + j, *pair) for j, pair in enumerate(pairs)]
    for copy in loads + table_loads:
        copy.start()

    barrier = pltpu.get_barrier_semaphore()

    def greet(target):
        pl.semaphore_signal(barrier, inc=1, device_id=target, device_id_type=MESH)

    greet(partner)
    greet(near)
    greet(across)
    for cond, target in ((inner, facing), (has_earlier, earlier), (has_later, later)):
        pl.when(cond)(functools.partial(greet, target))

    lane = lax.broadcasted_iota(jnp.int32, (tiles, LANES), 1)
    zero = jnp.zeros((tiles, LANES), jnp.float32)

    def when(cond, action):
        pl.when(cond)(action)

    def remote(src, dst, flow, sem, target):
        return pltpu.make_async_remote_copy(
            src_ref=src, dst_ref=dst, send_sem=sent.at[flow], recv_sem=sem,
            device_id=target, device_id_type=MESH,
        )

    def span(j, group=1):
        return pl.ds(pl.multiple_of(j * chunk * group, chunk * group), chunk * group)

    n_fine = rows // FINE

    def coarse(j):
        return pl.ds(pl.multiple_of(j * COARSE, COARSE), COARSE)

    def fine(j):
        return pl.ds(pl.multiple_of(j * FINE, FINE), FINE)

    def delayed(source, row, d, first):
        q, r = d >> 7, d & (LANES - 1)
        a = source[row, pl.ds(tiles - q, tiles), :]
        b = source[row, pl.ds(jnp.maximum(tiles - 1 - q, first), tiles), :]
        a, b = pltpu.roll(a, r, 1), pltpu.roll(b, r, 1)
        return jnp.where(lane >= r, a, b)

    def blocks(start, count, value, store):
        def body(base, size):
            values = [(base + u, value(base, u)) for u in range(size)]
            for m, v in values:
                store(m, v)

        def step(i, carry):
            body(start + i * UNROLL, UNROLL)
            return carry

        if count <= UNROLL:
            body(start, count)
        else:
            lax.fori_loop(0, count // UNROLL, step, 0)

    rim0 = rows // LANES
    full0, tail0, kept0 = pl.ds(tiles, tiles), pl.ds(2 * tiles - rim0, rim0), pl.ds(tiles - rim0, rim0)

    def part_of(j, row=0):
        return pl.ds(row, rows) if j is None else pl.ds(row + j * chunk0, chunk0)

    def own0(j, row):
        at_rows = raw.at[part_of(j, row), full0]
        return remote(at_rows, at_rows, 0, s_raw.at[j or 0], partner)

    def rim_out0(j):
        return remote(raw.at[part_of(j, rows), tail0], rim_in.at[part_of(j), kept0], 1, s_raw.at[n0 + (j or 0)], later)

    def rim_in0(j):
        at_rows = rim_in.at[part_of(j), kept0]
        return remote(at_rows, at_rows, 2, s_raw.at[2 * n0 + (j or 0)], partner)

    def spread(first, count, first_tile, last_tile):
        def body(step, carry):
            r = first + step * SUBLANES
            for tile in range(first_tile, last_tile):
                raw[pl.ds(c * rows + r, SUBLANES), tiles + tile, :] = x_ref[
                    pl.ds(r, SUBLANES), pl.ds(tile * LANES, LANES)
                ]
            return carry

        lax.fori_loop(0, count // SUBLANES, body, 0)

    for j in range(n0):
        with phase("spread"):
            loads[j].wait()
            spread(j * chunk0, chunk0, tiles - rim0, tiles)
    one = lambda cond: jnp.where(cond, 1, 0)
    with phase("greet"):
        pl.semaphore_wait(barrier, 3 + one(inner) + one(has_earlier) + one(has_later))
    for j in range(n0):
        when((c == 1) & has_later, rim_out0(j).start)
    for j in range(n0):
        with phase("send0"):
            spread(j * chunk0, chunk0, 0, tiles - rim0)
            own0(j, c * rows).start()

    def clear(count, store):
        def body(i, carry):
            for u in range(UNROLL):
                store(i * UNROLL + u)
            return carry

        lax.fori_loop(0, count // UNROLL, body, 0)

    @pl.when(t == 0)
    def _():
        def clear_raw(i):
            raw[rows + i, :tiles, :] = zero

        def clear_cur(i):
            cur[2 * rows + i, :tiles, :] = zero

        def clear_early(i):
            early[i] = zero

        clear(rows, clear_raw)
        clear(2 * rows, clear_cur)
        clear(rows, clear_early)

    chip_rows, half_rows = 2 * rows, 4 * rows
    flat = (SUBLANES, LANES)
    lane_at = lax.broadcasted_iota(jnp.int32, flat, 1)
    line_at = lax.broadcasted_iota(jnp.int32, flat, 0)
    none = jnp.zeros(flat, jnp.int32)
    groups = lambda count: range(count // LANES)

    def row_of(table, level, start):
        return jnp.broadcast_to(table[level : level + 1, pl.ds(pl.multiple_of(start, LANES), LANES)], flat)

    def wanted(start):
        return jnp.where(half == 0, row_of(lower, ITERS - 1, start), row_of(upper, ITERS - 1, start)) & (half_rows - 1)

    def set_columns(target, start, row):
        target[pl.ds(start, LANES), :] = jnp.broadcast_to(row[0:1], (LANES, LANES)).T

    def fold(values, combine):
        for s in (4, 2, 1):
            values = [combine(v, pltpu.roll(v, s, 0)) for v in values]
        return values

    def scan(count, init, step):
        def body(i, carry):
            for u in range(PLAN_UNROLL):
                at_row = (i * PLAN_UNROLL + u) * SUBLANES
                carry = step(pl.multiple_of(at_row, SUBLANES), line_at + at_row, carry)
            return carry

        return lax.fori_loop(0, count // SUBLANES // PLAN_UNROLL, body, init)

    add, least = lambda a, b: a + b, jnp.minimum
    bit = lambda cond, place: jnp.where(cond, 1 << place, 0)

    def find_order():
        for g in groups(half_rows):
            start = half * half_rows + g * LANES
            low, high = row_of(lower, 1, start), row_of(upper, 1, start)
            set_columns(columns, g * LANES, (low & (chip_rows - 1)) | (high & (chip_rows - 1)) << 9)
        want = [wanted((1 - half) * 3 * chip_rows + g * LANES) for g in groups(chip_rows)]

        def use(at_row, index, carry):
            line = columns[pl.ds(at_row, SUBLANES), :]
            return tuple(v + jnp.where(w == index, line, 0) for v, w in zip(carry, want))

        used = fold(scan(half_rows, (none,) * len(want), use), add)
        for g, row in enumerate(used):
            set_columns(columns, g * LANES, row)

        def meet(at_row, index, carry):
            line = columns[pl.ds(at_row, SUBLANES), :]
            low, high = line & (chip_rows - 1), line >> 9
            turn = 2 * (index & (rows - 1)) + lax.div(index, rows)
            hits = [(part, g) for part in (low, high) for g in groups(chip_rows)]
            return tuple(
                least(v, jnp.where(part == lane_at + g * LANES, turn, chip_rows)) for v, (part, g) in zip(carry, hits)
            )

        never = jnp.full(flat, chip_rows, jnp.int32)
        first = fold(scan(chip_rows, (never,) * (2 * len(want)), meet), least)
        keys = [v * chip_rows + lane_at + (g % len(want)) * LANES for g, v in enumerate(first)]
        for g, row in enumerate(keys):
            set_columns(columns, g * LANES, row)

        def count(at_row, index, carry):
            low = columns[pl.ds(at_row, SUBLANES), :]
            high = columns[pl.ds(chip_rows + at_row, SUBLANES), :]
            parts = [low] * len(want) + [high] * len(want)
            return tuple(v + jnp.where(part < key, 1, 0) for v, part, key in zip(carry, parts, keys))

        ranks = fold(scan(chip_rows, (none,) * len(keys), count), add)
        place = [(v & 1) * rows + (v >> 1) for v in ranks]
        for g in groups(chip_rows):
            low, high = place[g], place[len(want) + g]
            set_columns(places, g * LANES, low | high << 9)
            start = z * chip_rows + g * LANES
            low, high = row_of(lower, 0, start), row_of(upper, 0, start)
            live = bit(lane_at + g * LANES < counts[z], 28)
            word = (low & (chip_rows - 1)) | (high & (chip_rows - 1)) << 9 | row_of(delays, 0, start) << 18 | live
            set_columns(columns_0, g * LANES, word)

        def pick(at_row, index, carry):
            line = places[pl.ds(at_row, SUBLANES), :]
            own = jnp.where(zb == 0, line & (chip_rows - 1), line >> 9)
            word = columns_0[pl.ds(at_row, SUBLANES), :]
            return tuple(
                v + jnp.where(own == lane_at + (c * rows + g * LANES), word, 0) for g, v in enumerate(carry)
            )

        words = fold(scan(chip_rows, (none,) * len(groups(rows)), pick), add)
        for g, row in enumerate(words):
            plan_v[pl.ds(g, 1), :] = row[0:1]
            start = f * rows + g * LANES
            live = bit(lane_at + start < counts[2**ITERS - 2], 12)
            plan_v[pl.ds(rows // LANES + g, 1), :] = (row_of(delays, 2, start) | live)[0:1]
        pltpu.make_async_copy(plan_v, plan, s_plan.at[0]).start()

    def place_rows():
        marks = [half * half_rows + g * LANES for g in groups(half_rows)]
        low = [row_of(lower, 1, start) & (chip_rows - 1) for start in marks]
        high = [row_of(upper, 1, start) & (chip_rows - 1) for start in marks]

        def put(at_row, index, carry):
            line = places[pl.ds(at_row, SUBLANES), :]
            shifted = line >> 9 << 9
            line = line & (chip_rows - 1)
            return tuple(
                v + jnp.where(a == index, line, 0) + jnp.where(b == index, shifted, 0)
                for v, a, b in zip(carry, low, high)
            )

        words = fold(scan(chip_rows, (none,) * len(marks), put), add)
        for g, (start, word) in enumerate(zip(marks, words)):
            live = bit(lane_at + g * LANES < counts[2 ** (ITERS - 1) + half], 28)
            set_columns(columns, g * LANES, word | row_of(delays, 1, start) << 18 | live)

    def pick_rows():
        targets = (f + 4 - 8 * half, f + 2 - 4 * zb, f + 2 - 4 * half, f)
        want = [wanted(target * rows + g * LANES) for target in targets for g in groups(rows)]

        def pick(at_row, index, carry):
            line = columns[pl.ds(at_row, SUBLANES), :]
            return tuple(v + jnp.where(w == index, line, 0) for v, w in zip(carry, want))

        words = fold(scan(half_rows, (none,) * len(want), pick), add)
        for g, row in enumerate(words):
            picks_v[pl.ds(g, 1), :] = row[0:1]
        pltpu.make_async_copy(picks_v, picks, s_plan.at[1]).start()

    with phase("order"):
        for copy in table_loads:
            copy.wait()
        find_order()

    def take_rim():
        for j in range(n0):

            @pl.when((c == 1) & has_earlier)
            def _():
                with phase("rim_out"):
                    rim_out0(j).wait_recv()
                    rim_in0(j).start()

        for j in range(n0):
            with phase("rim_in"):
                when((c == 0) & has_earlier, rim_in0(j).wait_recv)

        @pl.when(has_earlier)
        def _():
            def fill(i):
                raw[rows + i, :tiles, :] = rim_in[i]

            clear(rows, fill)

    own_base, far_base = zb * 2 * rows, (1 - zb) * 2 * rows
    up_base = 2 * rows
    def entry(table, first, base, u):
        return table[first + (base >> 7), (base & (LANES - 1)) + u]

    def value0(base, u):
        word = entry(plan, 0, base, u)
        lo, up, d = word & 511, (word >> 9) & 511, (word >> 18) & 1023
        total = raw[lo, tiles:, :] + delayed(raw, up, d, tiles - rim0)
        return jnp.where((word >> 28) == 1, total, zero)

    split = tiles // 2

    def store0(m, v):
        mine[m] = v
        cur[own_base + c * rows + m, tiles:, :] = v

    def store_mine(m, v):
        mine[m] = v

    def store_head(m, v):
        mine[m, split:, :] = v[split:, :]

    def store_tail(m, v):
        mine[m, :split, :] = v[:split, :]

    rim1 = 2 * rows // LANES

    def value1(kind):
        def value(base, u):
            word = entry(picks, kind * (rows // LANES), base, u)
            a, b, d = word & 511, (word >> 9) & 511, (word >> 18) & 1023
            total = cur[a, tiles:, :] + delayed(cur, up_base + b, d, tiles - rim1)
            return jnp.where((word >> 28) == 1, total, zero)

        return value

    def store_picked(kind):
        def store(m, v):
            picked[kind, m] = v

        return store

    def store_land(m, v):
        land[half, m] = v

    def join(m):
        joined[m, :tiles, :] = early[m]
        joined[m, tiles:, :] = land[1, m]

    def value2(base, u):
        word = entry(plan, rows // LANES, base, u)
        total = land[0, base + u] + delayed(joined, base + u, word & 4095, 0)
        return jnp.where((word >> 12) == 1, total, zero)

    def store2(m, v):
        final[m] = v

    def finish(first, count):
        def step(i, carry):
            start = pl.multiple_of(first + i * FINE, FINE)
            for u in range(FINE):
                join(start + u)
            blocks(start, FINE, value2, store2)
            for tile in range(tiles):
                at_tile = pl.ds(tile * LANES, LANES)
                out_ref[pl.ds(start, FINE), at_tile] = final[pl.ds(start, FINE), tile, :]
            return carry

        lax.fori_loop(0, count // FINE, step, 0)

    rim = pl.ds(tiles - rim1, rim1)
    every = pl.ds(0, rows)

    def flow(index, src, dst, sems, target):
        def copy(j, group=1):
            at_rows = span(j, group)
            return remote(src(at_rows), dst(at_rows), index, sems.at[j], target)

        copy.coarse = lambda j: remote(src(coarse(j)), dst(coarse(j)), index, sems.at[j], target)
        copy.fine = lambda j: remote(src(fine(j)), dst(fine(j)), index, sems.at[lax.div(j, n_fine // sems.shape[0])], target)

        return copy, remote(src(every), dst(every), index, sems.at[0], target)

    lead, trail = pl.ds(split, tiles - split), pl.ds(0, split)
    head, head_all = flow(3, lambda r: mine.at[r, lead], lambda r: far_in.at[r, lead], s_head, near)
    far, far_all = flow(12, lambda r: mine.at[r, trail], lambda r: far_in.at[r, trail], s_far, near)
    far_on, far_on_all = flow(4, lambda r: far_in.at[r], lambda r: far_pass.at[r], s_far_pass, partner)
    own1, own1_all = flow(5, lambda r: mine.at[r], lambda r: own_in.at[r], s_own, partner)
    halo_mine, halo_all = flow(6, lambda r: mine.at[r, rim], lambda r: halo_in.at[r, rim], s_halo, later)
    halo_far, _ = flow(6, lambda r: far_in.at[r, rim], lambda r: halo_in.at[r, rim], s_halo, later)
    halo_on, halo_on_all = flow(7, lambda r: halo_in.at[r, rim], lambda r: halo_pass.at[r, rim], s_halo_pass, partner)
    to_half = lambda h: lambda r: land.at[h, r]
    _, far_outer_all = flow(8, lambda r: picked.at[0, r], to_half(half), s_fo, across)
    far_outer = lambda j: remote(
        picked.at[0, span(j)], land.at[half, span(j)], 8, s_fo.at[lax.div(j * chunk, COARSE)], across
    )
    near_outer, near_outer_all = flow(9, lambda r: picked.at[1, r], to_half(half), s_last, near)
    far_inner, far_inner_all = flow(10, lambda r: picked.at[2, r], to_half(half), s_last, facing)
    got_across, _ = flow(8, lambda r: picked.at[0, r], to_half(1 - half), s_fo, across)
    got_facing, _ = flow(10, lambda r: picked.at[2, r], to_half(1 - half), s_last, facing)
    edge, edge_all = flow(11, lambda r: land.at[1, r], lambda r: early.at[r], s_edge, later)

    def loop(name, count, body):
        def step(j, carry):
            with phase(name):
                body(j)
            return carry

        lax.fori_loop(0, count, step, 0)

    last_rows = zb == 1
    pieces = chunk // FINE
    taken = (n_fine - 1 - REST_FIRST) // REST_STEP + 1

    def take(j):
        when(inner, got_facing.fine(j).wait_recv)
        when(outer, near_outer.fine(j).wait_recv)
        when(last_rows & has_later, edge.fine(j).start)

    def keep_own(p):
        blocks(p * chunk, chunk, value1(3), store_land)

    def receive(p):
        @pl.when(p < n)
        def _():
            for i in range(pieces):
                j = p * pieces + i
                when(outer | (half == 1) | (j >= taken), functools.partial(take, j))

        when(inner & (half == 0) & (p < n - OWN_LEAD), functools.partial(keep_own, p + OWN_LEAD))

        @pl.when(p >= EDGE_LAG)
        def _():
            k = p - EDGE_LAG
            when(has_earlier, edge(k).wait_recv)
            finish(k * chunk, chunk)

    when(inner, place_rows)
    when(inner, pick_rows)
    for j in range(n0):
        with phase("own0"):
            own0(j, (1 - c) * rows).wait_recv()
    pltpu.make_async_copy(plan_v, plan, s_plan.at[0]).wait()

    @pl.when(outer)
    def _():
        def send_head(j):
            blocks(j * chunk, chunk, value0, store_head)
            head(j).start()

        loop("heads", HEAD, send_head)
        take_rim()

        def produce(j):
            @pl.when(j < HEAD)
            def _():
                blocks(j * chunk, chunk, value0, store_tail)

            far(j).start()

            @pl.when(j + HEAD < n)
            def _():
                blocks((j + HEAD) * chunk, chunk, value0, store_mine)
                head(j + HEAD).start()

        loop("produce", n, produce)

        def from_across(j):
            got_across.coarse(j).wait_recv()

            @pl.when((half == 0) & has_later)
            def _():
                for i in range(COARSE // FINE):
                    edge.fine(j * (COARSE // FINE) + i).start()

        loop("from_across", rows // COARSE, from_across)

    @pl.when(inner)
    def _():
        def produce(j):
            for i in range(OWN_GROUP):
                blocks((j * OWN_GROUP + i) * chunk, chunk, value0, store0)
                when((half == 0) & has_later, halo_mine(j * OWN_GROUP + i).start)
            own1(j, OWN_GROUP).start()

        take_rim()

        def pass_head(j):
            head(j).wait_recv()
            when((half == 1) & has_later, halo_far(j).start)

        def pass_halo(j):
            @pl.when(has_earlier)
            def _():
                halo_mine(j).wait_recv()
                halo_on(j).start()

        def begin(j):
            when(half == 1, functools.partial(pass_head, j))
            produce(j)

        loop("produce", FIRST_OWN, begin)
        loop("heads", HEAD, lambda j: when((half == 0) | (j >= FIRST_OWN), functools.partial(pass_head, j)))
        pltpu.make_async_copy(picks_v, picks, s_plan.at[1]).wait()
        loop("halos", HEAD - HALO_LAG, pass_halo)

        def gather(k):
            @pl.when(lax.rem(k, OWN_GROUP) == 0)
            def _():
                own1(lax.div(k, OWN_GROUP), OWN_GROUP).wait_recv()

            far_on(k).wait_recv()
            start = pl.multiple_of(k * chunk, chunk)
            mine_at, other_at = c * rows + start, (1 - c) * rows + start
            for u in range(chunk):
                cur[own_base + other_at + u, tiles:, :] = own_in[start + u]
                cur[far_base + mine_at + u, tiles:, :] = far_in[start + u]
                cur[far_base + other_at + u, tiles:, :] = far_pass[start + u]

            @pl.when(has_earlier)
            def _():
                halo_on(k).wait_recv()
                for u in range(chunk):
                    cur[up_base + mine_at + u, :tiles, :] = halo_in[start + u]
                    cur[up_base + other_at + u, :tiles, :] = halo_pass[start + u]

            blocks(k * chunk, chunk, value1(0), store_picked(0))
            far_outer(k).start()

        def stream(j):
            when(j > 0, functools.partial(gather, j - 1))

            @pl.when(j < n)
            def _():
                far(j).wait_recv()
                far_on(j).start()

            when(j < n - HEAD + HALO_LAG, functools.partial(pass_halo, j + HEAD - HALO_LAG))
            when(j < n - HEAD, functools.partial(pass_head, j + HEAD))
            group = lax.div(j, OWN_GROUP) + FIRST_OWN
            when((lax.rem(j, OWN_GROUP) == 0) & (group < n // OWN_GROUP), functools.partial(produce, group))

        loop("stream", n + 1, stream)

        def rest(j):
            blocks(j * FINE, FINE, value1(2), store_picked(2))
            far_inner.fine(j).start()
            blocks(j * FINE, FINE, value1(1), store_picked(1))
            near_outer.fine(j).start()

            @pl.when(half == 1)
            def _():
                blocks(j * FINE, FINE, value1(3), store_land)
                when(has_later, edge.fine(j).start)

            turn = j - REST_FIRST

            @pl.when((half == 0) & (turn >= 0) & (lax.rem(jnp.maximum(turn, 0), REST_STEP) == 0))
            def _():
                take(lax.div(turn, REST_STEP))

        loop("rest", n_fine, rest)
        when(half == 0, functools.partial(loop, "own", OWN_LEAD, keep_own))

    loop("receive", n + EDGE_LAG, receive)

    @pl.when(outer)
    def _():
        head_all.wait_send()
        far_all.wait_send()

    @pl.when(inner)
    def _():
        own1_all.wait_send()
        far_on_all.wait_send()
        when(has_later, halo_all.wait_send)
        when(has_earlier, halo_on_all.wait_send)
        far_outer_all.wait_send()
        near_outer_all.wait_send()
        far_inner_all.wait_send()

    when(has_later, edge_all.wait_send)
    own0(None, c * rows).wait_send()
    when((c == 1) & has_later, rim_out0(None).wait_send)
    when((c == 1) & has_earlier, rim_in0(None).wait_send)


def per_device_fused(tm_size, band_state, lower_rows, upper_rows, delays, counts):
    row_count, samples = band_state.shape
    tiles = samples // LANES
    n = row_count // CHUNK_ROWS
    dma = pltpu.SemaphoreType.DMA
    wide = pltpu.VMEM((row_count, tiles, LANES), jnp.float32)
    return pl.pallas_call(
        functools.partial(kernel, tiles, tm_size),
        out_shape=pltpu.VMEM((row_count, samples), jnp.float32),
        in_specs=[pl.BlockSpec(memory_space=pltpu.HBM)] * 5,
        out_specs=pl.BlockSpec(memory_space=pltpu.VMEM),
        scratch_shapes=[
            pltpu.VMEM(band_state.shape, jnp.float32),
            pltpu.VMEM(lower_rows.shape, jnp.int32),
            pltpu.VMEM(upper_rows.shape, jnp.int32),
            pltpu.VMEM(delays.shape, jnp.int32),
            pltpu.SMEM(counts.shape, jnp.int32),
            pltpu.VMEM((4 * row_count, LANES), jnp.int32),
            pltpu.VMEM((2 * row_count, LANES), jnp.int32),
            pltpu.VMEM((2 * row_count, LANES), jnp.int32),
            pltpu.VMEM((2 * row_count // LANES, LANES), jnp.int32),
            pltpu.SMEM((2 * row_count // LANES, LANES), jnp.int32),
            pltpu.VMEM((4 * row_count // LANES, LANES), jnp.int32),
            pltpu.SMEM((4 * row_count // LANES, LANES), jnp.int32),
            pltpu.VMEM((2 * row_count, 2 * tiles, LANES), jnp.float32),
            wide,
            wide,
            pltpu.VMEM((4 * row_count, 2 * tiles, LANES), jnp.float32),
            wide, wide, wide, wide, wide,
            pltpu.VMEM((3, row_count, tiles, LANES), jnp.float32),
            pltpu.VMEM((2, row_count, tiles, LANES), jnp.float32),
            wide,
            pltpu.VMEM((row_count, 2 * tiles, LANES), jnp.float32),
            wide,
            dma((13,)),
            dma((CHUNKS_0 + 4,)),
            dma((2,)),
            dma((3 * CHUNKS_0,)),
            dma((n,)),
            dma((n,)),
            dma((n,)),
            dma((n // OWN_GROUP,)),
            dma((n,)),
            dma((n,)),
            dma((row_count // COARSE,)),
            dma((row_count // FINE,)),
            dma((n,)),
        ],
        compiler_params=pltpu.CompilerParams(
            collective_id=0, has_side_effects=True, vmem_limit_bytes=58 * 2**20
        ),
    )(band_state, lower_rows, upper_rows, delays, counts)


def solution(mesh):
    if mesh.shape["freq"] == 2**ITERS:
        body = functools.partial(per_device_fused, mesh.shape["tm"])
    else:
        body = per_device_general
    return jax.shard_map(
        body,
        mesh=mesh,
        in_specs=(P("freq", "tm"), P(), P(), P(), P()),
        out_specs=P("freq", "tm"),
        check_vma=False,
    )
```

```python
import contextlib
import functools

import jax
import jax.numpy as jnp
from jax import lax
from jax.experimental import pallas as pl
from jax.experimental.pallas import tpu as pltpu
from jax.sharding import PartitionSpec as P

DMAX = 2048
ITERS = 3
LANES = 128
SUBLANES = 8
UNROLL = 16
CHUNKS_0 = 2
CHUNK_ROWS = 16
HEAD = 2
HALO_LAG = 2
FIRST_OWN = 2
OWN_GROUP = 2
PLAN_UNROLL = 8
EDGE_LAG = 3
REST_FIRST = 9
REST_STEP = 2
OWN_LEAD = 2
CROSS = 2
COARSE = 64
FINE = 16


def shifted_2(block, axis, distance):
    devices = range(lax.axis_size(axis))
    route = [(i - distance, i) for i in devices if i - distance in devices]
    return lax.ppermute(block, axis, route)


def delay_columns(extended, shifts, widest):
    row_count = extended.shape[0]
    for bit_index in range(widest.bit_length()):
        stride = 1 << bit_index
        shifted = jnp.concatenate(
            [jnp.zeros((row_count, stride), extended.dtype), extended[:, :-stride]], axis=1
        )
        extended = jnp.where((shifts >> bit_index & 1)[:, None] == 1, shifted, extended)
    return extended


def live_mask(global_rows, counts, width_out, offset, bands_out):
    band_index = global_rows // width_out
    band_counts = counts[offset : offset + bands_out]
    matches = band_index[:, None] == jnp.arange(bands_out, dtype=jnp.int32)[None, :]
    live_count = jnp.sum(jnp.where(matches, band_counts[None, :], 0), axis=1)
    return global_rows % width_out < live_count


def per_device_general(band_state, lower_rows, upper_rows, delays, counts):
    row_count, samples = band_state.shape
    freq_index = lax.axis_index("freq")
    first_row = freq_index * row_count
    global_rows = first_row + jnp.arange(row_count, dtype=jnp.int32)
    current = band_state
    for iteration in range(ITERS):
        width_in = DMAX >> ITERS - iteration
        width_out = 2 * width_in
        bands_out = DMAX // width_out
        offset = 2**ITERS - 2 ** (ITERS - iteration)
        lower_source = lax.dynamic_slice_in_dim(lower_rows[iteration], first_row, row_count)
        upper_source = lax.dynamic_slice_in_dim(upper_rows[iteration], first_row, row_count)
        own_delays = lax.dynamic_slice_in_dim(delays[iteration], first_row, row_count)
        gathered = lax.all_gather(current, "freq", axis=0, tiled=True)
        lower_values = jnp.take(gathered, lower_source, axis=0)
        upper_values = jnp.take(gathered, upper_source, axis=0)
        rim_columns = shifted_2(upper_values[:, samples - width_in :], "tm", 1)
        extended = jnp.concatenate([rim_columns, upper_values], axis=1)
        delayed = delay_columns(extended, own_delays, width_in)[:, width_in:]
        live_rows = live_mask(global_rows, counts, width_out, offset, bands_out)
        current = jnp.where(live_rows[:, None], lower_values + delayed, jnp.zeros_like(delayed))
    return current


MESH = pl.DeviceIdType.MESH


def phase(name):
    return contextlib.nullcontext()


def kernel(
    tiles, tm_size, x_in, lower_in, upper_in, delays_in, counts_in,
    out_ref, x_ref, lower, upper, delays, counts, columns, columns_0, places, plan_v, plan, picks_v, picks, raw, rim_in, mine, cur, own_in, far_in, far_pass, halo_in, halo_pass,
    picked, land, early, cross_own, cross_in, joined, final,
    sent, s_load, s_plan, s_raw, s_head, s_far, s_far_pass, s_own, s_halo, s_halo_pass, s_fo, s_last, s_edge, s_cross,
):
    f, t = lax.axis_index("freq"), lax.axis_index("tm")
    c, z = lax.rem(f, 2), lax.div(f, 2)
    zb, half = lax.rem(z, 2), lax.div(z, 2)
    rows = x_ref.shape[0]
    chunk = CHUNK_ROWS
    n = rows // chunk
    at = lambda ff, tt: {"freq": ff, "tm": tt}
    partner = at(f + 1 - 2 * c, t)
    near = at(f + 2 - 4 * zb, t)
    across = at(f + 4 - 8 * half, t)
    facing = at(f + 2 - 4 * half, t)
    later = at(f, t + 1)
    earlier = at(f, t - 1)
    inner = zb != half
    outer = zb == half
    has_later, has_earlier = t < tm_size - 1, t > 0

    n0, chunk0 = CHUNKS_0, rows // CHUNKS_0

    def load(j, source, target):
        return pltpu.make_async_copy(source, target, s_load.at[j])

    parts = [pl.ds(j * chunk0, chunk0) for j in range(n0)]
    loads = [load(j, x_in.at[part], x_ref.at[part]) for j, part in enumerate(parts)]
    pairs = ((lower_in, lower), (upper_in, upper), (delays_in, delays), (counts_in, counts))
    table_loads = [load(n0 + j, *pair) for j, pair in enumerate(pairs)]
    for copy in loads + table_loads:
        copy.start()

    barrier = pltpu.get_barrier_semaphore()

    def greet(target):
        pl.semaphore_signal(barrier, inc=1, device_id=target, device_id_type=MESH)

    greet(partner)
    greet(near)
    greet(across)
    for cond, target in ((inner, facing), (has_earlier, earlier), (has_later, later)):
        pl.when(cond)(functools.partial(greet, target))

    lane = lax.broadcasted_iota(jnp.int32, (tiles, LANES), 1)
    zero = jnp.zeros((tiles, LANES), jnp.float32)

    def when(cond, action):
        pl.when(cond)(action)

    def remote(src, dst, flow, sem, target):
        return pltpu.make_async_remote_copy(
            src_ref=src, dst_ref=dst, send_sem=sent.at[flow], recv_sem=sem,
            device_id=target, device_id_type=MESH,
        )

    def span(j, group=1):
        return pl.ds(pl.multiple_of(j * chunk * group, chunk * group), chunk * group)

    n_fine = rows // FINE

    def coarse(j):
        return pl.ds(pl.multiple_of(j * COARSE, COARSE), COARSE)

    def fine(j):
        return pl.ds(pl.multiple_of(j * FINE, FINE), FINE)

    def delayed(source, row, d, first):
        q, r = d >> 7, d & (LANES - 1)
        a = source[row, pl.ds(tiles - q, tiles), :]
        b = source[row, pl.ds(jnp.maximum(tiles - 1 - q, first), tiles), :]
        a, b = pltpu.roll(a, r, 1), pltpu.roll(b, r, 1)
        return jnp.where(lane >= r, a, b)

    def blocks(start, count, value, store):
        def body(base, size):
            values = [(base + u, value(base, u)) for u in range(size)]
            for m, v in values:
                store(m, v)

        def step(i, carry):
            body(start + i * UNROLL, UNROLL)
            return carry

        if count <= UNROLL:
            body(start, count)
        else:
            lax.fori_loop(0, count // UNROLL, step, 0)

    rim0 = rows // LANES
    full0, tail0, kept0 = pl.ds(tiles, tiles), pl.ds(2 * tiles - rim0, rim0), pl.ds(tiles - rim0, rim0)

    def part_of(j, row=0):
        return pl.ds(row, rows) if j is None else pl.ds(row + j * chunk0, chunk0)

    def own0(j, row):
        at_rows = raw.at[part_of(j, row), full0]
        return remote(at_rows, at_rows, 0, s_raw.at[j or 0], partner)

    def rim_out0(j):
        return remote(raw.at[part_of(j, rows), tail0], rim_in.at[part_of(j), kept0], 1, s_raw.at[n0 + (j or 0)], later)

    def rim_in0(j):
        at_rows = rim_in.at[part_of(j), kept0]
        return remote(at_rows, at_rows, 2, s_raw.at[2 * n0 + (j or 0)], partner)

    def spread(first, count, first_tile, last_tile):
        def body(step, carry):
            r = first + step * SUBLANES
            for tile in range(first_tile, last_tile):
                raw[pl.ds(c * rows + r, SUBLANES), tiles + tile, :] = x_ref[
                    pl.ds(r, SUBLANES), pl.ds(tile * LANES, LANES)
                ]
            return carry

        lax.fori_loop(0, count // SUBLANES, body, 0)

    for j in range(n0):
        with phase("spread"):
            loads[j].wait()
            spread(j * chunk0, chunk0, tiles - rim0, tiles)
    one = lambda cond: jnp.where(cond, 1, 0)
    with phase("greet"):
        pl.semaphore_wait(barrier, 3 + one(inner) + one(has_earlier) + one(has_later))
    for j in range(n0):
        when((c == 1) & has_later, rim_out0(j).start)
    for j in range(n0):
        with phase("send0"):
            spread(j * chunk0, chunk0, 0, tiles - rim0)
            own0(j, c * rows).start()

    def clear(count, store):
        def body(i, carry):
            for u in range(UNROLL):
                store(i * UNROLL + u)
            return carry

        lax.fori_loop(0, count // UNROLL, body, 0)

    @pl.when(t == 0)
    def _():
        def clear_raw(i):
            raw[rows + i, :tiles, :] = zero

        def clear_cur(i):
            cur[2 * rows + i, :tiles, :] = zero

        def clear_early(i):
            early[i] = zero

        clear(rows, clear_raw)
        clear(2 * rows, clear_cur)
        clear(rows, clear_early)

        def clear_cross(i):
            cross_in[i] = zero

        clear(CROSS * CHUNK_ROWS, clear_cross)

    chip_rows, half_rows = 2 * rows, 4 * rows
    flat = (SUBLANES, LANES)
    lane_at = lax.broadcasted_iota(jnp.int32, flat, 1)
    line_at = lax.broadcasted_iota(jnp.int32, flat, 0)
    none = jnp.zeros(flat, jnp.int32)
    groups = lambda count: range(count // LANES)

    def row_of(table, level, start):
        return jnp.broadcast_to(table[level : level + 1, pl.ds(pl.multiple_of(start, LANES), LANES)], flat)

    def wanted(start):
        return jnp.where(half == 0, row_of(lower, ITERS - 1, start), row_of(upper, ITERS - 1, start)) & (half_rows - 1)

    def set_columns(target, start, row):
        target[pl.ds(start, LANES), :] = jnp.broadcast_to(row[0:1], (LANES, LANES)).T

    def fold(values, combine):
        for s in (4, 2, 1):
            values = [combine(v, pltpu.roll(v, s, 0)) for v in values]
        return values

    def scan(count, init, step):
        def body(i, carry):
            for u in range(PLAN_UNROLL):
                at_row = (i * PLAN_UNROLL + u) * SUBLANES
                carry = step(pl.multiple_of(at_row, SUBLANES), line_at + at_row, carry)
            return carry

        return lax.fori_loop(0, count // SUBLANES // PLAN_UNROLL, body, init)

    add, least = lambda a, b: a + b, jnp.minimum
    bit = lambda cond, place: jnp.where(cond, 1 << place, 0)

    def find_order():
        for g in groups(half_rows):
            start = half * half_rows + g * LANES
            low, high = row_of(lower, 1, start), row_of(upper, 1, start)
            set_columns(columns, g * LANES, (low & (chip_rows - 1)) | (high & (chip_rows - 1)) << 9)
        want = [wanted((1 - half) * 3 * chip_rows + g * LANES) for g in groups(chip_rows)]

        def use(at_row, index, carry):
            line = columns[pl.ds(at_row, SUBLANES), :]
            return tuple(v + jnp.where(w == index, line, 0) for v, w in zip(carry, want))

        used = fold(scan(half_rows, (none,) * len(want), use), add)
        for g, row in enumerate(used):
            set_columns(columns, g * LANES, row)

        def meet(at_row, index, carry):
            line = columns[pl.ds(at_row, SUBLANES), :]
            low, high = line & (chip_rows - 1), line >> 9
            turn = 2 * (index & (rows - 1)) + lax.div(index, rows)
            hits = [(part, g) for part in (low, high) for g in groups(chip_rows)]
            return tuple(
                least(v, jnp.where(part == lane_at + g * LANES, turn, chip_rows)) for v, (part, g) in zip(carry, hits)
            )

        never = jnp.full(flat, chip_rows, jnp.int32)
        first = fold(scan(chip_rows, (never,) * (2 * len(want)), meet), least)
        keys = [v * chip_rows + lane_at + (g % len(want)) * LANES for g, v in enumerate(first)]
        for g, row in enumerate(keys):
            set_columns(columns, g * LANES, row)

        def count(at_row, index, carry):
            low = columns[pl.ds(at_row, SUBLANES), :]
            high = columns[pl.ds(chip_rows + at_row, SUBLANES), :]
            parts = [low] * len(want) + [high] * len(want)
            return tuple(v + jnp.where(part < key, 1, 0) for v, part, key in zip(carry, parts, keys))

        ranks = fold(scan(chip_rows, (none,) * len(keys), count), add)
        place = [(v & 1) * rows + (v >> 1) for v in ranks]
        for g in groups(chip_rows):
            low, high = place[g], place[len(want) + g]
            set_columns(places, g * LANES, low | high << 9)
            start = z * chip_rows + g * LANES
            low, high = row_of(lower, 0, start), row_of(upper, 0, start)
            live = bit(lane_at + g * LANES < counts[z], 28)
            word = (low & (chip_rows - 1)) | (high & (chip_rows - 1)) << 9 | row_of(delays, 0, start) << 18 | live
            set_columns(columns_0, g * LANES, word)

        def pick(at_row, index, carry):
            line = places[pl.ds(at_row, SUBLANES), :]
            own = jnp.where(zb == 0, line & (chip_rows - 1), line >> 9)
            word = columns_0[pl.ds(at_row, SUBLANES), :]
            return tuple(
                v + jnp.where(own == lane_at + (c * rows + g * LANES), word, 0) for g, v in enumerate(carry)
            )

        words = fold(scan(chip_rows, (none,) * len(groups(rows)), pick), add)
        for g, row in enumerate(words):
            plan_v[pl.ds(g, 1), :] = row[0:1]
            start = f * rows + g * LANES
            live = bit(lane_at + start < counts[2**ITERS - 2], 12)
            plan_v[pl.ds(rows // LANES + g, 1), :] = (row_of(delays, 2, start) | live)[0:1]
        facing_end = (f + 2 - 4 * half) * rows + rows - LANES
        plan_v[pl.ds(2 * rows // LANES, 1), :] = row_of(delays, 2, facing_end)[0:1]
        pltpu.make_async_copy(plan_v, plan, s_plan.at[0]).start()

    def place_rows():
        marks = [half * half_rows + g * LANES for g in groups(half_rows)]
        low = [row_of(lower, 1, start) & (chip_rows - 1) for start in marks]
        high = [row_of(upper, 1, start) & (chip_rows - 1) for start in marks]

        def put(at_row, index, carry):
            line = places[pl.ds(at_row, SUBLANES), :]
            shifted = line >> 9 << 9
            line = line & (chip_rows - 1)
            return tuple(
                v + jnp.where(a == index, line, 0) + jnp.where(b == index, shifted, 0)
                for v, a, b in zip(carry, low, high)
            )

        words = fold(scan(chip_rows, (none,) * len(marks), put), add)
        for g, (start, word) in enumerate(zip(marks, words)):
            live = bit(lane_at + g * LANES < counts[2 ** (ITERS - 1) + half], 28)
            set_columns(columns, g * LANES, word | row_of(delays, 1, start) << 18 | live)

    def pick_rows():
        targets = (f + 4 - 8 * half, f + 2 - 4 * zb, f + 2 - 4 * half, f)
        want = [wanted(target * rows + g * LANES) for target in targets for g in groups(rows)]

        def pick(at_row, index, carry):
            line = columns[pl.ds(at_row, SUBLANES), :]
            return tuple(v + jnp.where(w == index, line, 0) for v, w in zip(carry, want))

        words = fold(scan(half_rows, (none,) * len(want), pick), add)
        for g, row in enumerate(words):
            picks_v[pl.ds(g, 1), :] = row[0:1]
        pltpu.make_async_copy(picks_v, picks, s_plan.at[1]).start()

    with phase("order"):
        for copy in table_loads:
            copy.wait()
        find_order()

    def take_rim():
        for j in range(n0):

            @pl.when((c == 1) & has_earlier)
            def _():
                with phase("rim_out"):
                    rim_out0(j).wait_recv()
                    rim_in0(j).start()

        for j in range(n0):
            with phase("rim_in"):
                when((c == 0) & has_earlier, rim_in0(j).wait_recv)

        @pl.when(has_earlier)
        def _():
            def fill(i):
                raw[rows + i, :tiles, :] = rim_in[i]

            clear(rows, fill)

    own_base, far_base = zb * 2 * rows, (1 - zb) * 2 * rows
    up_base = 2 * rows
    def entry(table, first, base, u):
        return table[first + (base >> 7), (base & (LANES - 1)) + u]

    def value0(base, u):
        word = entry(plan, 0, base, u)
        lo, up, d = word & 511, (word >> 9) & 511, (word >> 18) & 1023
        total = raw[lo, tiles:, :] + delayed(raw, up, d, tiles - rim0)
        return jnp.where((word >> 28) == 1, total, zero)

    split = tiles // 2

    def store0(m, v):
        mine[m] = v
        cur[own_base + c * rows + m, tiles:, :] = v

    def store_mine(m, v):
        mine[m] = v

    def store_head(m, v):
        mine[m, split:, :] = v[split:, :]

    def store_tail(m, v):
        mine[m, :split, :] = v[:split, :]

    rim1 = 2 * rows // LANES

    def value1(kind):
        def value(base, u):
            word = entry(picks, kind * (rows // LANES), base, u)
            a, b, d = word & 511, (word >> 9) & 511, (word >> 18) & 1023
            total = cur[a, tiles:, :] + delayed(cur, up_base + b, d, tiles - rim1)
            return jnp.where((word >> 28) == 1, total, zero)

        return value

    def store_picked(kind):
        def store(m, v):
            picked[kind, m] = v

        return store

    def store_land(m, v):
        land[half, m] = v

    def join(m):
        joined[m, :tiles, :] = early[m]
        joined[m, tiles:, :] = land[1, m]

    def value2(base, u):
        word = entry(plan, rows // LANES, base, u)
        total = land[0, base + u] + delayed(joined, base + u, word & 4095, 0)
        return jnp.where((word >> 12) == 1, total, zero)

    def store2(m, v):
        final[m] = v

    def finish(first, count, prepare, value):
        def step(i, carry):
            start = pl.multiple_of(first + i * FINE, FINE)
            if prepare is not None:
                for u in range(FINE):
                    prepare(start + u)
            blocks(start, FINE, value, store2)
            for tile in range(tiles):
                at_tile = pl.ds(tile * LANES, LANES)
                out_ref[pl.ds(start, FINE), at_tile] = final[pl.ds(start, FINE), tile, :]
            return carry

        lax.fori_loop(0, count // FINE, step, 0)

    rim = pl.ds(tiles - rim1, rim1)
    every = pl.ds(0, rows)

    def flow(index, src, dst, sems, target):
        def copy(j, group=1):
            at_rows = span(j, group)
            return remote(src(at_rows), dst(at_rows), index, sems.at[j], target)

        copy.coarse = lambda j: remote(src(coarse(j)), dst(coarse(j)), index, sems.at[j], target)
        copy.fine = lambda j: remote(src(fine(j)), dst(fine(j)), index, sems.at[lax.div(j, n_fine // sems.shape[0])], target)

        return copy, remote(src(every), dst(every), index, sems.at[0], target)

    lead, trail = pl.ds(split, tiles - split), pl.ds(0, split)
    head, head_all = flow(3, lambda r: mine.at[r, lead], lambda r: far_in.at[r, lead], s_head, near)
    far, far_all = flow(12, lambda r: mine.at[r, trail], lambda r: far_in.at[r, trail], s_far, near)
    far_on, far_on_all = flow(4, lambda r: far_in.at[r], lambda r: far_pass.at[r], s_far_pass, partner)
    own1, own1_all = flow(5, lambda r: mine.at[r], lambda r: own_in.at[r], s_own, partner)
    halo_mine, halo_all = flow(6, lambda r: mine.at[r, rim], lambda r: halo_in.at[r, rim], s_halo, later)
    halo_far, _ = flow(6, lambda r: far_in.at[r, rim], lambda r: halo_in.at[r, rim], s_halo, later)
    halo_on, halo_on_all = flow(7, lambda r: halo_in.at[r, rim], lambda r: halo_pass.at[r, rim], s_halo_pass, partner)
    to_half = lambda h: lambda r: land.at[h, r]
    _, far_outer_all = flow(8, lambda r: picked.at[0, r], to_half(half), s_fo, across)
    far_outer = lambda j: remote(
        picked.at[0, span(j)], land.at[half, span(j)], 8, s_fo.at[lax.div(j * chunk, COARSE)], across
    )
    near_outer, near_outer_all = flow(9, lambda r: picked.at[1, r], to_half(half), s_last, near)
    far_inner, far_inner_all = flow(10, lambda r: picked.at[2, r], to_half(half), s_last, facing)
    got_across, _ = flow(8, lambda r: picked.at[0, r], to_half(1 - half), s_fo, across)
    got_facing, _ = flow(10, lambda r: picked.at[2, r], to_half(1 - half), s_last, facing)
    edge, edge_all = flow(11, lambda r: land.at[1, r], lambda r: early.at[r], s_edge, later)

    def loop(name, count, body):
        def step(j, carry):
            with phase(name):
                body(j)
            return carry

        lax.fori_loop(0, count, step, 0)

    last_rows = zb == 1
    pieces = chunk // FINE
    taken = (n_fine - 1 - REST_FIRST) // REST_STEP + 1

    n_plain = n - CROSS
    cross_row = n_plain * chunk
    joins_here = outer | (half == 1)
    whole = pl.ds(0, CROSS * chunk)
    cross = remote(cross_own.at[whole], cross_in.at[whole], 13, s_cross.at[0], later)

    def take(j):
        when(inner, got_facing.fine(j).wait_recv)
        when(outer, near_outer.fine(j).wait_recv)
        when(last_rows & has_later & (joins_here | (j < n_plain * pieces)), edge.fine(j).start)

    def store_cross(m, v):
        cross_own[m - cross_row] = v

    def cross_value(base, u):
        word = entry(plan, rows // LANES + 1, base, u)
        return delayed(joined, base + u, word, 0)

    def plain_value(base, u):
        word = entry(plan, rows // LANES, base, u)
        return jnp.where((word >> 12) == 1, land[0, base + u] + land[1, base + u], zero)

    def send_crossed(first):
        for u in range(FINE):
            joined[first + u, :tiles, :] = cross_in[first - cross_row + u]
            joined[first + u, tiles:, :] = cross_own[first - cross_row + u]
        blocks(first, FINE, cross_value, store_picked(2))

    def keep_own(p):
        blocks(p * chunk, chunk, value1(3), store_land)

    def receive(p):
        @pl.when(p < n)
        def _():
            for i in range(pieces):
                j = p * pieces + i
                when(outer | (half == 1) | (j >= taken), functools.partial(take, j))

        when(inner & (half == 0) & (p < n - OWN_LEAD), functools.partial(keep_own, p + OWN_LEAD))

        @pl.when(p >= EDGE_LAG)
        def _():
            k = p - EDGE_LAG
            joins = joins_here | (k < n_plain)

            @pl.when(joins)
            def _():
                when(has_earlier, edge(k).wait_recv)
                finish(k * chunk, chunk, join, value2)

            @pl.when(jnp.logical_not(joins))
            def _():
                finish(k * chunk, chunk, None, plain_value)

    when(inner, place_rows)
    when(inner, pick_rows)
    for j in range(n0):
        with phase("own0"):
            own0(j, (1 - c) * rows).wait_recv()
    pltpu.make_async_copy(plan_v, plan, s_plan.at[0]).wait()

    @pl.when(outer)
    def _():
        def send_head(j):
            blocks(j * chunk, chunk, value0, store_head)
            head(j).start()

        loop("heads", HEAD, send_head)
        take_rim()

        def produce(j):
            @pl.when(j < HEAD)
            def _():
                blocks(j * chunk, chunk, value0, store_tail)

            far(j).start()

            @pl.when(j + HEAD < n)
            def _():
                blocks((j + HEAD) * chunk, chunk, value0, store_mine)
                head(j + HEAD).start()

        loop("produce", n, produce)

        def from_across(j):
            got_across.coarse(j).wait_recv()

            @pl.when((half == 0) & has_later)
            def _():
                for i in range(COARSE // FINE):
                    edge.fine(j * (COARSE // FINE) + i).start()

        loop("from_across", rows // COARSE, from_across)

    @pl.when(inner)
    def _():
        def produce(j):
            for i in range(OWN_GROUP):
                blocks((j * OWN_GROUP + i) * chunk, chunk, value0, store0)
                when((half == 0) & has_later, halo_mine(j * OWN_GROUP + i).start)
            own1(j, OWN_GROUP).start()

        take_rim()

        def pass_head(j):
            head(j).wait_recv()
            when((half == 1) & has_later, halo_far(j).start)

        def pass_halo(j):
            @pl.when(has_earlier)
            def _():
                halo_mine(j).wait_recv()
                halo_on(j).start()

        def begin(j):
            when(half == 1, functools.partial(pass_head, j))
            produce(j)

        loop("produce", FIRST_OWN, begin)
        loop("heads", HEAD, lambda j: when((half == 0) | (j >= FIRST_OWN), functools.partial(pass_head, j)))
        pltpu.make_async_copy(picks_v, picks, s_plan.at[1]).wait()
        loop("halos", HEAD - HALO_LAG, pass_halo)

        def gather(k):
            @pl.when(lax.rem(k, OWN_GROUP) == 0)
            def _():
                own1(lax.div(k, OWN_GROUP), OWN_GROUP).wait_recv()

            far_on(k).wait_recv()
            start = pl.multiple_of(k * chunk, chunk)
            mine_at, other_at = c * rows + start, (1 - c) * rows + start
            for u in range(chunk):
                cur[own_base + other_at + u, tiles:, :] = own_in[start + u]
                cur[far_base + mine_at + u, tiles:, :] = far_in[start + u]
                cur[far_base + other_at + u, tiles:, :] = far_pass[start + u]

            @pl.when(has_earlier)
            def _():
                halo_on(k).wait_recv()
                for u in range(chunk):
                    cur[up_base + mine_at + u, :tiles, :] = halo_in[start + u]
                    cur[up_base + other_at + u, :tiles, :] = halo_pass[start + u]

            blocks(k * chunk, chunk, value1(0), store_picked(0))
            far_outer(k).start()

        def stream(j):
            when(j > 0, functools.partial(gather, j - 1))

            @pl.when(j < n)
            def _():
                far(j).wait_recv()
                far_on(j).start()

            when(j < n - HEAD + HALO_LAG, functools.partial(pass_halo, j + HEAD - HALO_LAG))
            when(j < n - HEAD, functools.partial(pass_head, j + HEAD))
            group = lax.div(j, OWN_GROUP) + FIRST_OWN
            when((lax.rem(j, OWN_GROUP) == 0) & (group < n // OWN_GROUP), functools.partial(produce, group))

        loop("stream", n + 1, stream)

        @pl.when(half == 1)
        def _():
            blocks(cross_row, CROSS * chunk, value1(2), store_cross)
            when(has_later, cross.start)

        def rest(j):
            crossed = (half == 1) & (j >= n_plain * pieces)

            @pl.when(crossed)
            def _():
                when(has_earlier & (j == n_plain * pieces), cross.wait_recv)
                send_crossed(pl.multiple_of(j * FINE, FINE))

            @pl.when(jnp.logical_not(crossed))
            def _():
                blocks(j * FINE, FINE, value1(2), store_picked(2))

            far_inner.fine(j).start()
            blocks(j * FINE, FINE, value1(1), store_picked(1))
            near_outer.fine(j).start()

            @pl.when(half == 1)
            def _():
                blocks(j * FINE, FINE, value1(3), store_land)
                when(has_later, edge.fine(j).start)

            turn = j - REST_FIRST

            @pl.when((half == 0) & (turn >= 0) & (lax.rem(jnp.maximum(turn, 0), REST_STEP) == 0))
            def _():
                take(lax.div(turn, REST_STEP))

        loop("rest", n_fine, rest)
        when(half == 0, functools.partial(loop, "own", OWN_LEAD, keep_own))

    loop("receive", n + EDGE_LAG, receive)

    @pl.when(outer)
    def _():
        head_all.wait_send()
        far_all.wait_send()

    @pl.when(inner)
    def _():
        own1_all.wait_send()
        far_on_all.wait_send()
        when(has_later, halo_all.wait_send)
        when(has_earlier, halo_on_all.wait_send)
        far_outer_all.wait_send()
        near_outer_all.wait_send()
        far_inner_all.wait_send()

        when((half == 1) & has_later, cross.wait_send)

    plain = pl.ds(0, cross_row)
    edge_plain = remote(land.at[1, plain], early.at[plain], 11, s_edge.at[0], later)
    when(has_later & joins_here, edge_all.wait_send)
    when(has_later & jnp.logical_not(joins_here), edge_plain.wait_send)
    own0(None, c * rows).wait_send()
    when((c == 1) & has_later, rim_out0(None).wait_send)
    when((c == 1) & has_earlier, rim_in0(None).wait_send)


def per_device_fused(tm_size, band_state, lower_rows, upper_rows, delays, counts):
    row_count, samples = band_state.shape
    tiles = samples // LANES
    n = row_count // CHUNK_ROWS
    dma = pltpu.SemaphoreType.DMA
    wide = pltpu.VMEM((row_count, tiles, LANES), jnp.float32)
    return pl.pallas_call(
        functools.partial(kernel, tiles, tm_size),
        out_shape=pltpu.VMEM((row_count, samples), jnp.float32),
        in_specs=[pl.BlockSpec(memory_space=pltpu.HBM)] * 5,
        out_specs=pl.BlockSpec(memory_space=pltpu.VMEM),
        scratch_shapes=[
            pltpu.VMEM(band_state.shape, jnp.float32),
            pltpu.VMEM(lower_rows.shape, jnp.int32),
            pltpu.VMEM(upper_rows.shape, jnp.int32),
            pltpu.VMEM(delays.shape, jnp.int32),
            pltpu.SMEM(counts.shape, jnp.int32),
            pltpu.VMEM((4 * row_count, LANES), jnp.int32),
            pltpu.VMEM((2 * row_count, LANES), jnp.int32),
            pltpu.VMEM((2 * row_count, LANES), jnp.int32),
            pltpu.VMEM((4 * row_count // LANES, LANES), jnp.int32),
            pltpu.SMEM((4 * row_count // LANES, LANES), jnp.int32),
            pltpu.VMEM((4 * row_count // LANES, LANES), jnp.int32),
            pltpu.SMEM((4 * row_count // LANES, LANES), jnp.int32),
            pltpu.VMEM((2 * row_count, 2 * tiles, LANES), jnp.float32),
            wide,
            wide,
            pltpu.VMEM((4 * row_count, 2 * tiles, LANES), jnp.float32),
            wide, wide, wide, wide, wide,
            pltpu.VMEM((3, row_count, tiles, LANES), jnp.float32),
            pltpu.VMEM((2, row_count, tiles, LANES), jnp.float32),
            wide,
            pltpu.VMEM((CROSS * CHUNK_ROWS, tiles, LANES), jnp.float32),
            pltpu.VMEM((CROSS * CHUNK_ROWS, tiles, LANES), jnp.float32),
            pltpu.VMEM((row_count, 2 * tiles, LANES), jnp.float32),
            wide,
            dma((14,)),
            dma((CHUNKS_0 + 4,)),
            dma((2,)),
            dma((3 * CHUNKS_0,)),
            dma((n,)),
            dma((n,)),
            dma((n,)),
            dma((n // OWN_GROUP,)),
            dma((n,)),
            dma((n,)),
            dma((row_count // COARSE,)),
            dma((row_count // FINE,)),
            dma((n,)),
            dma((1,)),
        ],
        compiler_params=pltpu.CompilerParams(
            collective_id=0, has_side_effects=True, vmem_limit_bytes=58 * 2**20
        ),
    )(band_state, lower_rows, upper_rows, delays, counts)


def solution(mesh):
    if mesh.shape["freq"] == 2**ITERS:
        body = functools.partial(per_device_fused, mesh.shape["tm"])
    else:
        body = per_device_general
    return jax.shard_map(
        body,
        mesh=mesh,
        in_specs=(P("freq", "tm"), P(), P(), P(), P()),
        out_specs=P("freq", "tm"),
        check_vma=False,
    )
```

```python
import contextlib
import functools

import jax
import jax.numpy as jnp
from jax import lax
from jax.experimental import pallas as pl
from jax.experimental.pallas import tpu as pltpu
from jax.sharding import PartitionSpec as P

DMAX = 2048
ITERS = 3
LANES = 128
SUBLANES = 8
UNROLL = 16
CHUNKS_0 = 2
CHUNK_ROWS = 16
HEAD = 2
HALO_LAG = 2
FIRST_OWN = 2
OWN_GROUP = 2
PLAN_UNROLL = 8
EDGE_LAG = 2
REST_FIRST = 9
REST_STEP = 2
OWN_LEAD = 2
CROSS = 2
COARSE = 64
FINE = 16


def shifted_2(block, axis, distance):
    devices = range(lax.axis_size(axis))
    route = [(i - distance, i) for i in devices if i - distance in devices]
    return lax.ppermute(block, axis, route)


def delay_columns(extended, shifts, widest):
    row_count = extended.shape[0]
    for bit_index in range(widest.bit_length()):
        stride = 1 << bit_index
        shifted = jnp.concatenate(
            [jnp.zeros((row_count, stride), extended.dtype), extended[:, :-stride]], axis=1
        )
        extended = jnp.where((shifts >> bit_index & 1)[:, None] == 1, shifted, extended)
    return extended


def live_mask(global_rows, counts, width_out, offset, bands_out):
    band_index = global_rows // width_out
    band_counts = counts[offset : offset + bands_out]
    matches = band_index[:, None] == jnp.arange(bands_out, dtype=jnp.int32)[None, :]
    live_count = jnp.sum(jnp.where(matches, band_counts[None, :], 0), axis=1)
    return global_rows % width_out < live_count


def per_device_general(band_state, lower_rows, upper_rows, delays, counts):
    row_count, samples = band_state.shape
    freq_index = lax.axis_index("freq")
    first_row = freq_index * row_count
    global_rows = first_row + jnp.arange(row_count, dtype=jnp.int32)
    current = band_state
    for iteration in range(ITERS):
        width_in = DMAX >> ITERS - iteration
        width_out = 2 * width_in
        bands_out = DMAX // width_out
        offset = 2**ITERS - 2 ** (ITERS - iteration)
        lower_source = lax.dynamic_slice_in_dim(lower_rows[iteration], first_row, row_count)
        upper_source = lax.dynamic_slice_in_dim(upper_rows[iteration], first_row, row_count)
        own_delays = lax.dynamic_slice_in_dim(delays[iteration], first_row, row_count)
        gathered = lax.all_gather(current, "freq", axis=0, tiled=True)
        lower_values = jnp.take(gathered, lower_source, axis=0)
        upper_values = jnp.take(gathered, upper_source, axis=0)
        rim_columns = shifted_2(upper_values[:, samples - width_in :], "tm", 1)
        extended = jnp.concatenate([rim_columns, upper_values], axis=1)
        delayed = delay_columns(extended, own_delays, width_in)[:, width_in:]
        live_rows = live_mask(global_rows, counts, width_out, offset, bands_out)
        current = jnp.where(live_rows[:, None], lower_values + delayed, jnp.zeros_like(delayed))
    return current


MESH = pl.DeviceIdType.MESH


def phase(name):
    return contextlib.nullcontext()


def kernel(
    tiles, tm_size, x_in, lower_in, upper_in, delays_in, counts_in,
    out_ref, x_ref, lower, upper, delays, counts, columns, columns_0, places, plan_v, plan, picks_v, picks, raw, rim_in, mine, cur, own_in, far_in, far_pass, halo_in, halo_pass,
    picked, land, early, cross_own, cross_in, joined, final,
    sent, s_load, s_plan, s_raw, s_head, s_far, s_far_pass, s_own, s_halo, s_halo_pass, s_fo, s_last, s_edge, s_cross,
):
    f, t = lax.axis_index("freq"), lax.axis_index("tm")
    c, z = lax.rem(f, 2), lax.div(f, 2)
    zb, half = lax.rem(z, 2), lax.div(z, 2)
    rows = x_ref.shape[0]
    chunk = CHUNK_ROWS
    n = rows // chunk
    at = lambda ff, tt: {"freq": ff, "tm": tt}
    partner = at(f + 1 - 2 * c, t)
    near = at(f + 2 - 4 * zb, t)
    across = at(f + 4 - 8 * half, t)
    facing = at(f + 2 - 4 * half, t)
    later = at(f, t + 1)
    earlier = at(f, t - 1)
    inner = zb != half
    outer = zb == half
    has_later, has_earlier = t < tm_size - 1, t > 0

    n0, chunk0 = CHUNKS_0, rows // CHUNKS_0

    def load(j, source, target):
        return pltpu.make_async_copy(source, target, s_load.at[j])

    parts = [pl.ds(j * chunk0, chunk0) for j in range(n0)]
    loads = [load(j, x_in.at[part], x_ref.at[part]) for j, part in enumerate(parts)]
    pairs = ((lower_in, lower), (upper_in, upper), (delays_in, delays), (counts_in, counts))
    table_loads = [load(n0 + j, *pair) for j, pair in enumerate(pairs)]
    for copy in loads + table_loads:
        copy.start()

    barrier = pltpu.get_barrier_semaphore()

    def greet(target):
        pl.semaphore_signal(barrier, inc=1, device_id=target, device_id_type=MESH)

    greet(partner)
    greet(near)
    greet(across)
    for cond, target in ((inner, facing), (has_earlier, earlier), (has_later, later)):
        pl.when(cond)(functools.partial(greet, target))

    lane = lax.broadcasted_iota(jnp.int32, (tiles, LANES), 1)
    zero = jnp.zeros((tiles, LANES), jnp.float32)

    def when(cond, action):
        pl.when(cond)(action)

    def remote(src, dst, flow, sem, target):
        return pltpu.make_async_remote_copy(
            src_ref=src, dst_ref=dst, send_sem=sent.at[flow], recv_sem=sem,
            device_id=target, device_id_type=MESH,
        )

    def span(j, group=1):
        return pl.ds(pl.multiple_of(j * chunk * group, chunk * group), chunk * group)

    n_fine = rows // FINE

    def coarse(j):
        return pl.ds(pl.multiple_of(j * COARSE, COARSE), COARSE)

    def fine(j):
        return pl.ds(pl.multiple_of(j * FINE, FINE), FINE)

    def delayed(source, row, d, first):
        q, r = d >> 7, d & (LANES - 1)
        a = source[row, pl.ds(tiles - q, tiles), :]
        b = source[row, pl.ds(jnp.maximum(tiles - 1 - q, first), tiles), :]
        a, b = pltpu.roll(a, r, 1), pltpu.roll(b, r, 1)
        return jnp.where(lane >= r, a, b)

    def blocks(start, count, value, store):
        def body(base, size):
            values = [(base + u, value(base, u)) for u in range(size)]
            for m, v in values:
                store(m, v)

        def step(i, carry):
            body(start + i * UNROLL, UNROLL)
            return carry

        if count <= UNROLL:
            body(start, count)
        else:
            lax.fori_loop(0, count // UNROLL, step, 0)

    rim0 = rows // LANES
    full0, tail0, kept0 = pl.ds(tiles, tiles), pl.ds(2 * tiles - rim0, rim0), pl.ds(tiles - rim0, rim0)

    def part_of(j, row=0):
        return pl.ds(row, rows) if j is None else pl.ds(row + j * chunk0, chunk0)

    def own0(j, row):
        at_rows = raw.at[part_of(j, row), full0]
        return remote(at_rows, at_rows, 0, s_raw.at[j or 0], partner)

    def rim_out0(j):
        return remote(raw.at[part_of(j, rows), tail0], rim_in.at[part_of(j), kept0], 1, s_raw.at[n0 + (j or 0)], later)

    def rim_in0(j):
        at_rows = rim_in.at[part_of(j), kept0]
        return remote(at_rows, at_rows, 2, s_raw.at[2 * n0 + (j or 0)], partner)

    def spread(first, count, first_tile, last_tile):
        def body(step, carry):
            r = first + step * SUBLANES
            for tile in range(first_tile, last_tile):
                raw[pl.ds(c * rows + r, SUBLANES), tiles + tile, :] = x_ref[
                    pl.ds(r, SUBLANES), pl.ds(tile * LANES, LANES)
                ]
            return carry

        lax.fori_loop(0, count // SUBLANES, body, 0)

    for j in range(n0):
        with phase("spread"):
            loads[j].wait()
            spread(j * chunk0, chunk0, tiles - rim0, tiles)
    one = lambda cond: jnp.where(cond, 1, 0)
    with phase("greet"):
        pl.semaphore_wait(barrier, 3 + one(inner) + one(has_earlier) + one(has_later))
    for j in range(n0):
        when((c == 1) & has_later, rim_out0(j).start)
    for j in range(n0):
        with phase("send0"):
            spread(j * chunk0, chunk0, 0, tiles - rim0)
            own0(j, c * rows).start()

    def clear(count, store):
        def body(i, carry):
            for u in range(UNROLL):
                store(i * UNROLL + u)
            return carry

        lax.fori_loop(0, count // UNROLL, body, 0)

    @pl.when(t == 0)
    def _():
        def clear_raw(i):
            raw[rows + i, :tiles, :] = zero

        def clear_cur(i):
            cur[2 * rows + i, :tiles, :] = zero

        def clear_early(i):
            early[i] = zero

        clear(rows, clear_raw)
        clear(2 * rows, clear_cur)
        clear(rows, clear_early)

        def clear_cross(i):
            cross_in[i] = zero

        clear(CROSS * CHUNK_ROWS, clear_cross)

    chip_rows, half_rows = 2 * rows, 4 * rows
    flat = (SUBLANES, LANES)
    lane_at = lax.broadcasted_iota(jnp.int32, flat, 1)
    line_at = lax.broadcasted_iota(jnp.int32, flat, 0)
    none = jnp.zeros(flat, jnp.int32)
    groups = lambda count: range(count // LANES)

    def row_of(table, level, start):
        return jnp.broadcast_to(table[level : level + 1, pl.ds(pl.multiple_of(start, LANES), LANES)], flat)

    def wanted(start):
        return jnp.where(half == 0, row_of(lower, ITERS - 1, start), row_of(upper, ITERS - 1, start)) & (half_rows - 1)

    def set_columns(target, start, row):
        target[pl.ds(start, LANES), :] = jnp.broadcast_to(row[0:1], (LANES, LANES)).T

    def fold(values, combine):
        for s in (4, 2, 1):
            values = [combine(v, pltpu.roll(v, s, 0)) for v in values]
        return values

    def scan(count, init, step):
        def body(i, carry):
            for u in range(PLAN_UNROLL):
                at_row = (i * PLAN_UNROLL + u) * SUBLANES
                carry = step(pl.multiple_of(at_row, SUBLANES), line_at + at_row, carry)
            return carry

        return lax.fori_loop(0, count // SUBLANES // PLAN_UNROLL, body, init)

    add, least = lambda a, b: a + b, jnp.minimum
    bit = lambda cond, place: jnp.where(cond, 1 << place, 0)

    def find_order():
        for g in groups(half_rows):
            start = half * half_rows + g * LANES
            low, high = row_of(lower, 1, start), row_of(upper, 1, start)
            set_columns(columns, g * LANES, (low & (chip_rows - 1)) | (high & (chip_rows - 1)) << 9)
        want = [wanted((1 - half) * 3 * chip_rows + g * LANES) for g in groups(chip_rows)]

        def use(at_row, index, carry):
            line = columns[pl.ds(at_row, SUBLANES), :]
            return tuple(v + jnp.where(w == index, line, 0) for v, w in zip(carry, want))

        used = fold(scan(half_rows, (none,) * len(want), use), add)
        for g, row in enumerate(used):
            set_columns(columns, g * LANES, row)

        def meet(at_row, index, carry):
            line = columns[pl.ds(at_row, SUBLANES), :]
            low, high = line & (chip_rows - 1), line >> 9
            turn = 2 * (index & (rows - 1)) + lax.div(index, rows)
            hits = [(part, g) for part in (low, high) for g in groups(chip_rows)]
            return tuple(
                least(v, jnp.where(part == lane_at + g * LANES, turn, chip_rows)) for v, (part, g) in zip(carry, hits)
            )

        never = jnp.full(flat, chip_rows, jnp.int32)
        first = fold(scan(chip_rows, (never,) * (2 * len(want)), meet), least)
        keys = [v * chip_rows + lane_at + (g % len(want)) * LANES for g, v in enumerate(first)]
        for g, row in enumerate(keys):
            set_columns(columns, g * LANES, row)

        def count(at_row, index, carry):
            low = columns[pl.ds(at_row, SUBLANES), :]
            high = columns[pl.ds(chip_rows + at_row, SUBLANES), :]
            parts = [low] * len(want) + [high] * len(want)
            return tuple(v + jnp.where(part < key, 1, 0) for v, part, key in zip(carry, parts, keys))

        ranks = fold(scan(chip_rows, (none,) * len(keys), count), add)
        place = [(v & 1) * rows + (v >> 1) for v in ranks]
        for g in groups(chip_rows):
            low, high = place[g], place[len(want) + g]
            set_columns(places, g * LANES, low | high << 9)
            start = z * chip_rows + g * LANES
            low, high = row_of(lower, 0, start), row_of(upper, 0, start)
            live = bit(lane_at + g * LANES < counts[z], 28)
            word = (low & (chip_rows - 1)) | (high & (chip_rows - 1)) << 9 | row_of(delays, 0, start) << 18 | live
            set_columns(columns_0, g * LANES, word)

        def pick(at_row, index, carry):
            line = places[pl.ds(at_row, SUBLANES), :]
            own = jnp.where(zb == 0, line & (chip_rows - 1), line >> 9)
            word = columns_0[pl.ds(at_row, SUBLANES), :]
            return tuple(
                v + jnp.where(own == lane_at + (c * rows + g * LANES), word, 0) for g, v in enumerate(carry)
            )

        words = fold(scan(chip_rows, (none,) * len(groups(rows)), pick), add)
        for g, row in enumerate(words):
            plan_v[pl.ds(g, 1), :] = row[0:1]
            start = f * rows + g * LANES
            live = bit(lane_at + start < counts[2**ITERS - 2], 12)
            plan_v[pl.ds(rows // LANES + g, 1), :] = (row_of(delays, 2, start) | live)[0:1]
        facing_end = (f + 2 - 4 * half) * rows + rows - LANES
        plan_v[pl.ds(2 * rows // LANES, 1), :] = row_of(delays, 2, facing_end)[0:1]
        pltpu.make_async_copy(plan_v, plan, s_plan.at[0]).start()

    def place_rows():
        marks = [half * half_rows + g * LANES for g in groups(half_rows)]
        low = [row_of(lower, 1, start) & (chip_rows - 1) for start in marks]
        high = [row_of(upper, 1, start) & (chip_rows - 1) for start in marks]

        def put(at_row, index, carry):
            line = places[pl.ds(at_row, SUBLANES), :]
            shifted = line >> 9 << 9
            line = line & (chip_rows - 1)
            return tuple(
                v + jnp.where(a == index, line, 0) + jnp.where(b == index, shifted, 0)
                for v, a, b in zip(carry, low, high)
            )

        words = fold(scan(chip_rows, (none,) * len(marks), put), add)
        for g, (start, word) in enumerate(zip(marks, words)):
            live = bit(lane_at + g * LANES < counts[2 ** (ITERS - 1) + half], 28)
            set_columns(columns, g * LANES, word | row_of(delays, 1, start) << 18 | live)

    def pick_rows():
        targets = (f + 4 - 8 * half, f + 2 - 4 * zb, f + 2 - 4 * half, f)
        want = [wanted(target * rows + g * LANES) for target in targets for g in groups(rows)]

        def pick(at_row, index, carry):
            line = columns[pl.ds(at_row, SUBLANES), :]
            return tuple(v + jnp.where(w == index, line, 0) for v, w in zip(carry, want))

        words = fold(scan(half_rows, (none,) * len(want), pick), add)
        for g, row in enumerate(words):
            picks_v[pl.ds(g, 1), :] = row[0:1]
        pltpu.make_async_copy(picks_v, picks, s_plan.at[1]).start()

    with phase("order"):
        for copy in table_loads:
            copy.wait()
        find_order()

    def take_rim():
        for j in range(n0):

            @pl.when((c == 1) & has_earlier)
            def _():
                with phase("rim_out"):
                    rim_out0(j).wait_recv()
                    rim_in0(j).start()

        for j in range(n0):
            with phase("rim_in"):
                when((c == 0) & has_earlier, rim_in0(j).wait_recv)

        @pl.when(has_earlier)
        def _():
            def fill(i):
                raw[rows + i, :tiles, :] = rim_in[i]

            clear(rows, fill)

    own_base, far_base = zb * 2 * rows, (1 - zb) * 2 * rows
    up_base = 2 * rows
    def entry(table, first, base, u):
        return table[first + (base >> 7), (base & (LANES - 1)) + u]

    def value0(base, u):
        word = entry(plan, 0, base, u)
        lo, up, d = word & 511, (word >> 9) & 511, (word >> 18) & 1023
        total = raw[lo, tiles:, :] + delayed(raw, up, d, tiles - rim0)
        return jnp.where((word >> 28) == 1, total, zero)

    split = tiles // 2

    def store0(m, v):
        mine[m] = v
        cur[own_base + c * rows + m, tiles:, :] = v

    def store_mine(m, v):
        mine[m] = v

    def store_head(m, v):
        mine[m, split:, :] = v[split:, :]

    def store_tail(m, v):
        mine[m, :split, :] = v[:split, :]

    rim1 = 2 * rows // LANES

    def value1(kind):
        def value(base, u):
            word = entry(picks, kind * (rows // LANES), base, u)
            a, b, d = word & 511, (word >> 9) & 511, (word >> 18) & 1023
            total = cur[a, tiles:, :] + delayed(cur, up_base + b, d, tiles - rim1)
            return jnp.where((word >> 28) == 1, total, zero)

        return value

    def store_picked(kind):
        def store(m, v):
            picked[kind, m] = v

        return store

    def store_land(m, v):
        land[half, m] = v

    def join(m):
        joined[m, :tiles, :] = early[m]
        joined[m, tiles:, :] = land[1, m]

    def value2(base, u):
        word = entry(plan, rows // LANES, base, u)
        total = land[0, base + u] + delayed(joined, base + u, word & 4095, 0)
        return jnp.where((word >> 12) == 1, total, zero)

    def store2(m, v):
        final[m] = v

    def finish(first, count, prepare, value):
        def step(i, carry):
            start = pl.multiple_of(first + i * FINE, FINE)
            if prepare is not None:
                for u in range(FINE):
                    prepare(start + u)
            blocks(start, FINE, value, store2)
            for tile in range(tiles):
                at_tile = pl.ds(tile * LANES, LANES)
                out_ref[pl.ds(start, FINE), at_tile] = final[pl.ds(start, FINE), tile, :]
            return carry

        lax.fori_loop(0, count // FINE, step, 0)

    rim = pl.ds(tiles - rim1, rim1)
    every = pl.ds(0, rows)

    def flow(index, src, dst, sems, target):
        def copy(j, group=1):
            at_rows = span(j, group)
            return remote(src(at_rows), dst(at_rows), index, sems.at[j], target)

        copy.coarse = lambda j: remote(src(coarse(j)), dst(coarse(j)), index, sems.at[j], target)
        copy.fine = lambda j: remote(src(fine(j)), dst(fine(j)), index, sems.at[lax.div(j, n_fine // sems.shape[0])], target)

        return copy, remote(src(every), dst(every), index, sems.at[0], target)

    lead, trail = pl.ds(split, tiles - split), pl.ds(0, split)
    head, head_all = flow(3, lambda r: mine.at[r, lead], lambda r: far_in.at[r, lead], s_head, near)
    far, far_all = flow(12, lambda r: mine.at[r, trail], lambda r: far_in.at[r, trail], s_far, near)
    far_on, far_on_all = flow(4, lambda r: far_in.at[r], lambda r: far_pass.at[r], s_far_pass, partner)
    own1, own1_all = flow(5, lambda r: mine.at[r], lambda r: own_in.at[r], s_own, partner)
    halo_mine, halo_all = flow(6, lambda r: mine.at[r, rim], lambda r: halo_in.at[r, rim], s_halo, later)
    halo_far, _ = flow(6, lambda r: far_in.at[r, rim], lambda r: halo_in.at[r, rim], s_halo, later)
    halo_on, halo_on_all = flow(7, lambda r: halo_in.at[r, rim], lambda r: halo_pass.at[r, rim], s_halo_pass, partner)
    to_half = lambda h: lambda r: land.at[h, r]
    _, far_outer_all = flow(8, lambda r: picked.at[0, r], to_half(half), s_fo, across)
    far_outer = lambda j: remote(
        picked.at[0, span(j)], land.at[half, span(j)], 8, s_fo.at[lax.div(j * chunk, COARSE)], across
    )
    near_outer, near_outer_all = flow(9, lambda r: picked.at[1, r], to_half(half), s_last, near)
    far_inner, far_inner_all = flow(10, lambda r: picked.at[2, r], to_half(half), s_last, facing)
    got_across, _ = flow(8, lambda r: picked.at[0, r], to_half(1 - half), s_fo, across)
    got_facing, _ = flow(10, lambda r: picked.at[2, r], to_half(1 - half), s_last, facing)
    edge, edge_all = flow(11, lambda r: land.at[1, r], lambda r: early.at[r], s_edge, later)

    def loop(name, count, body):
        def step(j, carry):
            with phase(name):
                body(j)
            return carry

        lax.fori_loop(0, count, step, 0)

    last_rows = zb == 1
    pieces = chunk // FINE
    taken = (n_fine - 1 - REST_FIRST) // REST_STEP + 1

    n_plain = n - CROSS
    cross_row = n_plain * chunk
    joins_here = outer | (half == 1)
    whole = pl.ds(0, CROSS * chunk)
    cross = remote(cross_own.at[whole], cross_in.at[whole], 13, s_cross.at[0], later)

    def take(j):
        when(inner, got_facing.fine(j).wait_recv)
        when(outer, near_outer.fine(j).wait_recv)
        when(last_rows & has_later & (joins_here | (j < n_plain * pieces)), edge.fine(j).start)

    def store_cross(m, v):
        cross_own[m - cross_row] = v

    def cross_value(base, u):
        word = entry(plan, rows // LANES + 1, base, u)
        return delayed(joined, base + u, word, 0)

    def plain_value(base, u):
        word = entry(plan, rows // LANES, base, u)
        return jnp.where((word >> 12) == 1, land[0, base + u] + land[1, base + u], zero)

    def send_crossed(first):
        for u in range(FINE):
            joined[first + u, :tiles, :] = cross_in[first - cross_row + u]
            joined[first + u, tiles:, :] = cross_own[first - cross_row + u]
        blocks(first, FINE, cross_value, store_picked(2))

    def keep_own(p):
        blocks(p * chunk, chunk, value1(3), store_land)

    def receive(p):
        @pl.when(p < n)
        def _():
            for i in range(pieces):
                j = p * pieces + i
                when(outer | (half == 1) | (j >= taken), functools.partial(take, j))

        when(inner & (half == 0) & (p < n - OWN_LEAD), functools.partial(keep_own, p + OWN_LEAD))

        k = p - jnp.where(last_rows, EDGE_LAG, 0)

        @pl.when((k >= 0) & (k < n))
        def _():
            joins = joins_here | (k < n_plain)

            @pl.when(joins)
            def _():
                when(has_earlier, edge(k).wait_recv)
                finish(k * chunk, chunk, join, value2)

            @pl.when(jnp.logical_not(joins))
            def _():
                finish(k * chunk, chunk, None, plain_value)

    when(inner, place_rows)
    when(inner, pick_rows)
    for j in range(n0):
        with phase("own0"):
            own0(j, (1 - c) * rows).wait_recv()
    pltpu.make_async_copy(plan_v, plan, s_plan.at[0]).wait()

    @pl.when(outer)
    def _():
        def send_head(j):
            blocks(j * chunk, chunk, value0, store_head)
            head(j).start()

        loop("heads", HEAD, send_head)
        take_rim()

        def produce(j):
            @pl.when(j < HEAD)
            def _():
                blocks(j * chunk, chunk, value0, store_tail)

            far(j).start()

            @pl.when(j + HEAD < n)
            def _():
                blocks((j + HEAD) * chunk, chunk, value0, store_mine)
                head(j + HEAD).start()

        loop("produce", n, produce)

        def from_across(j):
            got_across.coarse(j).wait_recv()

            @pl.when((half == 0) & has_later)
            def _():
                for i in range(COARSE // FINE):
                    edge.fine(j * (COARSE // FINE) + i).start()

        loop("from_across", rows // COARSE, from_across)

    @pl.when(inner)
    def _():
        def produce(j):
            for i in range(OWN_GROUP):
                blocks((j * OWN_GROUP + i) * chunk, chunk, value0, store0)
                when((half == 0) & has_later, halo_mine(j * OWN_GROUP + i).start)
            own1(j, OWN_GROUP).start()

        take_rim()

        def pass_head(j):
            head(j).wait_recv()
            when((half == 1) & has_later, halo_far(j).start)

        def pass_halo(j):
            @pl.when(has_earlier)
            def _():
                halo_mine(j).wait_recv()
                halo_on(j).start()

        def begin(j):
            when(half == 1, functools.partial(pass_head, j))
            produce(j)

        loop("produce", FIRST_OWN, begin)
        loop("heads", HEAD, lambda j: when((half == 0) | (j >= FIRST_OWN), functools.partial(pass_head, j)))
        pltpu.make_async_copy(picks_v, picks, s_plan.at[1]).wait()
        loop("halos", HEAD - HALO_LAG, pass_halo)

        def gather(k):
            @pl.when(lax.rem(k, OWN_GROUP) == 0)
            def _():
                own1(lax.div(k, OWN_GROUP), OWN_GROUP).wait_recv()

            far_on(k).wait_recv()
            start = pl.multiple_of(k * chunk, chunk)
            mine_at, other_at = c * rows + start, (1 - c) * rows + start
            for u in range(chunk):
                cur[own_base + other_at + u, tiles:, :] = own_in[start + u]
                cur[far_base + mine_at + u, tiles:, :] = far_in[start + u]
                cur[far_base + other_at + u, tiles:, :] = far_pass[start + u]

            @pl.when(has_earlier)
            def _():
                halo_on(k).wait_recv()
                for u in range(chunk):
                    cur[up_base + mine_at + u, :tiles, :] = halo_in[start + u]
                    cur[up_base + other_at + u, :tiles, :] = halo_pass[start + u]

            blocks(k * chunk, chunk, value1(0), store_picked(0))
            far_outer(k).start()

        def stream(j):
            when(j > 0, functools.partial(gather, j - 1))

            @pl.when(j < n)
            def _():
                far(j).wait_recv()
                far_on(j).start()

            when(j < n - HEAD + HALO_LAG, functools.partial(pass_halo, j + HEAD - HALO_LAG))
            when(j < n - HEAD, functools.partial(pass_head, j + HEAD))
            group = lax.div(j, OWN_GROUP) + FIRST_OWN
            when((lax.rem(j, OWN_GROUP) == 0) & (group < n // OWN_GROUP), functools.partial(produce, group))

        loop("stream", n + 1, stream)

        @pl.when(half == 1)
        def _():
            blocks(cross_row, CROSS * chunk, value1(2), store_cross)
            when(has_later, cross.start)

        def rest(j):
            crossed = (half == 1) & (j >= n_plain * pieces)

            @pl.when(crossed)
            def _():
                when(has_earlier & (j == n_plain * pieces), cross.wait_recv)
                send_crossed(pl.multiple_of(j * FINE, FINE))

            @pl.when(jnp.logical_not(crossed))
            def _():
                blocks(j * FINE, FINE, value1(2), store_picked(2))

            far_inner.fine(j).start()
            blocks(j * FINE, FINE, value1(1), store_picked(1))
            near_outer.fine(j).start()

            @pl.when(half == 1)
            def _():
                blocks(j * FINE, FINE, value1(3), store_land)
                when(has_later, edge.fine(j).start)

            turn = j - REST_FIRST

            @pl.when((half == 0) & (turn >= 0) & (lax.rem(jnp.maximum(turn, 0), REST_STEP) == 0))
            def _():
                take(lax.div(turn, REST_STEP))

        loop("rest", n_fine, rest)
        when(half == 0, functools.partial(loop, "own", OWN_LEAD, keep_own))

    loop("receive", n + EDGE_LAG, receive)

    @pl.when(outer)
    def _():
        head_all.wait_send()
        far_all.wait_send()

    @pl.when(inner)
    def _():
        own1_all.wait_send()
        far_on_all.wait_send()
        when(has_later, halo_all.wait_send)
        when(has_earlier, halo_on_all.wait_send)
        far_outer_all.wait_send()
        near_outer_all.wait_send()
        far_inner_all.wait_send()

        when((half == 1) & has_later, cross.wait_send)

    plain = pl.ds(0, cross_row)
    edge_plain = remote(land.at[1, plain], early.at[plain], 11, s_edge.at[0], later)
    when(has_later & joins_here, edge_all.wait_send)
    when(has_later & jnp.logical_not(joins_here), edge_plain.wait_send)
    own0(None, c * rows).wait_send()
    when((c == 1) & has_later, rim_out0(None).wait_send)
    when((c == 1) & has_earlier, rim_in0(None).wait_send)


def per_device_fused(tm_size, band_state, lower_rows, upper_rows, delays, counts):
    row_count, samples = band_state.shape
    tiles = samples // LANES
    n = row_count // CHUNK_ROWS
    dma = pltpu.SemaphoreType.DMA
    wide = pltpu.VMEM((row_count, tiles, LANES), jnp.float32)
    return pl.pallas_call(
        functools.partial(kernel, tiles, tm_size),
        out_shape=pltpu.VMEM((row_count, samples), jnp.float32),
        in_specs=[pl.BlockSpec(memory_space=pltpu.HBM)] * 5,
        out_specs=pl.BlockSpec(memory_space=pltpu.VMEM),
        scratch_shapes=[
            pltpu.VMEM(band_state.shape, jnp.float32),
            pltpu.VMEM(lower_rows.shape, jnp.int32),
            pltpu.VMEM(upper_rows.shape, jnp.int32),
            pltpu.VMEM(delays.shape, jnp.int32),
            pltpu.SMEM(counts.shape, jnp.int32),
            pltpu.VMEM((4 * row_count, LANES), jnp.int32),
            pltpu.VMEM((2 * row_count, LANES), jnp.int32),
            pltpu.VMEM((2 * row_count, LANES), jnp.int32),
            pltpu.VMEM((4 * row_count // LANES, LANES), jnp.int32),
            pltpu.SMEM((4 * row_count // LANES, LANES), jnp.int32),
            pltpu.VMEM((4 * row_count // LANES, LANES), jnp.int32),
            pltpu.SMEM((4 * row_count // LANES, LANES), jnp.int32),
            pltpu.VMEM((2 * row_count, 2 * tiles, LANES), jnp.float32),
            wide,
            wide,
            pltpu.VMEM((4 * row_count, 2 * tiles, LANES), jnp.float32),
            wide, wide, wide, wide, wide,
            pltpu.VMEM((3, row_count, tiles, LANES), jnp.float32),
            pltpu.VMEM((2, row_count, tiles, LANES), jnp.float32),
            wide,
            pltpu.VMEM((CROSS * CHUNK_ROWS, tiles, LANES), jnp.float32),
            pltpu.VMEM((CROSS * CHUNK_ROWS, tiles, LANES), jnp.float32),
            pltpu.VMEM((row_count, 2 * tiles, LANES), jnp.float32),
            wide,
            dma((14,)),
            dma((CHUNKS_0 + 4,)),
            dma((2,)),
            dma((3 * CHUNKS_0,)),
            dma((n,)),
            dma((n,)),
            dma((n,)),
            dma((n // OWN_GROUP,)),
            dma((n,)),
            dma((n,)),
            dma((row_count // COARSE,)),
            dma((row_count // FINE,)),
            dma((n,)),
            dma((1,)),
        ],
        compiler_params=pltpu.CompilerParams(
            collective_id=0, has_side_effects=True, vmem_limit_bytes=58 * 2**20
        ),
    )(band_state, lower_rows, upper_rows, delays, counts)


def solution(mesh):
    if mesh.shape["freq"] == 2**ITERS:
        body = functools.partial(per_device_fused, mesh.shape["tm"])
    else:
        body = per_device_general
    return jax.shard_map(
        body,
        mesh=mesh,
        in_specs=(P("freq", "tm"), P(), P(), P(), P()),
        out_specs=P("freq", "tm"),
        check_vma=False,
    )
```

```python
import contextlib
import functools

import jax
import jax.numpy as jnp
from jax import lax
from jax.experimental import pallas as pl
from jax.experimental.pallas import tpu as pltpu
from jax.sharding import PartitionSpec as P

DMAX = 2048
ITERS = 3
LANES = 128
SUBLANES = 8
UNROLL = 16
CHUNKS_0 = 2
CHUNK_ROWS = 16
HEAD = 2
HALO_LAG = 2
FIRST_OWN = 2
OWN_GROUP = 2
PLAN_UNROLL = 8
EDGE_LAG = 2
REST_FIRST = 9
REST_STEP = 2
OWN_LEAD = 2
CROSS = 2
COARSE = 64
FINE = 16


def shifted_2(block, axis, distance):
    devices = range(lax.axis_size(axis))
    route = [(i - distance, i) for i in devices if i - distance in devices]
    return lax.ppermute(block, axis, route)


def delay_columns(extended, shifts, widest):
    row_count = extended.shape[0]
    for bit_index in range(widest.bit_length()):
        stride = 1 << bit_index
        shifted = jnp.concatenate(
            [jnp.zeros((row_count, stride), extended.dtype), extended[:, :-stride]], axis=1
        )
        extended = jnp.where((shifts >> bit_index & 1)[:, None] == 1, shifted, extended)
    return extended


def live_mask(global_rows, counts, width_out, offset, bands_out):
    band_index = global_rows // width_out
    band_counts = counts[offset : offset + bands_out]
    matches = band_index[:, None] == jnp.arange(bands_out, dtype=jnp.int32)[None, :]
    live_count = jnp.sum(jnp.where(matches, band_counts[None, :], 0), axis=1)
    return global_rows % width_out < live_count


def per_device_general(band_state, lower_rows, upper_rows, delays, counts):
    row_count, samples = band_state.shape
    freq_index = lax.axis_index("freq")
    first_row = freq_index * row_count
    global_rows = first_row + jnp.arange(row_count, dtype=jnp.int32)
    current = band_state
    for iteration in range(ITERS):
        width_in = DMAX >> ITERS - iteration
        width_out = 2 * width_in
        bands_out = DMAX // width_out
        offset = 2**ITERS - 2 ** (ITERS - iteration)
        lower_source = lax.dynamic_slice_in_dim(lower_rows[iteration], first_row, row_count)
        upper_source = lax.dynamic_slice_in_dim(upper_rows[iteration], first_row, row_count)
        own_delays = lax.dynamic_slice_in_dim(delays[iteration], first_row, row_count)
        gathered = lax.all_gather(current, "freq", axis=0, tiled=True)
        lower_values = jnp.take(gathered, lower_source, axis=0)
        upper_values = jnp.take(gathered, upper_source, axis=0)
        rim_columns = shifted_2(upper_values[:, samples - width_in :], "tm", 1)
        extended = jnp.concatenate([rim_columns, upper_values], axis=1)
        delayed = delay_columns(extended, own_delays, width_in)[:, width_in:]
        live_rows = live_mask(global_rows, counts, width_out, offset, bands_out)
        current = jnp.where(live_rows[:, None], lower_values + delayed, jnp.zeros_like(delayed))
    return current


MESH = pl.DeviceIdType.MESH


def phase(name):
    return contextlib.nullcontext()


def kernel(
    tiles, tm_size, x_in, lower_in, upper_in, delays_in, counts_in,
    out_ref, x_ref, lower, upper, delays, counts, columns, columns_0, places, plan_v, plan, picks_v, picks, raw, rim_in, mine, cur, own_in, far_in, far_pass, halo_in, halo_pass,
    picked, land, early, cross_own, cross_in, joined, final,
    sent, s_load, s_plan, s_raw, s_head, s_far, s_far_pass, s_own, s_halo, s_halo_pass, s_fo, s_last, s_edge, s_cross,
):
    f, t = lax.axis_index("freq"), lax.axis_index("tm")
    c, z = lax.rem(f, 2), lax.div(f, 2)
    zb, half = lax.rem(z, 2), lax.div(z, 2)
    rows = x_ref.shape[0]
    chunk = CHUNK_ROWS
    n = rows // chunk
    at = lambda ff, tt: {"freq": ff, "tm": tt}
    partner = at(f + 1 - 2 * c, t)
    near = at(f + 2 - 4 * zb, t)
    across = at(f + 4 - 8 * half, t)
    facing = at(f + 2 - 4 * half, t)
    later = at(f, t + 1)
    earlier = at(f, t - 1)
    inner = zb != half
    outer = zb == half
    has_later, has_earlier = t < tm_size - 1, t > 0

    n0, chunk0 = CHUNKS_0, rows // CHUNKS_0

    def load(j, source, target):
        return pltpu.make_async_copy(source, target, s_load.at[j])

    parts = [pl.ds(j * chunk0, chunk0) for j in range(n0)]
    loads = [load(j, x_in.at[part], x_ref.at[part]) for j, part in enumerate(parts)]
    pairs = ((lower_in, lower), (upper_in, upper), (delays_in, delays), (counts_in, counts))
    table_loads = [load(n0 + j, *pair) for j, pair in enumerate(pairs)]
    for copy in loads + table_loads:
        copy.start()

    barrier = pltpu.get_barrier_semaphore()

    def greet(target):
        pl.semaphore_signal(barrier, inc=1, device_id=target, device_id_type=MESH)

    greet(partner)
    greet(near)
    greet(across)
    for cond, target in ((inner, facing), (has_earlier, earlier), (has_later, later)):
        pl.when(cond)(functools.partial(greet, target))

    lane = lax.broadcasted_iota(jnp.int32, (tiles, LANES), 1)
    zero = jnp.zeros((tiles, LANES), jnp.float32)

    def when(cond, action):
        pl.when(cond)(action)

    def remote(src, dst, flow, sem, target):
        return pltpu.make_async_remote_copy(
            src_ref=src, dst_ref=dst, send_sem=sent.at[flow], recv_sem=sem,
            device_id=target, device_id_type=MESH,
        )

    def span(j, group=1):
        return pl.ds(pl.multiple_of(j * chunk * group, chunk * group), chunk * group)

    n_fine = rows // FINE

    def coarse(j):
        return pl.ds(pl.multiple_of(j * COARSE, COARSE), COARSE)

    def fine(j):
        return pl.ds(pl.multiple_of(j * FINE, FINE), FINE)

    def delayed(source, row, d, first):
        q, r = d >> 7, d & (LANES - 1)
        a = source[row, pl.ds(tiles - q, tiles), :]
        b = source[row, pl.ds(jnp.maximum(tiles - 1 - q, first), tiles), :]
        a, b = pltpu.roll(a, r, 1), pltpu.roll(b, r, 1)
        return jnp.where(lane >= r, a, b)

    def blocks(start, count, value, store):
        def body(base, size):
            values = [(base + u, value(base, u)) for u in range(size)]
            for m, v in values:
                store(m, v)

        def step(i, carry):
            body(start + i * UNROLL, UNROLL)
            return carry

        if count <= UNROLL:
            body(start, count)
        else:
            lax.fori_loop(0, count // UNROLL, step, 0)

    rim0 = rows // LANES
    full0, tail0, kept0 = pl.ds(tiles, tiles), pl.ds(2 * tiles - rim0, rim0), pl.ds(tiles - rim0, rim0)

    def part_of(j, row=0):
        return pl.ds(row, rows) if j is None else pl.ds(row + j * chunk0, chunk0)

    def own0(j, row):
        at_rows = raw.at[part_of(j, row), full0]
        return remote(at_rows, at_rows, 0, s_raw.at[j or 0], partner)

    def rim_out0(j):
        return remote(raw.at[part_of(j, rows), tail0], rim_in.at[part_of(j), kept0], 1, s_raw.at[n0 + (j or 0)], later)

    def rim_in0(j):
        at_rows = rim_in.at[part_of(j), kept0]
        return remote(at_rows, at_rows, 2, s_raw.at[2 * n0 + (j or 0)], partner)

    def spread(first, count, first_tile, last_tile):
        def body(step, carry):
            r = first + step * SUBLANES
            for tile in range(first_tile, last_tile):
                raw[pl.ds(c * rows + r, SUBLANES), tiles + tile, :] = x_ref[
                    pl.ds(r, SUBLANES), pl.ds(tile * LANES, LANES)
                ]
            return carry

        lax.fori_loop(0, count // SUBLANES, body, 0)

    for j in range(n0):
        with phase("spread"):
            loads[j].wait()
            spread(j * chunk0, chunk0, tiles - rim0, tiles)
    one = lambda cond: jnp.where(cond, 1, 0)
    with phase("greet"):
        pl.semaphore_wait(barrier, 3 + one(inner) + one(has_earlier) + one(has_later))
    for j in range(n0):
        when((c == 1) & has_later, rim_out0(j).start)
    for j in range(n0):
        with phase("send0"):
            spread(j * chunk0, chunk0, 0, tiles - rim0)
            own0(j, c * rows).start()

    def clear(count, store):
        def body(i, carry):
            for u in range(UNROLL):
                store(i * UNROLL + u)
            return carry

        lax.fori_loop(0, count // UNROLL, body, 0)

    chip_rows, half_rows = 2 * rows, 4 * rows
    flat = (SUBLANES, LANES)
    lane_at = lax.broadcasted_iota(jnp.int32, flat, 1)
    line_at = lax.broadcasted_iota(jnp.int32, flat, 0)
    none = jnp.zeros(flat, jnp.int32)
    groups = lambda count: range(count // LANES)

    def row_of(table, level, start):
        return jnp.broadcast_to(table[level : level + 1, pl.ds(pl.multiple_of(start, LANES), LANES)], flat)

    def wanted(start):
        return jnp.where(half == 0, row_of(lower, ITERS - 1, start), row_of(upper, ITERS - 1, start)) & (half_rows - 1)

    def set_columns(target, start, row):
        target[pl.ds(start, LANES), :] = jnp.broadcast_to(row[0:1], (LANES, LANES)).T

    def fold(values, combine):
        for s in (4, 2, 1):
            values = [combine(v, pltpu.roll(v, s, 0)) for v in values]
        return values

    def scan(count, init, step):
        def body(i, carry):
            for u in range(PLAN_UNROLL):
                at_row = (i * PLAN_UNROLL + u) * SUBLANES
                carry = step(pl.multiple_of(at_row, SUBLANES), line_at + at_row, carry)
            return carry

        return lax.fori_loop(0, count // SUBLANES // PLAN_UNROLL, body, init)

    add, least = lambda a, b: a + b, jnp.minimum
    bit = lambda cond, place: jnp.where(cond, 1 << place, 0)

    def find_order():
        for g in groups(half_rows):
            start = half * half_rows + g * LANES
            low, high = row_of(lower, 1, start), row_of(upper, 1, start)
            set_columns(columns, g * LANES, (low & (chip_rows - 1)) | (high & (chip_rows - 1)) << 9)
        want = [wanted((1 - half) * 3 * chip_rows + g * LANES) for g in groups(chip_rows)]

        def use(at_row, index, carry):
            line = columns[pl.ds(at_row, SUBLANES), :]
            return tuple(v + jnp.where(w == index, line, 0) for v, w in zip(carry, want))

        used = fold(scan(half_rows, (none,) * len(want), use), add)
        for g, row in enumerate(used):
            set_columns(columns, g * LANES, row)

        def meet(at_row, index, carry):
            line = columns[pl.ds(at_row, SUBLANES), :]
            low, high = line & (chip_rows - 1), line >> 9
            turn = 2 * (index & (rows - 1)) + lax.div(index, rows)
            hits = [(part, g) for part in (low, high) for g in groups(chip_rows)]
            return tuple(
                least(v, jnp.where(part == lane_at + g * LANES, turn, chip_rows)) for v, (part, g) in zip(carry, hits)
            )

        never = jnp.full(flat, chip_rows, jnp.int32)
        first = fold(scan(chip_rows, (never,) * (2 * len(want)), meet), least)
        keys = [v * chip_rows + lane_at + (g % len(want)) * LANES for g, v in enumerate(first)]
        for g, row in enumerate(keys):
            set_columns(columns, g * LANES, row)

        def count(at_row, index, carry):
            low = columns[pl.ds(at_row, SUBLANES), :]
            high = columns[pl.ds(chip_rows + at_row, SUBLANES), :]
            parts = [low] * len(want) + [high] * len(want)
            return tuple(v + jnp.where(part < key, 1, 0) for v, part, key in zip(carry, parts, keys))

        ranks = fold(scan(chip_rows, (none,) * len(keys), count), add)
        place = [(v & 1) * rows + (v >> 1) for v in ranks]
        for g in groups(chip_rows):
            low, high = place[g], place[len(want) + g]
            set_columns(places, g * LANES, low | high << 9)
            start = z * chip_rows + g * LANES
            low, high = row_of(lower, 0, start), row_of(upper, 0, start)
            live = bit(lane_at + g * LANES < counts[z], 28)
            word = (low & (chip_rows - 1)) | (high & (chip_rows - 1)) << 9 | row_of(delays, 0, start) << 18 | live
            set_columns(columns_0, g * LANES, word)

        def pick(at_row, index, carry):
            line = places[pl.ds(at_row, SUBLANES), :]
            own = jnp.where(zb == 0, line & (chip_rows - 1), line >> 9)
            word = columns_0[pl.ds(at_row, SUBLANES), :]
            return tuple(
                v + jnp.where(own == lane_at + (c * rows + g * LANES), word, 0) for g, v in enumerate(carry)
            )

        words = fold(scan(chip_rows, (none,) * len(groups(rows)), pick), add)
        for g, row in enumerate(words):
            plan_v[pl.ds(g, 1), :] = row[0:1]
            start = f * rows + g * LANES
            live = bit(lane_at + start < counts[2**ITERS - 2], 12)
            plan_v[pl.ds(rows // LANES + g, 1), :] = (row_of(delays, 2, start) | live)[0:1]
        facing_end = (f + 2 - 4 * half) * rows + rows - LANES
        plan_v[pl.ds(2 * rows // LANES, 1), :] = row_of(delays, 2, facing_end)[0:1]
        pltpu.make_async_copy(plan_v, plan, s_plan.at[0]).start()

    def place_rows():
        marks = [half * half_rows + g * LANES for g in groups(half_rows)]
        low = [row_of(lower, 1, start) & (chip_rows - 1) for start in marks]
        high = [row_of(upper, 1, start) & (chip_rows - 1) for start in marks]

        def put(at_row, index, carry):
            line = places[pl.ds(at_row, SUBLANES), :]
            shifted = line >> 9 << 9
            line = line & (chip_rows - 1)
            return tuple(
                v + jnp.where(a == index, line, 0) + jnp.where(b == index, shifted, 0)
                for v, a, b in zip(carry, low, high)
            )

        words = fold(scan(chip_rows, (none,) * len(marks), put), add)
        for g, (start, word) in enumerate(zip(marks, words)):
            live = bit(lane_at + g * LANES < counts[2 ** (ITERS - 1) + half], 28)
            set_columns(columns, g * LANES, word | row_of(delays, 1, start) << 18 | live)

    def pick_rows():
        targets = (f + 4 - 8 * half, f + 2 - 4 * zb, f + 2 - 4 * half, f)
        want = [wanted(target * rows + g * LANES) for target in targets for g in groups(rows)]

        def pick(at_row, index, carry):
            line = columns[pl.ds(at_row, SUBLANES), :]
            return tuple(v + jnp.where(w == index, line, 0) for v, w in zip(carry, want))

        words = fold(scan(half_rows, (none,) * len(want), pick), add)
        for g, row in enumerate(words):
            picks_v[pl.ds(g, 1), :] = row[0:1]
        pltpu.make_async_copy(picks_v, picks, s_plan.at[1]).start()

    with phase("order"):
        for copy in table_loads:
            copy.wait()
        find_order()

    def take_rim():
        for j in range(n0):

            @pl.when((c == 1) & has_earlier)
            def _():
                with phase("rim_out"):
                    rim_out0(j).wait_recv()
                    rim_in0(j).start()

        for j in range(n0):
            with phase("rim_in"):
                when((c == 0) & has_earlier, rim_in0(j).wait_recv)

        @pl.when(has_earlier)
        def _():
            def fill(i):
                raw[rows + i, :tiles, :] = rim_in[i]

            clear(rows, fill)

    own_base, far_base = zb * 2 * rows, (1 - zb) * 2 * rows
    up_base = 2 * rows
    def entry(table, first, base, u):
        return table[first + (base >> 7), (base & (LANES - 1)) + u]

    def value0(base, u):
        word = entry(plan, 0, base, u)
        lo, up, d = word & 511, (word >> 9) & 511, (word >> 18) & 1023
        total = raw[lo, tiles:, :] + delayed(raw, up, d, tiles - rim0)
        return jnp.where((word >> 28) == 1, total, zero)

    split = tiles // 2

    def store0(m, v):
        mine[m] = v
        cur[own_base + c * rows + m, tiles:, :] = v

    def store_mine(m, v):
        mine[m] = v

    def store_head(m, v):
        mine[m, split:, :] = v[split:, :]

    def store_tail(m, v):
        mine[m, :split, :] = v[:split, :]

    rim1 = 2 * rows // LANES

    def value1(kind):
        def value(base, u):
            word = entry(picks, kind * (rows // LANES), base, u)
            a, b, d = word & 511, (word >> 9) & 511, (word >> 18) & 1023
            total = cur[a, tiles:, :] + delayed(cur, up_base + b, d, tiles - rim1)
            return jnp.where((word >> 28) == 1, total, zero)

        return value

    def store_picked(kind):
        def store(m, v):
            picked[kind, m] = v

        return store

    def store_land(m, v):
        land[half, m] = v

    def join(m):
        joined[m, :tiles, :] = early[m]
        joined[m, tiles:, :] = land[1, m]

    def value2(base, u):
        word = entry(plan, rows // LANES, base, u)
        total = land[0, base + u] + delayed(joined, base + u, word & 4095, 0)
        return jnp.where((word >> 12) == 1, total, zero)

    def store2(m, v):
        final[m] = v

    def finish(first, count, prepare, value):
        def step(i, carry):
            start = pl.multiple_of(first + i * FINE, FINE)
            if prepare is not None:
                for u in range(FINE):
                    prepare(start + u)
            blocks(start, FINE, value, store2)
            for tile in range(tiles):
                at_tile = pl.ds(tile * LANES, LANES)
                out_ref[pl.ds(start, FINE), at_tile] = final[pl.ds(start, FINE), tile, :]
            return carry

        lax.fori_loop(0, count // FINE, step, 0)

    rim = pl.ds(tiles - rim1, rim1)
    every = pl.ds(0, rows)

    def flow(index, src, dst, sems, target):
        def copy(j, group=1):
            at_rows = span(j, group)
            return remote(src(at_rows), dst(at_rows), index, sems.at[j], target)

        copy.coarse = lambda j: remote(src(coarse(j)), dst(coarse(j)), index, sems.at[j], target)
        copy.fine = lambda j: remote(src(fine(j)), dst(fine(j)), index, sems.at[lax.div(j, n_fine // sems.shape[0])], target)

        return copy, remote(src(every), dst(every), index, sems.at[0], target)

    lead, trail = pl.ds(split, tiles - split), pl.ds(0, split)
    head, head_all = flow(3, lambda r: mine.at[r, lead], lambda r: far_in.at[r, lead], s_head, near)
    far, far_all = flow(12, lambda r: mine.at[r, trail], lambda r: far_in.at[r, trail], s_far, near)
    far_on, far_on_all = flow(4, lambda r: far_in.at[r], lambda r: far_pass.at[r], s_far_pass, partner)
    own1, own1_all = flow(5, lambda r: mine.at[r], lambda r: own_in.at[r], s_own, partner)
    halo_mine, halo_all = flow(6, lambda r: mine.at[r, rim], lambda r: halo_in.at[r, rim], s_halo, later)
    halo_far, _ = flow(6, lambda r: far_in.at[r, rim], lambda r: halo_in.at[r, rim], s_halo, later)
    halo_on, halo_on_all = flow(7, lambda r: halo_in.at[r, rim], lambda r: halo_pass.at[r, rim], s_halo_pass, partner)
    to_half = lambda h: lambda r: land.at[h, r]
    _, far_outer_all = flow(8, lambda r: picked.at[0, r], to_half(half), s_fo, across)
    far_outer = lambda j: remote(
        picked.at[0, span(j)], land.at[half, span(j)], 8, s_fo.at[lax.div(j * chunk, COARSE)], across
    )
    near_outer, near_outer_all = flow(9, lambda r: picked.at[1, r], to_half(half), s_last, near)
    far_inner, far_inner_all = flow(10, lambda r: picked.at[2, r], to_half(half), s_last, facing)
    got_across, _ = flow(8, lambda r: picked.at[0, r], to_half(1 - half), s_fo, across)
    got_facing, _ = flow(10, lambda r: picked.at[2, r], to_half(1 - half), s_last, facing)
    edge, edge_all = flow(11, lambda r: land.at[1, r], lambda r: early.at[r], s_edge, later)

    def loop(name, count, body):
        def step(j, carry):
            with phase(name):
                body(j)
            return carry

        lax.fori_loop(0, count, step, 0)

    @pl.when(t == 0)
    def _():
        def clear_raw(i):
            raw[rows + i, :tiles, :] = zero

        def clear_cur(i):
            cur[2 * rows + i, :tiles, :] = zero

        def clear_early(i):
            early[i] = zero

        clear(rows, clear_raw)
        when(inner, lambda: clear(2 * rows, clear_cur))
        clear(rows, clear_early)

        def clear_cross(i):
            cross_in[i] = zero

        clear(CROSS * CHUNK_ROWS, clear_cross)

    last_rows = zb == 1
    pieces = chunk // FINE
    taken = (n_fine - 1 - REST_FIRST) // REST_STEP + 1

    n_plain = n - CROSS
    cross_row = n_plain * chunk
    joins_here = outer | (half == 1)
    whole = pl.ds(0, CROSS * chunk)
    cross = remote(cross_own.at[whole], cross_in.at[whole], 13, s_cross.at[0], later)

    def take(j):
        when(inner, got_facing.fine(j).wait_recv)
        when(outer, near_outer.fine(j).wait_recv)
        when(last_rows & has_later & (joins_here | (j < n_plain * pieces)), edge.fine(j).start)

    def store_cross(m, v):
        cross_own[m - cross_row] = v

    def cross_value(base, u):
        word = entry(plan, rows // LANES + 1, base, u)
        return delayed(joined, base + u, word, 0)

    def plain_value(base, u):
        word = entry(plan, rows // LANES, base, u)
        return jnp.where((word >> 12) == 1, land[0, base + u] + land[1, base + u], zero)

    def send_crossed(first):
        for u in range(FINE):
            joined[first + u, :tiles, :] = cross_in[first - cross_row + u]
            joined[first + u, tiles:, :] = cross_own[first - cross_row + u]
        blocks(first, FINE, cross_value, store_picked(2))

    def keep_own(p):
        blocks(p * chunk, chunk, value1(3), store_land)

    def receive(p):
        @pl.when(p < n)
        def _():
            for i in range(pieces):
                j = p * pieces + i
                when(outer | (half == 1) | (j >= taken), functools.partial(take, j))

        when(inner & (half == 0) & (p < n - OWN_LEAD), functools.partial(keep_own, p + OWN_LEAD))

        k = p - jnp.where(last_rows, EDGE_LAG, 0)

        @pl.when((k >= 0) & (k < n))
        def _():
            joins = joins_here | (k < n_plain)

            @pl.when(joins)
            def _():
                when(has_earlier, edge(k).wait_recv)
                finish(k * chunk, chunk, join, value2)

            @pl.when(jnp.logical_not(joins))
            def _():
                finish(k * chunk, chunk, None, plain_value)

    when(inner, place_rows)
    when(inner, pick_rows)
    for j in range(n0):
        with phase("own0"):
            own0(j, (1 - c) * rows).wait_recv()
    pltpu.make_async_copy(plan_v, plan, s_plan.at[0]).wait()

    @pl.when(outer)
    def _():
        def send_head(j):
            blocks(j * chunk, chunk, value0, store_head)
            head(j).start()

        loop("heads", HEAD, send_head)
        take_rim()

        def produce(j):
            @pl.when(j < HEAD)
            def _():
                blocks(j * chunk, chunk, value0, store_tail)

            far(j).start()

            @pl.when(j + HEAD < n)
            def _():
                blocks((j + HEAD) * chunk, chunk, value0, store_mine)
                head(j + HEAD).start()

        loop("produce", n, produce)

        def from_across(j):
            got_across.coarse(j).wait_recv()

            @pl.when((half == 0) & has_later)
            def _():
                for i in range(COARSE // FINE):
                    edge.fine(j * (COARSE // FINE) + i).start()

        loop("from_across", rows // COARSE, from_across)

    @pl.when(inner)
    def _():
        def produce(j):
            for i in range(OWN_GROUP):
                blocks((j * OWN_GROUP + i) * chunk, chunk, value0, store0)
                when((half == 0) & has_later, halo_mine(j * OWN_GROUP + i).start)
            own1(j, OWN_GROUP).start()

        take_rim()

        def pass_head(j):
            head(j).wait_recv()
            when((half == 1) & has_later, halo_far(j).start)

        def pass_halo(j):
            @pl.when(has_earlier)
            def _():
                halo_mine(j).wait_recv()
                halo_on(j).start()

        def begin(j):
            when(half == 1, functools.partial(pass_head, j))
            produce(j)

        loop("produce", FIRST_OWN, begin)
        loop("heads", HEAD, lambda j: when((half == 0) | (j >= FIRST_OWN), functools.partial(pass_head, j)))
        pltpu.make_async_copy(picks_v, picks, s_plan.at[1]).wait()
        loop("halos", HEAD - HALO_LAG, pass_halo)

        def gather(k):
            @pl.when(lax.rem(k, OWN_GROUP) == 0)
            def _():
                own1(lax.div(k, OWN_GROUP), OWN_GROUP).wait_recv()

            far_on(k).wait_recv()
            start = pl.multiple_of(k * chunk, chunk)
            mine_at, other_at = c * rows + start, (1 - c) * rows + start
            for u in range(chunk):
                cur[own_base + other_at + u, tiles:, :] = own_in[start + u]
                cur[far_base + mine_at + u, tiles:, :] = far_in[start + u]
                cur[far_base + other_at + u, tiles:, :] = far_pass[start + u]

            @pl.when(has_earlier)
            def _():
                halo_on(k).wait_recv()
                for u in range(chunk):
                    cur[up_base + mine_at + u, :tiles, :] = halo_in[start + u]
                    cur[up_base + other_at + u, :tiles, :] = halo_pass[start + u]

            blocks(k * chunk, chunk, value1(0), store_picked(0))
            far_outer(k).start()

        def stream(j):
            when(j > 0, functools.partial(gather, j - 1))

            @pl.when(j < n)
            def _():
                far(j).wait_recv()
                far_on(j).start()

            when(j < n - HEAD + HALO_LAG, functools.partial(pass_halo, j + HEAD - HALO_LAG))
            when(j < n - HEAD, functools.partial(pass_head, j + HEAD))
            group = lax.div(j, OWN_GROUP) + FIRST_OWN
            when((lax.rem(j, OWN_GROUP) == 0) & (group < n // OWN_GROUP), functools.partial(produce, group))

        loop("stream", n + 1, stream)

        @pl.when(half == 1)
        def _():
            blocks(cross_row, CROSS * chunk, value1(2), store_cross)
            when(has_later, cross.start)

        def rest(j):
            blocks(j * FINE, FINE, value1(1), store_picked(1))
            near_outer.fine(j).start()
            crossed = (half == 1) & (j >= n_plain * pieces)

            @pl.when(crossed)
            def _():
                when(has_earlier & (j == n_plain * pieces), cross.wait_recv)
                send_crossed(pl.multiple_of(j * FINE, FINE))

            @pl.when(jnp.logical_not(crossed))
            def _():
                blocks(j * FINE, FINE, value1(2), store_picked(2))

            far_inner.fine(j).start()

            @pl.when(half == 1)
            def _():
                blocks(j * FINE, FINE, value1(3), store_land)
                when(has_later, edge.fine(j).start)

            turn = j - REST_FIRST

            @pl.when((half == 0) & (turn >= 0) & (lax.rem(jnp.maximum(turn, 0), REST_STEP) == 0))
            def _():
                take(lax.div(turn, REST_STEP))

        loop("rest", n_fine, rest)
        when(half == 0, functools.partial(loop, "own", OWN_LEAD, keep_own))

    loop("receive", n + EDGE_LAG, receive)

    @pl.when(outer)
    def _():
        head_all.wait_send()
        far_all.wait_send()

    @pl.when(inner)
    def _():
        own1_all.wait_send()
        far_on_all.wait_send()
        when(has_later, halo_all.wait_send)
        when(has_earlier, halo_on_all.wait_send)
        far_outer_all.wait_send()
        near_outer_all.wait_send()
        far_inner_all.wait_send()

        when((half == 1) & has_later, cross.wait_send)

    plain = pl.ds(0, cross_row)
    edge_plain = remote(land.at[1, plain], early.at[plain], 11, s_edge.at[0], later)
    when(has_later & joins_here, edge_all.wait_send)
    when(has_later & jnp.logical_not(joins_here), edge_plain.wait_send)
    own0(None, c * rows).wait_send()
    when((c == 1) & has_later, rim_out0(None).wait_send)
    when((c == 1) & has_earlier, rim_in0(None).wait_send)


def per_device_fused(tm_size, band_state, lower_rows, upper_rows, delays, counts):
    row_count, samples = band_state.shape
    tiles = samples // LANES
    n = row_count // CHUNK_ROWS
    dma = pltpu.SemaphoreType.DMA
    wide = pltpu.VMEM((row_count, tiles, LANES), jnp.float32)
    return pl.pallas_call(
        functools.partial(kernel, tiles, tm_size),
        out_shape=pltpu.VMEM((row_count, samples), jnp.float32),
        in_specs=[pl.BlockSpec(memory_space=pltpu.HBM)] * 5,
        out_specs=pl.BlockSpec(memory_space=pltpu.VMEM),
        scratch_shapes=[
            pltpu.VMEM(band_state.shape, jnp.float32),
            pltpu.VMEM(lower_rows.shape, jnp.int32),
            pltpu.VMEM(upper_rows.shape, jnp.int32),
            pltpu.VMEM(delays.shape, jnp.int32),
            pltpu.SMEM(counts.shape, jnp.int32),
            pltpu.VMEM((4 * row_count, LANES), jnp.int32),
            pltpu.VMEM((2 * row_count, LANES), jnp.int32),
            pltpu.VMEM((2 * row_count, LANES), jnp.int32),
            pltpu.VMEM((4 * row_count // LANES, LANES), jnp.int32),
            pltpu.SMEM((4 * row_count // LANES, LANES), jnp.int32),
            pltpu.VMEM((4 * row_count // LANES, LANES), jnp.int32),
            pltpu.SMEM((4 * row_count // LANES, LANES), jnp.int32),
            pltpu.VMEM((2 * row_count, 2 * tiles, LANES), jnp.float32),
            wide,
            wide,
            pltpu.VMEM((4 * row_count, 2 * tiles, LANES), jnp.float32),
            wide, wide, wide, wide, wide,
            pltpu.VMEM((3, row_count, tiles, LANES), jnp.float32),
            pltpu.VMEM((2, row_count, tiles, LANES), jnp.float32),
            wide,
            pltpu.VMEM((CROSS * CHUNK_ROWS, tiles, LANES), jnp.float32),
            pltpu.VMEM((CROSS * CHUNK_ROWS, tiles, LANES), jnp.float32),
            pltpu.VMEM((row_count, 2 * tiles, LANES), jnp.float32),
            wide,
            dma((14,)),
            dma((CHUNKS_0 + 4,)),
            dma((2,)),
            dma((3 * CHUNKS_0,)),
            dma((n,)),
            dma((n,)),
            dma((n,)),
            dma((n // OWN_GROUP,)),
            dma((n,)),
            dma((n,)),
            dma((row_count // COARSE,)),
            dma((row_count // FINE,)),
            dma((n,)),
            dma((1,)),
        ],
        compiler_params=pltpu.CompilerParams(
            collective_id=0, has_side_effects=True, vmem_limit_bytes=58 * 2**20
        ),
    )(band_state, lower_rows, upper_rows, delays, counts)


def solution(mesh):
    if mesh.shape["freq"] == 2**ITERS:
        body = functools.partial(per_device_fused, mesh.shape["tm"])
    else:
        body = per_device_general
    return jax.shard_map(
        body,
        mesh=mesh,
        in_specs=(P("freq", "tm"), P(), P(), P(), P()),
        out_specs=P("freq", "tm"),
        check_vma=False,
    )
```

```python
import contextlib
import functools

import jax
import jax.numpy as jnp
from jax import lax
from jax.experimental import pallas as pl
from jax.experimental.pallas import tpu as pltpu
from jax.sharding import PartitionSpec as P

DMAX = 2048
ITERS = 3
LANES = 128
SUBLANES = 8
UNROLL = 16
CHUNKS_0 = 2
CHUNK_ROWS = 16
HEAD = 2
HALO_LAG = 2
FIRST_OWN = 1
OWN_GROUP = 2
PLAN_UNROLL = 8
EDGE_LAG = 2
REST_FIRST = 8
REST_STEP = 2
OWN_LEAD = 2
CROSS = 2
COARSE = 64
FINE = 16


def shifted_2(block, axis, distance):
    devices = range(lax.axis_size(axis))
    route = [(i - distance, i) for i in devices if i - distance in devices]
    return lax.ppermute(block, axis, route)


def delay_columns(extended, shifts, widest):
    row_count = extended.shape[0]
    for bit_index in range(widest.bit_length()):
        stride = 1 << bit_index
        shifted = jnp.concatenate(
            [jnp.zeros((row_count, stride), extended.dtype), extended[:, :-stride]], axis=1
        )
        extended = jnp.where((shifts >> bit_index & 1)[:, None] == 1, shifted, extended)
    return extended


def live_mask(global_rows, counts, width_out, offset, bands_out):
    band_index = global_rows // width_out
    band_counts = counts[offset : offset + bands_out]
    matches = band_index[:, None] == jnp.arange(bands_out, dtype=jnp.int32)[None, :]
    live_count = jnp.sum(jnp.where(matches, band_counts[None, :], 0), axis=1)
    return global_rows % width_out < live_count


def per_device_general(band_state, lower_rows, upper_rows, delays, counts):
    row_count, samples = band_state.shape
    freq_index = lax.axis_index("freq")
    first_row = freq_index * row_count
    global_rows = first_row + jnp.arange(row_count, dtype=jnp.int32)
    current = band_state
    for iteration in range(ITERS):
        width_in = DMAX >> ITERS - iteration
        width_out = 2 * width_in
        bands_out = DMAX // width_out
        offset = 2**ITERS - 2 ** (ITERS - iteration)
        lower_source = lax.dynamic_slice_in_dim(lower_rows[iteration], first_row, row_count)
        upper_source = lax.dynamic_slice_in_dim(upper_rows[iteration], first_row, row_count)
        own_delays = lax.dynamic_slice_in_dim(delays[iteration], first_row, row_count)
        gathered = lax.all_gather(current, "freq", axis=0, tiled=True)
        lower_values = jnp.take(gathered, lower_source, axis=0)
        upper_values = jnp.take(gathered, upper_source, axis=0)
        rim_columns = shifted_2(upper_values[:, samples - width_in :], "tm", 1)
        extended = jnp.concatenate([rim_columns, upper_values], axis=1)
        delayed = delay_columns(extended, own_delays, width_in)[:, width_in:]
        live_rows = live_mask(global_rows, counts, width_out, offset, bands_out)
        current = jnp.where(live_rows[:, None], lower_values + delayed, jnp.zeros_like(delayed))
    return current


MESH = pl.DeviceIdType.MESH


def phase(name):
    return contextlib.nullcontext()


def kernel(
    tiles, tm_size, x_in, lower_in, upper_in, delays_in, counts_in,
    out_ref, x_ref, lower, upper, delays, counts, columns, columns_0, places, plan_v, plan, picks_v, picks, raw, rim_in, mine, cur, own_in, far_in, far_pass, halo_in, halo_pass,
    picked, land, early, cross_own, cross_in, joined, final,
    sent, s_load, s_plan, s_raw, s_head, s_far, s_far_pass, s_own, s_halo, s_halo_pass, s_fo, s_last, s_edge, s_cross,
):
    f, t = lax.axis_index("freq"), lax.axis_index("tm")
    c, z = lax.rem(f, 2), lax.div(f, 2)
    zb, half = lax.rem(z, 2), lax.div(z, 2)
    rows = x_ref.shape[0]
    chunk = CHUNK_ROWS
    n = rows // chunk
    at = lambda ff, tt: {"freq": ff, "tm": tt}
    partner = at(f + 1 - 2 * c, t)
    near = at(f + 2 - 4 * zb, t)
    across = at(f + 4 - 8 * half, t)
    facing = at(f + 2 - 4 * half, t)
    later = at(f, t + 1)
    earlier = at(f, t - 1)
    inner = zb != half
    outer = zb == half
    has_later, has_earlier = t < tm_size - 1, t > 0

    n0, chunk0 = CHUNKS_0, rows // CHUNKS_0

    def load(j, source, target):
        return pltpu.make_async_copy(source, target, s_load.at[j])

    parts = [pl.ds(j * chunk0, chunk0) for j in range(n0)]
    loads = [load(j, x_in.at[part], x_ref.at[part]) for j, part in enumerate(parts)]
    pairs = ((lower_in, lower), (upper_in, upper), (delays_in, delays), (counts_in, counts))
    table_loads = [load(n0 + j, *pair) for j, pair in enumerate(pairs)]
    for copy in loads + table_loads:
        copy.start()

    barrier = pltpu.get_barrier_semaphore()

    def greet(target):
        pl.semaphore_signal(barrier, inc=1, device_id=target, device_id_type=MESH)

    greet(partner)
    greet(near)
    greet(across)
    for cond, target in ((inner, facing), (has_earlier, earlier), (has_later, later)):
        pl.when(cond)(functools.partial(greet, target))

    lane = lax.broadcasted_iota(jnp.int32, (tiles, LANES), 1)
    zero = jnp.zeros((tiles, LANES), jnp.float32)

    def when(cond, action):
        pl.when(cond)(action)

    def remote(src, dst, flow, sem, target):
        return pltpu.make_async_remote_copy(
            src_ref=src, dst_ref=dst, send_sem=sent.at[flow], recv_sem=sem,
            device_id=target, device_id_type=MESH,
        )

    def span(j, group=1):
        return pl.ds(pl.multiple_of(j * chunk * group, chunk * group), chunk * group)

    n_fine = rows // FINE

    def coarse(j):
        return pl.ds(pl.multiple_of(j * COARSE, COARSE), COARSE)

    def fine(j):
        return pl.ds(pl.multiple_of(j * FINE, FINE), FINE)

    def delayed(source, row, d, first):
        q, r = d >> 7, d & (LANES - 1)
        a = source[row, pl.ds(tiles - q, tiles), :]
        b = source[row, pl.ds(jnp.maximum(tiles - 1 - q, first), tiles), :]
        a, b = pltpu.roll(a, r, 1), pltpu.roll(b, r, 1)
        return jnp.where(lane >= r, a, b)

    def blocks(start, count, value, store):
        def body(base, size):
            values = [(base + u, value(base, u)) for u in range(size)]
            for m, v in values:
                store(m, v)

        def step(i, carry):
            body(start + i * UNROLL, UNROLL)
            return carry

        if count <= UNROLL:
            body(start, count)
        else:
            lax.fori_loop(0, count // UNROLL, step, 0)

    rim0 = rows // LANES
    full0, tail0, kept0 = pl.ds(tiles, tiles), pl.ds(2 * tiles - rim0, rim0), pl.ds(tiles - rim0, rim0)

    def part_of(j, row=0):
        return pl.ds(row, rows) if j is None else pl.ds(row + j * chunk0, chunk0)

    def own0(j, row):
        at_rows = raw.at[part_of(j, row), full0]
        return remote(at_rows, at_rows, 0, s_raw.at[j or 0], partner)

    def rim_out0(j):
        return remote(raw.at[part_of(j, rows), tail0], rim_in.at[part_of(j), kept0], 1, s_raw.at[n0 + (j or 0)], later)

    def rim_in0(j):
        at_rows = rim_in.at[part_of(j), kept0]
        return remote(at_rows, at_rows, 2, s_raw.at[2 * n0 + (j or 0)], partner)

    def spread(first, count, first_tile, last_tile):
        def body(step, carry):
            r = first + step * SUBLANES
            for tile in range(first_tile, last_tile):
                raw[pl.ds(c * rows + r, SUBLANES), tiles + tile, :] = x_ref[
                    pl.ds(r, SUBLANES), pl.ds(tile * LANES, LANES)
                ]
            return carry

        lax.fori_loop(0, count // SUBLANES, body, 0)

    for j in range(n0):
        with phase("spread"):
            loads[j].wait()
            spread(j * chunk0, chunk0, tiles - rim0, tiles)
    one = lambda cond: jnp.where(cond, 1, 0)
    with phase("greet"):
        pl.semaphore_wait(barrier, 3 + one(inner) + one(has_earlier) + one(has_later))
    for j in range(n0):
        when((c == 1) & has_later, rim_out0(j).start)
    for j in range(n0):
        with phase("send0"):
            spread(j * chunk0, chunk0, 0, tiles - rim0)
            own0(j, c * rows).start()

    def clear(count, store):
        def body(i, carry):
            for u in range(UNROLL):
                store(i * UNROLL + u)
            return carry

        lax.fori_loop(0, count // UNROLL, body, 0)

    @pl.when(t == 0)
    def _():
        def clear_raw(i):
            raw[rows + i, :tiles, :] = zero

        def clear_cur(i):
            cur[2 * rows + i, :tiles, :] = zero

        def clear_early(i):
            early[i] = zero

        clear(rows, clear_raw)
        clear(2 * rows, clear_cur)
        clear(rows, clear_early)

        def clear_cross(i):
            cross_in[i] = zero

        clear(CROSS * CHUNK_ROWS, clear_cross)

    chip_rows, half_rows = 2 * rows, 4 * rows
    flat = (SUBLANES, LANES)
    lane_at = lax.broadcasted_iota(jnp.int32, flat, 1)
    line_at = lax.broadcasted_iota(jnp.int32, flat, 0)
    none = jnp.zeros(flat, jnp.int32)
    groups = lambda count: range(count // LANES)

    def row_of(table, level, start):
        return jnp.broadcast_to(table[level : level + 1, pl.ds(pl.multiple_of(start, LANES), LANES)], flat)

    def wanted(start):
        return jnp.where(half == 0, row_of(lower, ITERS - 1, start), row_of(upper, ITERS - 1, start)) & (half_rows - 1)

    def set_columns(target, start, row):
        target[pl.ds(start, LANES), :] = jnp.broadcast_to(row[0:1], (LANES, LANES)).T

    def fold(values, combine):
        for s in (4, 2, 1):
            values = [combine(v, pltpu.roll(v, s, 0)) for v in values]
        return values

    def scan(count, init, step):
        def body(i, carry):
            for u in range(PLAN_UNROLL):
                at_row = (i * PLAN_UNROLL + u) * SUBLANES
                carry = step(pl.multiple_of(at_row, SUBLANES), line_at + at_row, carry)
            return carry

        return lax.fori_loop(0, count // SUBLANES // PLAN_UNROLL, body, init)

    add, least = lambda a, b: a + b, jnp.minimum
    bit = lambda cond, place: jnp.where(cond, 1 << place, 0)

    def find_order():
        for g in groups(half_rows):
            start = half * half_rows + g * LANES
            low, high = row_of(lower, 1, start), row_of(upper, 1, start)
            set_columns(columns, g * LANES, (low & (chip_rows - 1)) | (high & (chip_rows - 1)) << 9)
        want = [wanted((1 - half) * 3 * chip_rows + g * LANES) for g in groups(chip_rows)]

        def use(at_row, index, carry):
            line = columns[pl.ds(at_row, SUBLANES), :]
            return tuple(v + jnp.where(w == index, line, 0) for v, w in zip(carry, want))

        used = fold(scan(half_rows, (none,) * len(want), use), add)
        for g, row in enumerate(used):
            set_columns(columns, g * LANES, row)

        def meet(at_row, index, carry):
            line = columns[pl.ds(at_row, SUBLANES), :]
            low, high = line & (chip_rows - 1), line >> 9
            turn = 2 * (index & (rows - 1)) + lax.div(index, rows)
            hits = [(part, g) for part in (low, high) for g in groups(chip_rows)]
            return tuple(
                least(v, jnp.where(part == lane_at + g * LANES, turn, chip_rows)) for v, (part, g) in zip(carry, hits)
            )

        never = jnp.full(flat, chip_rows, jnp.int32)
        first = fold(scan(chip_rows, (never,) * (2 * len(want)), meet), least)
        keys = [v * chip_rows + lane_at + (g % len(want)) * LANES for g, v in enumerate(first)]
        for g, row in enumerate(keys):
            set_columns(columns, g * LANES, row)

        def count(at_row, index, carry):
            low = columns[pl.ds(at_row, SUBLANES), :]
            high = columns[pl.ds(chip_rows + at_row, SUBLANES), :]
            parts = [low] * len(want) + [high] * len(want)
            return tuple(v + jnp.where(part < key, 1, 0) for v, part, key in zip(carry, parts, keys))

        ranks = fold(scan(chip_rows, (none,) * len(keys), count), add)
        place = [(v & 1) * rows + (v >> 1) for v in ranks]
        for g in groups(chip_rows):
            low, high = place[g], place[len(want) + g]
            set_columns(places, g * LANES, low | high << 9)
            start = z * chip_rows + g * LANES
            low, high = row_of(lower, 0, start), row_of(upper, 0, start)
            live = bit(lane_at + g * LANES < counts[z], 28)
            word = (low & (chip_rows - 1)) | (high & (chip_rows - 1)) << 9 | row_of(delays, 0, start) << 18 | live
            set_columns(columns_0, g * LANES, word)

        def pick(at_row, index, carry):
            line = places[pl.ds(at_row, SUBLANES), :]
            own = jnp.where(zb == 0, line & (chip_rows - 1), line >> 9)
            word = columns_0[pl.ds(at_row, SUBLANES), :]
            return tuple(
                v + jnp.where(own == lane_at + (c * rows + g * LANES), word, 0) for g, v in enumerate(carry)
            )

        words = fold(scan(chip_rows, (none,) * len(groups(rows)), pick), add)
        for g, row in enumerate(words):
            plan_v[pl.ds(g, 1), :] = row[0:1]
            start = f * rows + g * LANES
            live = bit(lane_at + start < counts[2**ITERS - 2], 12)
            plan_v[pl.ds(rows // LANES + g, 1), :] = (row_of(delays, 2, start) | live)[0:1]
        facing_end = (f + 2 - 4 * half) * rows + rows - LANES
        plan_v[pl.ds(2 * rows // LANES, 1), :] = row_of(delays, 2, facing_end)[0:1]
        pltpu.make_async_copy(plan_v, plan, s_plan.at[0]).start()

    def place_rows():
        marks = [half * half_rows + g * LANES for g in groups(half_rows)]
        low = [row_of(lower, 1, start) & (chip_rows - 1) for start in marks]
        high = [row_of(upper, 1, start) & (chip_rows - 1) for start in marks]

        def put(at_row, index, carry):
            line = places[pl.ds(at_row, SUBLANES), :]
            shifted = line >> 9 << 9
            line = line & (chip_rows - 1)
            return tuple(
                v + jnp.where(a == index, line, 0) + jnp.where(b == index, shifted, 0)
                for v, a, b in zip(carry, low, high)
            )

        words = fold(scan(chip_rows, (none,) * len(marks), put), add)
        for g, (start, word) in enumerate(zip(marks, words)):
            live = bit(lane_at + g * LANES < counts[2 ** (ITERS - 1) + half], 28)
            set_columns(columns, g * LANES, word | row_of(delays, 1, start) << 18 | live)

    def pick_rows():
        targets = (f + 4 - 8 * half, f + 2 - 4 * zb, f + 2 - 4 * half, f)
        want = [wanted(target * rows + g * LANES) for target in targets for g in groups(rows)]

        def pick(at_row, index, carry):
            line = columns[pl.ds(at_row, SUBLANES), :]
            return tuple(v + jnp.where(w == index, line, 0) for v, w in zip(carry, want))

        words = fold(scan(half_rows, (none,) * len(want), pick), add)
        for g, row in enumerate(words):
            picks_v[pl.ds(g, 1), :] = row[0:1]
        pltpu.make_async_copy(picks_v, picks, s_plan.at[1]).start()

    with phase("order"):
        for copy in table_loads:
            copy.wait()
        find_order()

    def take_rim():
        for j in range(n0):

            @pl.when((c == 1) & has_earlier)
            def _():
                with phase("rim_out"):
                    rim_out0(j).wait_recv()
                    rim_in0(j).start()

        for j in range(n0):
            with phase("rim_in"):
                when((c == 0) & has_earlier, rim_in0(j).wait_recv)

        @pl.when(has_earlier)
        def _():
            def fill(i):
                raw[rows + i, :tiles, :] = rim_in[i]

            clear(rows, fill)

    own_base, far_base = zb * 2 * rows, (1 - zb) * 2 * rows
    up_base = 2 * rows
    def entry(table, first, base, u):
        return table[first + (base >> 7), (base & (LANES - 1)) + u]

    def value0(base, u):
        word = entry(plan, 0, base, u)
        lo, up, d = word & 511, (word >> 9) & 511, (word >> 18) & 1023
        total = raw[lo, tiles:, :] + delayed(raw, up, d, tiles - rim0)
        return jnp.where((word >> 28) == 1, total, zero)

    split = tiles // 2

    def store0(m, v):
        mine[m] = v
        cur[own_base + c * rows + m, tiles:, :] = v

    def store_mine(m, v):
        mine[m] = v

    def store_head(m, v):
        mine[m, split:, :] = v[split:, :]

    def store_tail(m, v):
        mine[m, :split, :] = v[:split, :]

    rim1 = 2 * rows // LANES

    def value1(kind):
        def value(base, u):
            word = entry(picks, kind * (rows // LANES), base, u)
            a, b, d = word & 511, (word >> 9) & 511, (word >> 18) & 1023
            total = cur[a, tiles:, :] + delayed(cur, up_base + b, d, tiles - rim1)
            return jnp.where((word >> 28) == 1, total, zero)

        return value

    def store_picked(kind):
        def store(m, v):
            picked[kind, m] = v

        return store

    def store_land(m, v):
        land[half, m] = v

    def join(m):
        joined[m, :tiles, :] = early[m]
        joined[m, tiles:, :] = land[1, m]

    def value2(base, u):
        word = entry(plan, rows // LANES, base, u)
        total = land[0, base + u] + delayed(joined, base + u, word & 4095, 0)
        return jnp.where((word >> 12) == 1, total, zero)

    def store2(m, v):
        final[m] = v

    def finish(first, count, prepare, value):
        def step(i, carry):
            start = pl.multiple_of(first + i * FINE, FINE)
            if prepare is not None:
                for u in range(FINE):
                    prepare(start + u)
            blocks(start, FINE, value, store2)
            for tile in range(tiles):
                at_tile = pl.ds(tile * LANES, LANES)
                out_ref[pl.ds(start, FINE), at_tile] = final[pl.ds(start, FINE), tile, :]
            return carry

        lax.fori_loop(0, count // FINE, step, 0)

    rim = pl.ds(tiles - rim1, rim1)
    every = pl.ds(0, rows)

    def flow(index, src, dst, sems, target):
        def copy(j, group=1):
            at_rows = span(j, group)
            return remote(src(at_rows), dst(at_rows), index, sems.at[j], target)

        copy.coarse = lambda j: remote(src(coarse(j)), dst(coarse(j)), index, sems.at[j], target)
        copy.fine = lambda j: remote(src(fine(j)), dst(fine(j)), index, sems.at[lax.div(j, n_fine // sems.shape[0])], target)

        return copy, remote(src(every), dst(every), index, sems.at[0], target)

    lead, trail = pl.ds(split, tiles - split), pl.ds(0, split)
    head, head_all = flow(3, lambda r: mine.at[r, lead], lambda r: far_in.at[r, lead], s_head, near)
    far, far_all = flow(12, lambda r: mine.at[r, trail], lambda r: far_in.at[r, trail], s_far, near)
    far_on, far_on_all = flow(4, lambda r: far_in.at[r], lambda r: far_pass.at[r], s_far_pass, partner)
    own1, own1_all = flow(5, lambda r: mine.at[r], lambda r: own_in.at[r], s_own, partner)
    halo_mine, halo_all = flow(6, lambda r: mine.at[r, rim], lambda r: halo_in.at[r, rim], s_halo, later)
    halo_far, _ = flow(6, lambda r: far_in.at[r, rim], lambda r: halo_in.at[r, rim], s_halo, later)
    halo_on, halo_on_all = flow(7, lambda r: halo_in.at[r, rim], lambda r: halo_pass.at[r, rim], s_halo_pass, partner)
    to_half = lambda h: lambda r: land.at[h, r]
    _, far_outer_all = flow(8, lambda r: picked.at[0, r], to_half(half), s_fo, across)
    far_outer = lambda j: remote(
        picked.at[0, span(j)], land.at[half, span(j)], 8, s_fo.at[lax.div(j * chunk, COARSE)], across
    )
    near_outer, near_outer_all = flow(9, lambda r: picked.at[1, r], to_half(half), s_last, near)
    far_inner, far_inner_all = flow(10, lambda r: picked.at[2, r], to_half(half), s_last, facing)
    got_across, _ = flow(8, lambda r: picked.at[0, r], to_half(1 - half), s_fo, across)
    got_facing, _ = flow(10, lambda r: picked.at[2, r], to_half(1 - half), s_last, facing)
    edge, edge_all = flow(11, lambda r: land.at[1, r], lambda r: early.at[r], s_edge, later)

    def loop(name, count, body):
        def step(j, carry):
            with phase(name):
                body(j)
            return carry

        lax.fori_loop(0, count, step, 0)

    last_rows = zb == 1
    pieces = chunk // FINE
    taken = (n_fine - 1 - REST_FIRST) // REST_STEP + 1

    n_plain = n - CROSS
    cross_row = n_plain * chunk
    joins_here = outer | (half == 1)
    whole = pl.ds(0, CROSS * chunk)
    cross = remote(cross_own.at[whole], cross_in.at[whole], 13, s_cross.at[0], later)

    def take(j):
        when(inner, got_facing.fine(j).wait_recv)
        when(outer, near_outer.fine(j).wait_recv)
        when(last_rows & has_later & (joins_here | (j < n_plain * pieces)), edge.fine(j).start)

    def store_cross(m, v):
        cross_own[m - cross_row] = v

    def cross_value(base, u):
        word = entry(plan, rows // LANES + 1, base, u)
        return delayed(joined, base + u, word, 0)

    def plain_value(base, u):
        word = entry(plan, rows // LANES, base, u)
        return jnp.where((word >> 12) == 1, land[0, base + u] + land[1, base + u], zero)

    def send_crossed(first):
        for u in range(FINE):
            joined[first + u, :tiles, :] = cross_in[first - cross_row + u]
            joined[first + u, tiles:, :] = cross_own[first - cross_row + u]
        blocks(first, FINE, cross_value, store_picked(2))

    def keep_own(p):
        blocks(p * chunk, chunk, value1(3), store_land)

    def receive(p):
        @pl.when(p < n)
        def _():
            for i in range(pieces):
                j = p * pieces + i
                when(outer | (half == 1) | (j >= taken), functools.partial(take, j))

        when(inner & (half == 0) & (p < n - OWN_LEAD), functools.partial(keep_own, p + OWN_LEAD))

        k = p - jnp.where(last_rows, EDGE_LAG, 0)

        @pl.when((k >= 0) & (k < n))
        def _():
            joins = joins_here | (k < n_plain)

            @pl.when(joins)
            def _():
                when(has_earlier, edge(k).wait_recv)
                finish(k * chunk, chunk, join, value2)

            @pl.when(jnp.logical_not(joins))
            def _():
                finish(k * chunk, chunk, None, plain_value)

    when(inner, place_rows)
    when(inner, pick_rows)
    for j in range(n0):
        with phase("own0"):
            own0(j, (1 - c) * rows).wait_recv()
    pltpu.make_async_copy(plan_v, plan, s_plan.at[0]).wait()

    @pl.when(outer)
    def _():
        def send_head(j):
            blocks(j * chunk, chunk, value0, store_head)
            head(j).start()

        loop("heads", HEAD, send_head)
        take_rim()

        def produce(j):
            @pl.when(j < HEAD)
            def _():
                blocks(j * chunk, chunk, value0, store_tail)

            far(j).start()

            @pl.when(j + HEAD < n)
            def _():
                blocks((j + HEAD) * chunk, chunk, value0, store_mine)
                head(j + HEAD).start()

        loop("produce", n, produce)

        def from_across(j):
            got_across.coarse(j).wait_recv()

            @pl.when((half == 0) & has_later)
            def _():
                for i in range(COARSE // FINE):
                    edge.fine(j * (COARSE // FINE) + i).start()

        loop("from_across", rows // COARSE, from_across)

    @pl.when(inner)
    def _():
        def produce(j):
            for i in range(OWN_GROUP):
                blocks((j * OWN_GROUP + i) * chunk, chunk, value0, store0)
                when((half == 0) & has_later, halo_mine(j * OWN_GROUP + i).start)
            own1(j, OWN_GROUP).start()

        take_rim()

        def pass_head(j):
            head(j).wait_recv()
            when((half == 1) & has_later, halo_far(j).start)

        def pass_halo(j):
            @pl.when(has_earlier)
            def _():
                halo_mine(j).wait_recv()
                halo_on(j).start()

        def begin(j):
            when(half == 1, functools.partial(pass_head, j))
            produce(j)

        loop("produce", FIRST_OWN, begin)
        loop("heads", HEAD, lambda j: when((half == 0) | (j >= FIRST_OWN), functools.partial(pass_head, j)))
        pltpu.make_async_copy(picks_v, picks, s_plan.at[1]).wait()
        loop("halos", HEAD - HALO_LAG, pass_halo)

        def gather(k):
            @pl.when(lax.rem(k, OWN_GROUP) == 0)
            def _():
                own1(lax.div(k, OWN_GROUP), OWN_GROUP).wait_recv()

            far_on(k).wait_recv()
            start = pl.multiple_of(k * chunk, chunk)
            mine_at, other_at = c * rows + start, (1 - c) * rows + start
            for u in range(chunk):
                cur[own_base + other_at + u, tiles:, :] = own_in[start + u]
                cur[far_base + mine_at + u, tiles:, :] = far_in[start + u]
                cur[far_base + other_at + u, tiles:, :] = far_pass[start + u]

            @pl.when(has_earlier)
            def _():
                halo_on(k).wait_recv()
                for u in range(chunk):
                    cur[up_base + mine_at + u, :tiles, :] = halo_in[start + u]
                    cur[up_base + other_at + u, :tiles, :] = halo_pass[start + u]

            blocks(k * chunk, chunk, value1(0), store_picked(0))
            far_outer(k).start()

        def stream(j):
            when(j > 0, functools.partial(gather, j - 1))

            @pl.when(j < n)
            def _():
                far(j).wait_recv()
                far_on(j).start()

            when(j < n - HEAD + HALO_LAG, functools.partial(pass_halo, j + HEAD - HALO_LAG))
            when(j < n - HEAD, functools.partial(pass_head, j + HEAD))
            group = lax.div(j, OWN_GROUP) + FIRST_OWN
            when((lax.rem(j, OWN_GROUP) == 0) & (group < n // OWN_GROUP), functools.partial(produce, group))

        loop("stream", n + 1, stream)

        @pl.when(half == 1)
        def _():
            blocks(cross_row, CROSS * chunk, value1(2), store_cross)
            when(has_later, cross.start)

        def rest(j):
            crossed = (half == 1) & (j >= n_plain * pieces)

            @pl.when(crossed)
            def _():
                when(has_earlier & (j == n_plain * pieces), cross.wait_recv)
                send_crossed(pl.multiple_of(j * FINE, FINE))

            @pl.when(jnp.logical_not(crossed))
            def _():
                blocks(j * FINE, FINE, value1(2), store_picked(2))

            far_inner.fine(j).start()
            blocks(j * FINE, FINE, value1(1), store_picked(1))
            near_outer.fine(j).start()

            @pl.when(half == 1)
            def _():
                blocks(j * FINE, FINE, value1(3), store_land)
                when(has_later, edge.fine(j).start)

            turn = j - REST_FIRST

            @pl.when((half == 0) & (turn >= 0) & (lax.rem(jnp.maximum(turn, 0), REST_STEP) == 0))
            def _():
                take(lax.div(turn, REST_STEP))

        loop("rest", n_fine, rest)
        when(half == 0, functools.partial(loop, "own", OWN_LEAD, keep_own))

    loop("receive", n + EDGE_LAG, receive)

    @pl.when(outer)
    def _():
        head_all.wait_send()
        far_all.wait_send()

    @pl.when(inner)
    def _():
        own1_all.wait_send()
        far_on_all.wait_send()
        when(has_later, halo_all.wait_send)
        when(has_earlier, halo_on_all.wait_send)
        far_outer_all.wait_send()
        near_outer_all.wait_send()
        far_inner_all.wait_send()

        when((half == 1) & has_later, cross.wait_send)

    plain = pl.ds(0, cross_row)
    edge_plain = remote(land.at[1, plain], early.at[plain], 11, s_edge.at[0], later)
    when(has_later & joins_here, edge_all.wait_send)
    when(has_later & jnp.logical_not(joins_here), edge_plain.wait_send)
    own0(None, c * rows).wait_send()
    when((c == 1) & has_later, rim_out0(None).wait_send)
    when((c == 1) & has_earlier, rim_in0(None).wait_send)


def per_device_fused(tm_size, band_state, lower_rows, upper_rows, delays, counts):
    row_count, samples = band_state.shape
    tiles = samples // LANES
    n = row_count // CHUNK_ROWS
    dma = pltpu.SemaphoreType.DMA
    wide = pltpu.VMEM((row_count, tiles, LANES), jnp.float32)
    return pl.pallas_call(
        functools.partial(kernel, tiles, tm_size),
        out_shape=pltpu.VMEM((row_count, samples), jnp.float32),
        in_specs=[pl.BlockSpec(memory_space=pltpu.HBM)] * 5,
        out_specs=pl.BlockSpec(memory_space=pltpu.VMEM),
        scratch_shapes=[
            pltpu.VMEM(band_state.shape, jnp.float32),
            pltpu.VMEM(lower_rows.shape, jnp.int32),
            pltpu.VMEM(upper_rows.shape, jnp.int32),
            pltpu.VMEM(delays.shape, jnp.int32),
            pltpu.SMEM(counts.shape, jnp.int32),
            pltpu.VMEM((4 * row_count, LANES), jnp.int32),
            pltpu.VMEM((2 * row_count, LANES), jnp.int32),
            pltpu.VMEM((2 * row_count, LANES), jnp.int32),
            pltpu.VMEM((4 * row_count // LANES, LANES), jnp.int32),
            pltpu.SMEM((4 * row_count // LANES, LANES), jnp.int32),
            pltpu.VMEM((4 * row_count // LANES, LANES), jnp.int32),
            pltpu.SMEM((4 * row_count // LANES, LANES), jnp.int32),
            pltpu.VMEM((2 * row_count, 2 * tiles, LANES), jnp.float32),
            wide,
            wide,
            pltpu.VMEM((4 * row_count, 2 * tiles, LANES), jnp.float32),
            wide, wide, wide, wide, wide,
            pltpu.VMEM((3, row_count, tiles, LANES), jnp.float32),
            pltpu.VMEM((2, row_count, tiles, LANES), jnp.float32),
            wide,
            pltpu.VMEM((CROSS * CHUNK_ROWS, tiles, LANES), jnp.float32),
            pltpu.VMEM((CROSS * CHUNK_ROWS, tiles, LANES), jnp.float32),
            pltpu.VMEM((row_count, 2 * tiles, LANES), jnp.float32),
            wide,
            dma((14,)),
            dma((CHUNKS_0 + 4,)),
            dma((2,)),
            dma((3 * CHUNKS_0,)),
            dma((n,)),
            dma((n,)),
            dma((n,)),
            dma((n // OWN_GROUP,)),
            dma((n,)),
            dma((n,)),
            dma((row_count // COARSE,)),
            dma((row_count // FINE,)),
            dma((n,)),
            dma((1,)),
        ],
        compiler_params=pltpu.CompilerParams(
            collective_id=0, has_side_effects=True, vmem_limit_bytes=58 * 2**20
        ),
    )(band_state, lower_rows, upper_rows, delays, counts)


def solution(mesh):
    if mesh.shape["freq"] == 2**ITERS:
        body = functools.partial(per_device_fused, mesh.shape["tm"])
    else:
        body = per_device_general
    return jax.shard_map(
        body,
        mesh=mesh,
        in_specs=(P("freq", "tm"), P(), P(), P(), P()),
        out_specs=P("freq", "tm"),
        check_vma=False,
    )
```
